128 devices in a mesh: seq: 8 (over z_hi, x), exp: 16 (over z_lo, y, core).
Axes of the slice: x: 4, y: 4, z: 4 (z_hi: 2, z_lo: 2; z = z_hi * 2 + z_lo), core: 2. Of those that a mesh axis runs over, the one named last changes fastest.
Arguments:
- queries: bfloat16 [16384, 3072], P(('seq', 'exp')), may hold values from -123 to 123
- keys: bfloat16 [16384, 512], P(('seq', 'exp')), may hold values from -6 to 6
- values: bfloat16 [16384, 512], P(('seq', 'exp')), may hold values from -9 to 9
- residual: bfloat16 [16384, 6144], P(('seq', 'exp')), may hold values from -51 to 51
- proj_weight: bfloat16 [3072, 6144], P('seq', 'exp'), may hold values from -0.109375 to 0.109375
- norm_gain: bfloat16 [6144], replicated, may hold values from 0.099609375 to 1.8984375
- router: bfloat16 [6144, 8], replicated, may hold values from -0.078125 to 0.078125
- expert_ids: int32 [16384, 2], P(('seq', 'exp')), may hold values from 0 to 7, all different within a row; in each aligned block of 128 rows (0 to 127, 128 to 255, ...) at most 33 rows name the same one
- u_gate_up: bfloat16 [16, 3072, 1024], P('exp'), may hold values from -0.078125 to 0.078125
- v_gate_up: bfloat16 [16, 2, 512, 4096], P('exp'), may hold values from -0.25 to 0.25
- u_down: bfloat16 [16, 4096, 512], P('exp'), may hold values from -0.0625 to 0.0625
- v_down: bfloat16 [16, 512, 3072], P('exp'), may hold values from -0.25 to 0.25
Outputs:
- layer_out: bfloat16 [16384, 6144], P(('seq', 'exp'))
The draws below stay inside these ranges and needn't reach their ends.
Inputs may be any that keep to these rules, and one draw needn't show every extreme that they name: `expert_ids`: the two experts of a token differ. Among the tokens of one device no expert is named more than 33 times, and in some devices' tokens some expert is named exactly 33 times.
All inputs are finite; a program needn't handle non-finite values.
Results may differ from the reference program's by a relative error of at most 0.02.
Values may be sent and summed in bfloat16 or wider, within the bound.
No kernel may reach another device: no remote copies, remote signals or barrier semaphores. Data moves between devices by JAX's collectives and lax.ppermute only.
A program may use at most 192 MiB of HBM per device.

```python
import math
import jax
import jax.numpy as jnp
import numpy as np
from jax import lax

D = 6144
HEADS = 24
KV_HEADS = 4
HEAD_DIM = 128
EXPERTS = 8
TOP = 2
RANK = 512
FF = 8192
TOK_DEV = 128
CAP = 33
PIECES = 2
TOKENS = 16384


def draw_queries(key, part):
    noise_draw = jax.random.normal(jax.random.fold_in(key, 902), (TOKENS, HEADS, HEAD_DIM), jnp.float32)
    noise_draw = jnp.clip(noise_draw, -6.0, 6.0)
    return noise_draw.reshape(TOKENS, HEADS * HEAD_DIM).astype(jnp.bfloat16)


def draw_keys(key, part):
    noise_draw = jax.random.normal(jax.random.fold_in(key, 903), (TOKENS, KV_HEADS, HEAD_DIM), jnp.float32)
    noise_draw = jnp.clip(noise_draw, -6.0, 6.0)
    return noise_draw.reshape(TOKENS, KV_HEADS * HEAD_DIM).astype(jnp.bfloat16)


def draw_values(key, part):
    noise_draw = jax.random.normal(jax.random.fold_in(key, 904), (TOKENS, KV_HEADS * HEAD_DIM), jnp.float32)
    noise_draw = jnp.clip(noise_draw, -6.0, 6.0)
    levels = jax.random.normal(jax.random.fold_in(key, 905), (TOKENS // 256, KV_HEADS * HEAD_DIM), jnp.float32)
    levels = jnp.clip(levels, -3.0, 3.0)
    level_rows = jnp.repeat(levels, 256, axis=0)
    return (noise_draw + level_rows).astype(jnp.bfloat16)


def draw_residual(key, part):
    noise_draw = jax.random.normal(jax.random.fold_in(key, 907), (TOKENS, D), jnp.float32)
    noise_draw = jnp.clip(noise_draw, -4.0, 4.0)
    return noise_draw.astype(jnp.bfloat16)


def block_levels(own_key, dims, shards, least, top_value):
    gain = 1.0
    for dim, parts in shards:
        heights = jax.random.uniform(jax.random.fold_in(jax.random.fold_in(own_key, 6), dim), (parts,), jnp.float32, least / len(shards), top_value / len(shards))
        gain = gain * jnp.repeat(jnp.exp(heights), dims[dim] // parts).reshape((-1,) + (1,) * (len(dims) - 1 - dim))
    return gain


def assign_block(own_key, own, number, rows, number_of, top, limit, slope):
    ranking = jax.random.permutation(own_key, number_of)
    heavy_load, ordinary = load_shares(number_of, rows * top, limit, slope, True), load_shares(number_of, rows * top, limit, slope, False)
    places = jnp.arange(number_of)

    def named(lengths, turn):
        used = int((lengths > 0).sum())
        fixed = max(1, used // 4)
        passed = fixed + (places - fixed + turn * (used - fixed)) % max(1, number_of - fixed)
        return jnp.zeros((number_of,), jnp.int32).at[ranking[jnp.where(places < fixed, places, passed)]].set(jnp.asarray(lengths, jnp.int32))

    lengths = jnp.where(number % 4 == 0, named(heavy_load, number // 4), named(ordinary, number - number // 4 - 1))
    mixed = jax.random.permutation(jax.random.fold_in(own, 3), number_of)
    giver, sink = mixed[0:number_of // 2 * 2:2], mixed[1:number_of // 2 * 2:2]
    slack = jnp.minimum(lengths[giver] - 1, limit - lengths[sink]) // 2
    slack = jnp.where((giver == ranking[0]) | (sink == ranking[0]) | (lengths[sink] == 0), 0, jnp.maximum(slack, 0))
    passed = jax.random.randint(jax.random.fold_in(own, 4), (number_of // 2,), 0, 1 << 20) % (slack + 1)
    lengths = lengths.at[giver].add(-passed).at[sink].add(passed)
    items = jnp.searchsorted(jnp.cumsum(lengths), jnp.arange(rows * top), side="right").astype(jnp.int32)
    grid = items.reshape(top, rows).T
    grid = grid[jax.random.permutation(jax.random.fold_in(own, 1), rows)]
    turn = jax.random.randint(jax.random.fold_in(own, 2), (rows, 1), 0, top)
    return jnp.take_along_axis(grid, (jnp.arange(top)[None, :] + turn) % top, axis=1)


def load_shares(amount, total, most, slope, full):
    weights = [(1 << 20) // math.isqrt(rank ** slope) + 1 for rank in range(1, amount + 1)]
    largest = most if full else min(most, max(-(-total // amount), total * weights[0] // sum(weights)))
    least = 1 if total - largest >= amount - 1 else 0
    given, surplus = [largest] + [least] * (amount - 1), total - largest - least * (amount - 1)
    while surplus > 0:
        movable = [i for i in range(1, amount) if given[i] < largest] or [i for i in range(1, amount) if given[i] < most]
        whole, left = sum([weights[i] for i in movable]), surplus
        for i in movable:
            more = min(most - given[i], max(1, left * weights[i] // whole), surplus)
            given[i] = given[i] + more
            surplus = surplus - more
    return np.array(given)


def normal_values(key, shape, scale, bound, split=(), kind=jnp.bfloat16):
    factor_of = block_levels(key, shape, split, -0.22, 0.18) if split else 1.0
    drawn = jax.random.normal(key, shape, jnp.float32) * scale * factor_of
    return jnp.minimum(jnp.maximum(drawn, -bound), bound).astype(kind)


def setup_inputs(seed: int = 0) -> dict:
    streams_of = jax.random.split(jax.random.key(seed), 13)
    queries = draw_queries(jax.random.fold_in(streams_of[12], 71), 0)
    keys = draw_keys(jax.random.fold_in(streams_of[12], 71), 0)
    values = draw_values(jax.random.fold_in(streams_of[12], 71), 0)
    residual = draw_residual(jax.random.fold_in(streams_of[12], 71), 0)
    proj_weight = normal_values(streams_of[4], (HEADS * HEAD_DIM, D), (HEADS * HEAD_DIM) ** -0.5, 0.109375, ((0, 8), (1, 16)))
    norm_gain = jnp.clip(1.0 + 0.18 * jax.random.normal(streams_of[5], (D,), jnp.float32), 0.099609375, 1.8984375).astype(jnp.bfloat16)
    router = normal_values(streams_of[6], (D, EXPERTS), D ** -0.5, 0.078125)
    expert_ids_keys = jax.random.split(jax.random.fold_in(streams_of[7], 1), TOKENS // TOK_DEV)
    expert_ids_turns = jax.random.permutation(jax.random.fold_in(streams_of[7], 3), TOKENS // TOK_DEV)
    expert_ids = jax.vmap(lambda own, number: assign_block(jax.random.fold_in(streams_of[7], 2), own, number, TOK_DEV, EXPERTS, TOP, CAP, 2))(expert_ids_keys, expert_ids_turns).reshape((TOKENS, TOP))
    u_gate_up = normal_values(streams_of[8], (EXPERTS * PIECES, D // PIECES, 2 * RANK), D ** -0.5, 0.078125, ((0, 16),))
    v_gate_up = normal_values(streams_of[9], (EXPERTS * PIECES, 2, RANK, FF // PIECES), RANK ** -0.5, 0.25, ((0, 16),))
    u_down = normal_values(streams_of[10], (EXPERTS * PIECES, FF // PIECES, RANK), FF ** -0.5, 0.0625, ((0, 16),))
    v_down = normal_values(streams_of[11], (EXPERTS * PIECES, RANK, D // PIECES), RANK ** -0.5, 0.25, ((0, 16),))
    return {"queries": queries, "keys": keys, "values": values, "residual": residual, "proj_weight": proj_weight, "norm_gain": norm_gain, "router": router, "expert_ids": expert_ids, "u_gate_up": u_gate_up, "v_gate_up": v_gate_up, "u_down": u_down, "v_down": v_down}


EPS = 1e-05

def causal_attention(queries, keys, values):
    tile_rows = min(1024, TOKENS)
    tile_count = TOKENS // tile_rows
    per_kv = HEADS // KV_HEADS
    query_tiles = queries.reshape(tile_count, tile_rows, KV_HEADS, per_kv, HEAD_DIM)
    key_tiles = keys.reshape(tile_count, tile_rows, KV_HEADS, HEAD_DIM)
    value_tiles = values.reshape(tile_count, tile_rows, KV_HEADS, HEAD_DIM)
    score_scale = HEAD_DIM ** (-0.5)
    offsets = jnp.arange(tile_rows, dtype=jnp.int32)

    def one_tile(tile_index):
        query_block = lax.dynamic_index_in_dim(query_tiles, tile_index, 0, keepdims=False).astype(jnp.float32)
        query_pos = tile_index * tile_rows + offsets

        def scores_of(key_index):
            key_block = lax.dynamic_index_in_dim(key_tiles, key_index, 0, keepdims=False).astype(jnp.float32)
            scores = jnp.einsum('qhjd,khd->hjqk', query_block, key_block) * score_scale
            key_pos = key_index * tile_rows + offsets
            allowed = key_pos[None, :] <= query_pos[:, None]
            return jnp.where(allowed[None, None], scores, -jnp.inf)

        def max_step(key_index, row_max):
            return jnp.maximum(row_max, lax.optimization_barrier(jnp.max(scores_of(key_index), axis=-1)))
        start_max = jnp.full((KV_HEADS, per_kv, tile_rows), -jnp.inf, jnp.float32)
        row_max = lax.fori_loop(jnp.int32(0), tile_index + 1, max_step, start_max)

        def sum_step(key_index, carried):
            row_sum, weighted = carried
            exp_terms = jnp.exp(scores_of(key_index) - row_max[..., None])
            rounded = lax.optimization_barrier(exp_terms.astype(jnp.bfloat16)).astype(jnp.float32)
            value_block = lax.dynamic_index_in_dim(value_tiles, key_index, 0, keepdims=False).astype(jnp.float32)
            row_sum = row_sum + lax.optimization_barrier(jnp.sum(exp_terms, axis=-1))
            weighted = weighted + jnp.einsum('hjqk,khd->hjqd', rounded, value_block)
            return (row_sum, weighted)
        start_sum = jnp.zeros((KV_HEADS, per_kv, tile_rows), jnp.float32)
        start_acc = jnp.zeros((KV_HEADS, per_kv, tile_rows, HEAD_DIM), jnp.float32)
        row_sum, weighted = lax.fori_loop(jnp.int32(0), tile_index + 1, sum_step, (start_sum, start_acc))
        result = weighted / row_sum[..., None]
        return jnp.transpose(result, (2, 0, 1, 3)).reshape(tile_rows, HEADS * HEAD_DIM)
    outputs = lax.map(one_tile, jnp.arange(tile_count, dtype=jnp.int32))
    return outputs.reshape(TOKENS, HEADS * HEAD_DIM).astype(jnp.bfloat16)

def expert_stack(u_gate_up, v_gate_up, u_down, v_down):
    first_in = u_gate_up.reshape(EXPERTS, D, 2 * RANK)
    second_in = jnp.transpose(v_gate_up.reshape(EXPERTS, PIECES, 2, RANK, FF // PIECES), (0, 2, 3, 1, 4))
    second_in = second_in.reshape(EXPERTS, 2, RANK, FF)
    first_out = u_down.reshape(EXPERTS, FF, RANK)
    second_out = jnp.transpose(v_down.reshape(EXPERTS, PIECES, RANK, D // PIECES), (0, 2, 1, 3))
    second_out = second_out.reshape(EXPERTS, RANK, D)
    return (first_in, second_in, first_out, second_out)

def reference(queries, keys, values, residual, proj_weight, norm_gain, router, expert_ids, u_gate_up, v_gate_up, u_down, v_down):
    attended = causal_attention(queries, keys, values)
    attn_update = jnp.dot(attended, proj_weight, preferred_element_type=jnp.float32).astype(jnp.bfloat16)
    stream = residual.astype(jnp.float32) + attn_update.astype(jnp.float32)
    mean_sq = lax.optimization_barrier(jnp.mean(stream * stream, axis=-1, keepdims=True))
    normed = (stream * lax.rsqrt(mean_sq + EPS) * norm_gain.astype(jnp.float32)).astype(jnp.bfloat16)
    logits = jnp.dot(normed, router, preferred_element_type=jnp.float32)
    expert_range = jnp.arange(EXPERTS, dtype=jnp.int32)
    picked = (expert_ids[:, :, None] == expert_range[None, None, :]).astype(jnp.float32)
    chosen = lax.optimization_barrier(jnp.sum(picked * logits[:, None, :], axis=-1))
    mix_first = jax.nn.sigmoid(chosen[:, 0] - chosen[:, 1])
    mix_second = jax.nn.sigmoid(chosen[:, 1] - chosen[:, 0])
    mix_weight = jnp.stack([mix_first, mix_second], axis=1)
    block_count = TOKENS // TOK_DEV
    normed_blocks = normed.reshape(block_count, TOK_DEV, D).astype(jnp.float32)
    ids_blocks = expert_ids.reshape(block_count, TOK_DEV * 2)
    weight_blocks = mix_weight.reshape(block_count, TOK_DEV, 2)
    slot_range = jnp.arange(CAP, dtype=jnp.int32)
    first_in, second_in, first_out, second_out = expert_stack(u_gate_up, v_gate_up, u_down, v_down)

    def one_expert(carried, expert_index):
        member = (ids_blocks == expert_index).astype(jnp.int32)
        slot_of = jnp.cumsum(member, axis=1) - 1
        placed = (member[..., None] * (slot_of[..., None] == slot_range).astype(jnp.int32)).astype(jnp.float32)
        placed_tok = placed.reshape(block_count, TOK_DEV, 2, CAP)
        select = lax.optimization_barrier(jnp.sum(placed_tok, axis=2))
        rows_in = jnp.einsum('btc,btd->bcd', select, normed_blocks).astype(jnp.bfloat16)
        rows_in = rows_in.reshape(block_count * CAP, D)
        w_first = lax.dynamic_index_in_dim(first_in, expert_index, 0, keepdims=False)
        w_middle = lax.dynamic_index_in_dim(second_in, expert_index, 0, keepdims=False)
        w_down = lax.dynamic_index_in_dim(first_out, expert_index, 0, keepdims=False)
        w_last = lax.dynamic_index_in_dim(second_out, expert_index, 0, keepdims=False)
        rank_in = jnp.dot(rows_in, w_first, preferred_element_type=jnp.float32).astype(jnp.bfloat16)
        gate_part = jnp.dot(rank_in[:, :RANK], w_middle[0], preferred_element_type=jnp.float32)
        up_part = jnp.dot(rank_in[:, RANK:], w_middle[1], preferred_element_type=jnp.float32)
        hidden = (jax.nn.silu(gate_part) * up_part).astype(jnp.bfloat16)
        rank_down = jnp.dot(hidden, w_down, preferred_element_type=jnp.float32).astype(jnp.bfloat16)
        out_rows = jnp.dot(rank_down, w_last, preferred_element_type=jnp.float32).astype(jnp.bfloat16)
        back_rows = out_rows.astype(jnp.float32).reshape(block_count, CAP, D)
        weights_tok = jnp.einsum('btsc,bts->btc', placed_tok, weight_blocks)
        carried = carried + jnp.einsum('btc,bcd->btd', weights_tok, back_rows)
        return (carried, None)
    start_mix = jnp.zeros((block_count, TOK_DEV, D), jnp.float32)
    mixture, unused = lax.scan(one_expert, start_mix, jnp.arange(EXPERTS, dtype=jnp.int32))
    return (stream + mixture.reshape(TOKENS, D)).astype(jnp.bfloat16)
```

```python
import functools

import jax
import jax.numpy as jnp
from jax import lax
from jax.experimental import pallas as pl
from jax.experimental.pallas import tpu as pltpu
from jax.sharding import Mesh
from jax.sharding import PartitionSpec as P

D = 6144
HEAD_DIM = 128
GROUP_HEADS = 3
GROUP_WIDTH = GROUP_HEADS * HEAD_DIM
EXPERTS = 8
RANK = 512
FF_PIECE = 4096
TOK_DEV = 128
HALF = D // 2
BLOCKS = 8
BLOCK_WIDTH = HALF // BLOCKS
SLOTS = 32
EPS = 1e-05
SCALE = HEAD_DIM**-0.5 * 1.4426950408889634
LOW = -1e30
Q_ROWS = 512
Q_TILE = 256
KEY_PART = 256

Z = ("zh", "zl")
PLANE = ("zh", "x", "zl")
GROUP = ("y", "c")
EXP = ("zl", "y", "c")


VMEM = pl.BlockSpec(memory_space=pltpu.VMEM)
SMEM = pl.BlockSpec(memory_space=pltpu.SMEM)
ANY = pl.BlockSpec(memory_space=pl.ANY)


def params(mib=48, **more):
    return pltpu.CompilerParams(vmem_limit_bytes=mib << 20, **more)


def cost(flops, moved, transcendentals=0):
    return pl.CostEstimate(flops=flops, bytes_accessed=moved, transcendentals=transcendentals)


def shifted(value, axis, step):
    return lax.ppermute(value, axis, [(i, (i + step) % 4) for i in range(4)])


def other_core(value):
    return lax.ppermute(value, "c", [(0, 1), (1, 0)])


def mirrored(value):
    return lax.ppermute(value, PLANE, [(i, 15 - i) for i in range(16)])


def ring_pieces(value, axis):
    half = value.shape[0] // 2
    up = shifted(value, axis, 1)
    down = shifted(value, axis, -1)
    far_up = shifted(up[:half], axis, 1)
    far_down = shifted(down[half:], axis, -1)
    return [value, up, down, far_up, far_down]


def relative(mine, theirs):
    gap = (mine - theirs) % 4
    return jnp.where(gap == 3, 2, jnp.where(gap == 2, 3, gap))


def attention_kernel(items, kpos_ref, q_ref, *refs):
    pieces = refs[:20]
    out_ref = refs[20]
    kv_ref, max_ref, acc_ref, sems = refs[21:]
    copies = []
    for which in range(4):
        for number in range(5):
            source = pieces[which * 5 + number]
            if number < 3:
                target = kv_ref.at[which, pl.ds(number * 4, 4)]
            else:
                target = kv_ref.at[which, pl.ds(12 + (number - 3) * 2, 2)]
            copies.append(pltpu.make_async_copy(source, target, sems.at[which * 5 + number]))
    for copy in copies:
        copy.start()
    max_ref[...] = jnp.full(max_ref.shape, LOW, jnp.float32)
    acc_ref[...] = jnp.zeros(acc_ref.shape, jnp.float32)
    for copy in copies:
        copy.wait()

    def work(slot, at, masked):
        keys, values = [], []
        ones = jnp.ones((KEY_PART, HEAD_DIM), jnp.bfloat16)
        for which in range(4):
            block = at[which % 2]
            keys.append(kv_ref[which, block, :, 0:HEAD_DIM])
            value = kv_ref[which, block, :, HEAD_DIM : 2 * HEAD_DIM]
            values.append(jnp.concatenate([value, ones], axis=1))
        for tile in range(Q_ROWS // Q_TILE):
            rows = pl.ds(tile * Q_TILE, Q_TILE)
            for head in range(GROUP_HEADS):
                query = q_ref[slot, rows, head * HEAD_DIM : (head + 1) * HEAD_DIM]
                scores = []
                for which in range(4):
                    part = lax.dot_general(
                        query,
                        keys[which],
                        (((1,), (1,)), ((), ())),
                        preferred_element_type=jnp.float32,
                    )
                    if masked:
                        row_pos = (
                            slot * Q_ROWS
                            + tile * Q_TILE
                            + lax.broadcasted_iota(jnp.int32, (Q_TILE, KEY_PART), 0)
                        )
                        part = jnp.where(kpos_ref[which : which + 1, :] <= row_pos, part, LOW)
                    scores.append(part)
                highest = jnp.maximum(
                    jnp.maximum(scores[0], scores[1]), jnp.maximum(scores[2], scores[3])
                )
                old_max = max_ref[slot, head, rows, :]
                new_max = jnp.maximum(old_max, jnp.max(highest, axis=1, keepdims=True))
                level = jnp.tile(new_max * SCALE, (1, KEY_PART // HEAD_DIM))
                update = None
                for which in range(4):
                    weights = jnp.exp2(scores[which] * SCALE - level).astype(jnp.bfloat16)
                    term = jnp.dot(weights, values[which], preferred_element_type=jnp.float32)
                    update = term if update is None else update + term
                fading = jnp.exp2((old_max - new_max) * SCALE)
                max_ref[slot, head, rows, :] = new_max
                acc_ref[slot, head, rows, 0:HEAD_DIM] = (
                    acc_ref[slot, head, rows, 0:HEAD_DIM] * fading + update[:, :HEAD_DIM]
                )
                acc_ref[slot, head, rows, HEAD_DIM:] = (
                    acc_ref[slot, head, rows, HEAD_DIM:] * fading + update[:, HEAD_DIM:]
                )

    open_count = items[0]
    masked_count = items[1]

    def open_step(number, carry):
        at = 2 + 3 * number
        work(items[at], (items[at + 1], items[at + 2]), False)
        return carry

    def masked_step(number, carry):
        at = 2 + 3 * (open_count + number)
        work(items[at], (items[at + 1], items[at + 2]), True)
        return carry

    lax.fori_loop(0, open_count, open_step, 0)
    lax.fori_loop(0, masked_count, masked_step, 0)
    for slot in range(2):
        for head in range(GROUP_HEADS):
            out_ref[slot, :, head * HEAD_DIM : (head + 1) * HEAD_DIM] = (
                acc_ref[slot, head, :, 0:HEAD_DIM] / acc_ref[slot, head, :, HEAD_DIM:]
            ).astype(jnp.bfloat16)


def attention(items, kpos, query_pair, pieces):
    shaped = [p.reshape(-1, KEY_PART, 2 * HEAD_DIM) for p in pieces]
    return pl.pallas_call(
        attention_kernel,
        out_shape=jax.ShapeDtypeStruct((2, Q_ROWS, GROUP_WIDTH), jnp.bfloat16),
        in_specs=[SMEM, VMEM, VMEM] + [ANY] * 20,
        out_specs=VMEM,
        scratch_shapes=[
            pltpu.VMEM((4, 16, KEY_PART, 2 * HEAD_DIM), jnp.bfloat16),
            pltpu.VMEM((2, GROUP_HEADS, Q_ROWS, HEAD_DIM), jnp.float32),
            pltpu.VMEM((2, GROUP_HEADS, Q_ROWS, 2 * HEAD_DIM), jnp.float32),
            pltpu.SemaphoreType.DMA((20,)),
        ],
        compiler_params=params(40),
        cost_estimate=cost(27_000_000_000, 10_000_000, 26_000_000),
        name="attention",
    )(items, kpos, query_pair, *shaped)


def projection_kernel(groups, w_ref, *refs):
    pieces = refs[:10]
    out_ref = refs[10]
    for half in range(2):
        total = [None, None]
        for core in range(2):
            for number in range(4):
                if number < 3:
                    rows = pieces[core * 5 + number][half * 512 : (half + 1) * 512, :]
                else:
                    rows = pieces[core * 5 + 3 + half][...]
                group = groups[core * 4 + number]
                for side in range(2):
                    term = jnp.dot(rows, w_ref[group, side], preferred_element_type=jnp.float32)
                    total[side] = term if total[side] is None else total[side] + term
        for side in range(2):
            done = total[side].astype(jnp.bfloat16).reshape(4, TOK_DEV, GROUP_WIDTH)
            out_ref[half * 4 : (half + 1) * 4, :, side * GROUP_WIDTH : (side + 1) * GROUP_WIDTH] = done


def projection(groups, weights, pieces):
    return pl.pallas_call(
        projection_kernel,
        out_shape=jax.ShapeDtypeStruct((8, TOK_DEV, 2 * GROUP_WIDTH), jnp.bfloat16),
        in_specs=[SMEM] + [VMEM] * 11,
        out_specs=VMEM,
        compiler_params=params(48),
        cost_estimate=cost(4_900_000_000, 13_000_000),
        name="projection",
    )(groups, weights, *pieces)


def slot_tables(ids_t):
    expert = lax.broadcasted_iota(jnp.int32, (EXPERTS, TOK_DEV), 0)
    first = (expert == ids_t[0:1, :]).astype(jnp.float32)
    second = (expert == ids_t[1:2, :]).astype(jnp.float32)
    member = first + second
    before = (
        lax.broadcasted_iota(jnp.int32, (TOK_DEV, TOK_DEV), 0)
        < lax.broadcasted_iota(jnp.int32, (TOK_DEV, TOK_DEV), 1)
    ).astype(jnp.bfloat16)
    slot = jnp.dot(member.astype(jnp.bfloat16), before, preferred_element_type=jnp.float32)
    return first, second, member, slot


def dispatch_kernel(ids_ref, update_ref, residual_ref, gain_ref, router_ref, send_ref, mix_ref, normed_ref):
    squares = jnp.zeros((TOK_DEV, 1), jnp.float32)
    for half in range(2):
        for group in range(BLOCKS):
            at = half * HALF + group * BLOCK_WIDTH
            row = residual_ref[:, at : at + BLOCK_WIDTH].astype(jnp.float32) + update_ref[
                group, :, half * BLOCK_WIDTH : (half + 1) * BLOCK_WIDTH
            ].astype(jnp.float32)
            squares = squares + jnp.sum(row * row, axis=1, keepdims=True)
    factor = lax.rsqrt(squares / D + EPS)
    for half in range(2):
        for group in range(BLOCKS):
            at = half * HALF + group * BLOCK_WIDTH
            row = residual_ref[:, at : at + BLOCK_WIDTH].astype(jnp.float32) + update_ref[
                group, :, half * BLOCK_WIDTH : (half + 1) * BLOCK_WIDTH
            ].astype(jnp.float32)
            gain = gain_ref[:, at : at + BLOCK_WIDTH].astype(jnp.float32)
            normed_ref[:, at : at + BLOCK_WIDTH] = (row * factor * gain).astype(jnp.bfloat16)
    first, second, member, slot = slot_tables(ids_ref[...])
    slot_ids = lax.broadcasted_iota(jnp.int32, (SLOTS, TOK_DEV), 0).astype(jnp.float32)
    picks, tails = [], []
    last = jnp.where(slot == float(SLOTS), member, 0.0)
    for expert in range(EXPERTS):
        picks.append(
            jnp.where(slot[expert : expert + 1, :] == slot_ids, member[expert : expert + 1, :], 0.0)
        )
        tails.append(jnp.broadcast_to(last[expert : expert + 1, :], (BLOCKS, TOK_DEV)))
    pick = jnp.concatenate(picks, axis=0)
    tail = jnp.concatenate(tails, axis=0)
    tail_block = lax.broadcasted_iota(jnp.int32, (EXPERTS * BLOCKS, TOK_DEV), 0) % BLOCKS
    pick_low = pick.astype(jnp.bfloat16)
    for half in range(2):
        tail_rows = None
        for block in range(BLOCKS):
            at = half * HALF + block * BLOCK_WIDTH
            rows = normed_ref[:, at : at + BLOCK_WIDTH]
            moved = jnp.dot(pick_low, rows, preferred_element_type=jnp.float32).astype(jnp.bfloat16)
            for expert in range(EXPERTS):
                send_ref[2 * expert + half, block * SLOTS : (block + 1) * SLOTS, :] = moved[
                    expert * SLOTS : (expert + 1) * SLOTS, :
                ]
            chosen = jnp.where(tail_block == block, tail, 0.0).astype(jnp.bfloat16)
            term = jnp.dot(chosen, rows, preferred_element_type=jnp.float32)
            tail_rows = term if tail_rows is None else tail_rows + term
        tail_rows = tail_rows.astype(jnp.bfloat16)
        for expert in range(EXPERTS):
            send_ref[2 * expert + half, BLOCKS * SLOTS :, :] = tail_rows[
                expert * BLOCKS : (expert + 1) * BLOCKS, :
            ]
    logits = lax.dot_general(
        router_ref[...],
        normed_ref[...],
        (((1,), (1,)), ((), ())),
        preferred_element_type=jnp.float32,
    )
    chosen_first = jnp.sum(first * logits, axis=0, keepdims=True)
    chosen_second = jnp.sum(second * logits, axis=0, keepdims=True)
    mix_first = 1.0 / (1.0 + jnp.exp(chosen_second - chosen_first))
    mix_second = 1.0 / (1.0 + jnp.exp(chosen_first - chosen_second))
    share = first * mix_first + second * mix_second
    for expert in range(EXPERTS):
        mine = share[expert : expert + 1, :]
        mix_ref[expert * SLOTS : (expert + 1) * SLOTS, :] = picks[expert] * mine
        mix_ref[
            EXPERTS * SLOTS + expert * BLOCKS : EXPERTS * SLOTS + (expert + 1) * BLOCKS, :
        ] = tails[expert] * mine


def dispatch(ids_t, update, residual, gain, router_t):
    return pl.pallas_call(
        dispatch_kernel,
        out_shape=(
            jax.ShapeDtypeStruct((16, BLOCKS * (SLOTS + 1), BLOCK_WIDTH), jnp.bfloat16),
            jax.ShapeDtypeStruct((EXPERTS * (SLOTS + BLOCKS), TOK_DEV), jnp.float32),
        ),
        in_specs=[VMEM] * 5,
        out_specs=(VMEM, VMEM),
        scratch_shapes=[pltpu.VMEM((TOK_DEV, D), jnp.bfloat16)],
        compiler_params=params(32),
        cost_estimate=cost(800_000_000, 8_000_000),
        name="dispatch",
    )(ids_t, update, residual, gain, router_t)


ROWS = 16 * SLOTS
ALL_ROWS = ROWS + 16


def row_pick(block):
    source = lax.broadcasted_iota(jnp.int32, (16, 16 * BLOCKS), 0)
    place = lax.broadcasted_iota(jnp.int32, (16, 16 * BLOCKS), 1)
    return (place == source * BLOCKS + block).astype(jnp.bfloat16)


def first_kernel(rows_ref, tail_ref, u_ref, out_ref, low_ref):
    step = pl.program_id(0)
    rows = rows_ref[...].reshape(ROWS, BLOCK_WIDTH)
    tail = tail_ref[...].reshape(16 * BLOCKS, BLOCK_WIDTH)
    tail = jnp.dot(row_pick(step), tail, preferred_element_type=jnp.float32).astype(jnp.bfloat16)
    main = jnp.dot(rows, u_ref[0], preferred_element_type=jnp.float32)
    extra = jnp.dot(tail, u_ref[0], preferred_element_type=jnp.float32)

    @pl.when(step == 0)
    def _():
        out_ref[:ROWS, :] = main
        out_ref[ROWS:, :] = extra

    @pl.when(step > 0)
    def _():
        out_ref[:ROWS, :] += main
        out_ref[ROWS:, :] += extra

    @pl.when(step == BLOCKS - 1)
    def _():
        low_ref[...] = out_ref[...].astype(jnp.bfloat16)


def first_factor(received, u_gate_up):
    return pl.pallas_call(
        first_kernel,
        grid=(BLOCKS,),
        out_shape=(
            jax.ShapeDtypeStruct((ALL_ROWS, 2 * RANK), jnp.float32),
            jax.ShapeDtypeStruct((ALL_ROWS, 2 * RANK), jnp.bfloat16),
        ),
        in_specs=[
            pl.BlockSpec((16, SLOTS, BLOCK_WIDTH), lambda b: (0, b, 0)),
            pl.BlockSpec((16, BLOCKS, BLOCK_WIDTH), lambda b: (0, SLOTS, 0)),
            pl.BlockSpec((1, BLOCK_WIDTH, 2 * RANK), lambda b: (0, b, 0)),
        ],
        out_specs=(
            pl.BlockSpec((ALL_ROWS, 2 * RANK), lambda b: (0, 0)),
            pl.BlockSpec((ALL_ROWS, 2 * RANK), lambda b: (0, 0)),
        ),
        compiler_params=params(32, dimension_semantics=("arbitrary",)),
        cost_estimate=cost(3_400_000_000, 12_000_000),
        name="first_factor",
    )(received, received, u_gate_up)


FF_TILE = 512


def middle_kernel(own_ref, got_ref, v_ref, u_ref, out_ref, low_ref, rank_ref):
    step = pl.program_id(0)

    @pl.when(step == 0)
    def _():
        rank_ref[...] = (own_ref[...] + got_ref[...].astype(jnp.float32)).astype(jnp.bfloat16)

    gate = jnp.dot(rank_ref[:, :RANK], v_ref[0, 0], preferred_element_type=jnp.float32)
    up = jnp.dot(rank_ref[:, RANK:], v_ref[0, 1], preferred_element_type=jnp.float32)
    hidden = (gate / (1.0 + jnp.exp(-gate)) * up).astype(jnp.bfloat16)
    term = jnp.dot(hidden, u_ref[0], preferred_element_type=jnp.float32)

    @pl.when(step == 0)
    def _():
        out_ref[...] = term

    @pl.when(step > 0)
    def _():
        out_ref[...] += term

    @pl.when(step == FF_PIECE // FF_TILE - 1)
    def _():
        low_ref[...] = out_ref[...].astype(jnp.bfloat16)


def middle(own, got, v_gate_up, u_down):
    return pl.pallas_call(
        middle_kernel,
        grid=(FF_PIECE // FF_TILE,),
        out_shape=(
            jax.ShapeDtypeStruct((ALL_ROWS, RANK), jnp.float32),
            jax.ShapeDtypeStruct((ALL_ROWS, RANK), jnp.bfloat16),
        ),
        in_specs=[
            pl.BlockSpec((ALL_ROWS, 2 * RANK), lambda f: (0, 0)),
            pl.BlockSpec((ALL_ROWS, 2 * RANK), lambda f: (0, 0)),
            pl.BlockSpec((1, 2, RANK, FF_TILE), lambda f: (0, 0, 0, f)),
            pl.BlockSpec((1, FF_TILE, RANK), lambda f: (0, f, 0)),
        ],
        out_specs=(
            pl.BlockSpec((ALL_ROWS, RANK), lambda f: (0, 0)),
            pl.BlockSpec((ALL_ROWS, RANK), lambda f: (0, 0)),
        ),
        scratch_shapes=[pltpu.VMEM((ALL_ROWS, 2 * RANK), jnp.bfloat16)],
        compiler_params=params(32, dimension_semantics=("arbitrary",)),
        cost_estimate=cost(6_700_000_000, 16_000_000, 2_200_000),
        name="middle",
    )(own, got, v_gate_up, u_down)


def last_kernel(own_ref, got_ref, v_ref, out_ref, down_ref):
    step = pl.program_id(0)

    @pl.when(step == 0)
    def _():
        down_ref[...] = (own_ref[...] + got_ref[...].astype(jnp.float32)).astype(jnp.bfloat16)

    for block in range(BLOCKS):
        weights = v_ref[0, :, block * BLOCK_WIDTH : (block + 1) * BLOCK_WIDTH]
        result = jnp.dot(down_ref[:ROWS, :], weights, preferred_element_type=jnp.float32)
        result = result.astype(jnp.bfloat16).reshape(16, SLOTS, BLOCK_WIDTH)
        out_ref[:, block * SLOTS : (block + 1) * SLOTS, :] = result
    total = None
    place = lax.broadcasted_iota(jnp.int32, (16 * BLOCKS, 16), 0)
    source = lax.broadcasted_iota(jnp.int32, (16 * BLOCKS, 16), 1)
    for block in range(BLOCKS):
        weights = v_ref[0, :, block * BLOCK_WIDTH : (block + 1) * BLOCK_WIDTH]
        spread = (place == source * BLOCKS + block).astype(jnp.bfloat16)
        lifted = jnp.dot(spread, down_ref[ROWS:, :], preferred_element_type=jnp.float32)
        term = jnp.dot(lifted.astype(jnp.bfloat16), weights, preferred_element_type=jnp.float32)
        total = term if total is None else total + term
    out_ref[:, BLOCKS * SLOTS :, :] = total.astype(jnp.bfloat16).reshape(16, BLOCKS, BLOCK_WIDTH)


def last_factor(own, got, v_down):
    return pl.pallas_call(
        last_kernel,
        grid=(1,),
        out_shape=jax.ShapeDtypeStruct((16, BLOCKS * (SLOTS + 1), BLOCK_WIDTH), jnp.bfloat16),
        in_specs=[
            pl.BlockSpec((ALL_ROWS, RANK), lambda b: (0, 0)),
            pl.BlockSpec((ALL_ROWS, RANK), lambda b: (0, 0)),
            pl.BlockSpec((1, RANK, HALF), lambda b: (0, 0, 0)),
        ],
        out_specs=pl.BlockSpec((16, BLOCKS * (SLOTS + 1), BLOCK_WIDTH), lambda b: (0, 0, 0)),
        scratch_shapes=[pltpu.VMEM((ALL_ROWS, RANK), jnp.bfloat16)],
        compiler_params=params(32),
        cost_estimate=cost(1_700_000_000, 8_000_000),
        name="last_factor",
    )(own, got, v_down)


def combine_kernel(mix_ref, update_ref, residual_ref, back_ref, out_ref):
    mix = mix_ref[: EXPERTS * SLOTS, :].T
    tail = mix_ref[EXPERTS * SLOTS :, :].T
    mix_high = mix.astype(jnp.bfloat16)
    mix_low = (mix - mix_high.astype(jnp.float32)).astype(jnp.bfloat16)
    tail_block = lax.broadcasted_iota(jnp.int32, (TOK_DEV, EXPERTS * BLOCKS), 1) % BLOCKS
    for half in range(2):
        tail_rows = jnp.concatenate(
            [back_ref[2 * expert + half, BLOCKS * SLOTS :, :] for expert in range(EXPERTS)], axis=0
        )
        for block in range(BLOCKS):
            rows = jnp.concatenate(
                [
                    back_ref[2 * expert + half, block * SLOTS : (block + 1) * SLOTS, :]
                    for expert in range(EXPERTS)
                ],
                axis=0,
            )
            here = jnp.where(tail_block == block, tail, 0.0)
            here_high = here.astype(jnp.bfloat16)
            here_low = (here - here_high.astype(jnp.float32)).astype(jnp.bfloat16)
            mixture = jnp.dot(mix_high, rows, preferred_element_type=jnp.float32)
            mixture = mixture + jnp.dot(mix_low, rows, preferred_element_type=jnp.float32)
            mixture = mixture + jnp.dot(here_high, tail_rows, preferred_element_type=jnp.float32)
            mixture = mixture + jnp.dot(here_low, tail_rows, preferred_element_type=jnp.float32)
            at = half * HALF + block * BLOCK_WIDTH
            stream = residual_ref[:, at : at + BLOCK_WIDTH].astype(jnp.float32) + update_ref[
                block, :, half * BLOCK_WIDTH : (half + 1) * BLOCK_WIDTH
            ].astype(jnp.float32)
            out_ref[:, at : at + BLOCK_WIDTH] = (stream + mixture).astype(jnp.bfloat16)


def combine(mix, update, residual, back):
    return pl.pallas_call(
        combine_kernel,
        out_shape=jax.ShapeDtypeStruct((TOK_DEV, D), jnp.bfloat16),
        in_specs=[VMEM] * 4,
        out_specs=VMEM,
        compiler_params=params(32),
        cost_estimate=cost(1_000_000_000, 8_000_000),
        name="combine",
    )(mix, update, residual, back)


def per_device(
    queries,
    keys,
    values,
    residual,
    proj_weight,
    norm_gain,
    router,
    expert_ids,
    u_gate_up,
    v_gate_up,
    u_down,
    v_down,
):
    zh, x, zl = lax.axis_index("zh"), lax.axis_index("x"), lax.axis_index("zl")
    y, c = lax.axis_index("y"), lax.axis_index("c")
    z = zh * 2 + zl
    chunk = zh * 8 + x * 2 + zl

    kv = jnp.concatenate(
        [keys.reshape(TOK_DEV, 4, HEAD_DIM), values.reshape(TOK_DEV, 4, HEAD_DIM)], axis=2
    )
    kv = jnp.transpose(kv, (1, 0, 2))
    kv = lax.all_to_all(kv, "y", split_axis=0, concat_axis=0, tiled=True)
    kv = kv.reshape(4 * TOK_DEV, 2 * HEAD_DIM)
    early, late = kv[:256], kv[256:]

    def joined(pieces):
        return jnp.concatenate(pieces, axis=0)

    early_pieces = ring_pieces(joined(ring_pieces(early, Z)), "x")
    late_pieces = ring_pieces(joined(ring_pieces(late, "x")), Z)
    own = early_pieces + late_pieces
    swapped = [other_core(p) for p in own]

    q = jnp.transpose(queries.reshape(TOK_DEV, 8, GROUP_WIDTH), (1, 0, 2))
    q = lax.all_to_all(q, GROUP, split_axis=0, concat_axis=0, tiled=True)
    q = q.reshape(2, Q_ROWS, GROUP_WIDTH)
    query_pair = jnp.stack([q[0], mirrored(q[1])])

    numbers = jnp.arange(16, dtype=jnp.int32)
    far_chunk = 15 - chunk
    order = jnp.arange(17, dtype=jnp.int32)
    order = order[:15]
    is_far = order >= chunk
    slot_list = jnp.concatenate([is_far.astype(jnp.int32), jnp.array([0, 1], jnp.int32)])
    chunk_list = jnp.concatenate(
        [jnp.where(is_far, order - chunk, order), jnp.stack([chunk, far_chunk])]
    )
    there_z = chunk_list // 8 * 2 + chunk_list % 2
    there_x = chunk_list // 2 % 4
    rel_z = relative(z, there_z)
    rel_x = relative(x, there_x)
    rows = jnp.stack([slot_list, rel_x * 4 + rel_z, rel_z * 4 + rel_x], axis=1)
    items = jnp.concatenate([jnp.array([15, 2], jnp.int32), rows.reshape(-1)]).astype(jnp.int32)
    key_ids = jnp.arange(KEY_PART, dtype=jnp.int32)
    base = key_ids // TOK_DEV * 256 + key_ids % TOK_DEV
    kpos = jnp.stack(
        [
            base + c * TOK_DEV,
            base + c * TOK_DEV + 512,
            base + (1 - c) * TOK_DEV,
            base + (1 - c) * TOK_DEV + 512,
        ]
    ).astype(jnp.int32)

    attended = attention(items, kpos, query_pair, own + swapped)
    attended = jnp.concatenate([attended[0], mirrored(attended[1])], axis=0)

    weight_rows = lax.all_gather(proj_weight, PLANE, axis=0, tiled=True)
    weight_rows = weight_rows.reshape(8, 2, GROUP_WIDTH, GROUP_WIDTH)
    pieces = ring_pieces(attended, "y")
    pieces = pieces + [other_core(p) for p in pieces]
    from_y = jnp.stack([y, (y - 1) % 4, (y + 1) % 4, (y + 2) % 4])
    groups = jnp.concatenate([from_y * 2 + c, from_y * 2 + 1 - c]).astype(jnp.int32)
    projected = projection(groups, weight_rows, pieces)
    update = lax.all_to_all(projected, GROUP, split_axis=0, concat_axis=0, tiled=True)

    ids_t = expert_ids.T
    send, mix = dispatch(ids_t, update, residual, norm_gain.reshape(1, D), router.T)
    received = lax.all_to_all(send, EXP, split_axis=0, concat_axis=0, tiled=True)
    rank_own, rank_low = first_factor(received, u_gate_up)
    down_own, down_low = middle(rank_own, other_core(rank_low), v_gate_up, u_down)
    out_rows = last_factor(down_own, other_core(down_low), v_down)
    back = lax.all_to_all(out_rows, EXP, split_axis=0, concat_axis=0, tiled=True)
    return combine(mix, update, residual, back)


def solution(mesh):
    fine = Mesh(mesh.devices.reshape(2, 4, 2, 4, 2), ("zh", "x", "zl", "y", "c"))
    seq, exp = ("zh", "x"), ("zl", "y", "c")
    in_specs = (
        P(seq + exp, None),
        P(seq + exp, None),
        P(seq + exp, None),
        P(seq + exp, None),
        P(seq, exp),
        P(),
        P(),
        P(seq + exp, None),
        P(exp, None, None),
        P(exp, None, None, None),
        P(exp, None, None),
        P(exp, None, None),
    )
    return jax.shard_map(
        per_device, mesh=fine, in_specs=in_specs, out_specs=P(seq + exp, None), check_vma=False
    )
```

```python
import functools

import jax
import jax.numpy as jnp
from jax import lax
from jax.experimental import pallas as pl
from jax.experimental.pallas import tpu as pltpu
from jax.sharding import Mesh
from jax.sharding import PartitionSpec as P


D = 6144
HEAD_DIM = 128
GROUP_HEADS = 3
GROUP_WIDTH = GROUP_HEADS * HEAD_DIM
EXPERTS = 8
RANK = 512
FF_PIECE = 4096
TOK_DEV = 128
HALF = D // 2
BLOCKS = 8
BLOCK_WIDTH = HALF // BLOCKS
SLOTS = 32
PART = 16
EPS = 1e-05
SCALE = HEAD_DIM**-0.5 * 1.4426950408889634
LOW = -1e30
Q_ROWS = 512
Q_TILE = 256
KEY_PART = 256

Z = ("zh", "zl")
PLANE = ("zh", "x", "zl")
GROUP = ("y", "c")
EXP = ("zl", "y", "c")


VMEM = pl.BlockSpec(memory_space=pltpu.VMEM)
SMEM = pl.BlockSpec(memory_space=pltpu.SMEM)
ANY = pl.BlockSpec(memory_space=pl.ANY)
HBM = pl.BlockSpec(memory_space=pltpu.HBM)


def params(mib=48, **more):
    return pltpu.CompilerParams(vmem_limit_bytes=mib << 20, **more)


def cost(flops, moved, transcendentals=0):
    return pl.CostEstimate(flops=flops, bytes_accessed=moved, transcendentals=transcendentals)


def shifted(value, axis, step):
    return lax.ppermute(value, axis, [(i, (i + step) % 4) for i in range(4)])


def other_core(value):
    return lax.ppermute(value, "c", [(0, 1), (1, 0)])


def mirrored(value):
    return lax.ppermute(value, PLANE, [(i, 15 - i) for i in range(16)])


def ring_pieces(value, axis):
    half = value.shape[0] // 2
    up = shifted(value, axis, 1)
    down = shifted(value, axis, -1)
    far_up = shifted(up[:half], axis, 1)
    far_down = shifted(down[half:], axis, -1)
    return [value, up, down, far_up, far_down]


def relative(mine, theirs):
    gap = (mine - theirs) % 4
    return jnp.where(gap == 3, 2, jnp.where(gap == 2, 3, gap))


def attention_kernel(items, kpos_ref, q_ref, *refs):
    pieces = refs[:20]
    out_ref = refs[20]
    kv_ref, max_ref, acc_ref, sems = refs[21:]
    copies = []
    for which in range(4):
        for number in range(5):
            source = pieces[which * 5 + number]
            if number < 3:
                target = kv_ref.at[which, pl.ds(number * 4, 4)]
            else:
                target = kv_ref.at[which, pl.ds(12 + (number - 3) * 2, 2)]
            copies.append(pltpu.make_async_copy(source, target, sems.at[which * 5 + number]))
    for copy in copies:
        copy.start()
    max_ref[...] = jnp.full(max_ref.shape, LOW, jnp.float32)
    acc_ref[...] = jnp.zeros(acc_ref.shape, jnp.float32)
    for copy in copies:
        copy.wait()

    def work(slot, at, masked):
        keys, values = [], []
        ones = jnp.ones((KEY_PART, HEAD_DIM), jnp.bfloat16)
        for which in range(4):
            block = at[which % 2]
            keys.append(kv_ref[which, block, :, 0:HEAD_DIM])
            value = kv_ref[which, block, :, HEAD_DIM : 2 * HEAD_DIM]
            values.append(jnp.concatenate([value, ones], axis=1))
        for tile in range(Q_ROWS // Q_TILE):
            rows = pl.ds(tile * Q_TILE, Q_TILE)
            for head in range(GROUP_HEADS):
                query = q_ref[slot, rows, head * HEAD_DIM : (head + 1) * HEAD_DIM]
                scores = []
                for which in range(4):
                    part = lax.dot_general(
                        query,
                        keys[which],
                        (((1,), (1,)), ((), ())),
                        preferred_element_type=jnp.float32,
                    )
                    if masked:
                        row_pos = (
                            slot * Q_ROWS
                            + tile * Q_TILE
                            + lax.broadcasted_iota(jnp.int32, (Q_TILE, KEY_PART), 0)
                        )
                        part = jnp.where(kpos_ref[which : which + 1, :] <= row_pos, part, LOW)
                    scores.append(part)
                highest = jnp.maximum(
                    jnp.maximum(scores[0], scores[1]), jnp.maximum(scores[2], scores[3])
                )
                old_max = max_ref[slot, head, rows, :]
                new_max = jnp.maximum(old_max, jnp.max(highest, axis=1, keepdims=True))
                level = jnp.tile(new_max * SCALE, (1, KEY_PART // HEAD_DIM))
                update = None
                for which in range(4):
                    weights = jnp.exp2(scores[which] * SCALE - level).astype(jnp.bfloat16)
                    term = jnp.dot(weights, values[which], preferred_element_type=jnp.float32)
                    update = term if update is None else update + term
                fading = jnp.exp2((old_max - new_max) * SCALE)
                max_ref[slot, head, rows, :] = new_max
                acc_ref[slot, head, rows, 0:HEAD_DIM] = (
                    acc_ref[slot, head, rows, 0:HEAD_DIM] * fading + update[:, :HEAD_DIM]
                )
                acc_ref[slot, head, rows, HEAD_DIM:] = (
                    acc_ref[slot, head, rows, HEAD_DIM:] * fading + update[:, HEAD_DIM:]
                )

    open_count = items[0]
    masked_count = items[1]

    def open_step(number, carry):
        at = 2 + 3 * number
        work(items[at], (items[at + 1], items[at + 2]), False)
        return carry

    def masked_step(number, carry):
        at = 2 + 3 * (open_count + number)
        work(items[at], (items[at + 1], items[at + 2]), True)
        return carry

    lax.fori_loop(0, open_count, open_step, 0)
    lax.fori_loop(0, masked_count, masked_step, 0)
    for slot in range(2):
        for head in range(GROUP_HEADS):
            out_ref[slot, :, head * HEAD_DIM : (head + 1) * HEAD_DIM] = (
                acc_ref[slot, head, :, 0:HEAD_DIM] / acc_ref[slot, head, :, HEAD_DIM:]
            ).astype(jnp.bfloat16)


def attention(items, kpos, query_pair, pieces):
    shaped = [p.reshape(-1, KEY_PART, 2 * HEAD_DIM) for p in pieces]
    return pl.pallas_call(
        attention_kernel,
        out_shape=jax.ShapeDtypeStruct((2, Q_ROWS, GROUP_WIDTH), jnp.bfloat16),
        in_specs=[SMEM, VMEM, VMEM] + [ANY] * 20,
        out_specs=VMEM,
        scratch_shapes=[
            pltpu.VMEM((4, 16, KEY_PART, 2 * HEAD_DIM), jnp.bfloat16),
            pltpu.VMEM((2, GROUP_HEADS, Q_ROWS, HEAD_DIM), jnp.float32),
            pltpu.VMEM((2, GROUP_HEADS, Q_ROWS, 2 * HEAD_DIM), jnp.float32),
            pltpu.SemaphoreType.DMA((20,)),
        ],
        compiler_params=params(28),
        cost_estimate=cost(27_000_000_000, 10_000_000, 26_000_000),
        name="attention",
    )(items, kpos, query_pair, *shaped)


def projection_kernel(first, groups, w_ref, *refs):
    pieces = refs[:10]
    out_ref, rows_ref, w_all, done_ref, sems, w_sems, out_sem = refs[-7:]
    copies = []
    for core in range(2):
        for number in range(4):
            at = (core * 4 + number) * GROUP_WIDTH
            for side in range(2):
                copies.append(
                    pltpu.make_async_copy(
                        w_ref.at[groups[core * 4 + number], side],
                        w_all.at[pl.ds(at, GROUP_WIDTH), pl.ds(side * GROUP_WIDTH, GROUP_WIDTH)],
                        w_sems.at[(core * 4 + number) * 2 + side],
                    )
                )
        for number in range(5):
            at = (core * 4 + min(number, 3)) * GROUP_WIDTH
            source = pieces[core * 5 + number]
            low = 256 if number == 4 else 0
            copies.append(
                pltpu.make_async_copy(
                    source,
                    rows_ref.at[pl.ds(low, source.shape[0]), pl.ds(at, GROUP_WIDTH)],
                    sems.at[core * 5 + number],
                )
            )
    for copy in copies:
        copy.start()
    for copy in copies:
        copy.wait()
    for tile in range(Q_ROWS // Q_TILE):
        total = jnp.dot(
            rows_ref[tile * Q_TILE : (tile + 1) * Q_TILE, :],
            w_all[...],
            preferred_element_type=jnp.float32,
        )
        done_ref[tile * 2 : (tile + 1) * 2] = total.astype(jnp.bfloat16).reshape(
            2, TOK_DEV, 2 * GROUP_WIDTH
        )
    out = pltpu.make_async_copy(done_ref, out_ref.at[pl.ds(first, 4)], out_sem)
    out.start()
    out.wait()


def projection(first, groups, weights, pieces, before):
    more = [] if before is None else [before]
    return pl.pallas_call(
        functools.partial(projection_kernel, first),
        out_shape=jax.ShapeDtypeStruct((8, TOK_DEV, 2 * GROUP_WIDTH), jnp.bfloat16),
        in_specs=[SMEM] + [ANY] * (11 + len(more)),
        out_specs=ANY,
        scratch_shapes=[
            pltpu.VMEM((Q_ROWS, 8 * GROUP_WIDTH), jnp.bfloat16),
            pltpu.VMEM((8 * GROUP_WIDTH, 2 * GROUP_WIDTH), jnp.bfloat16),
            pltpu.VMEM((4, TOK_DEV, 2 * GROUP_WIDTH), jnp.bfloat16),
            pltpu.SemaphoreType.DMA((10,)),
            pltpu.SemaphoreType.DMA((16,)),
            pltpu.SemaphoreType.DMA,
        ],
        input_output_aliases={12: 0} if more else {},
        compiler_params=params(16),
        cost_estimate=cost(2_500_000_000, 9_000_000),
        name="projection",
    )(groups, weights, *pieces, *more)


def slot_tables(ids_t):
    expert = lax.broadcasted_iota(jnp.int32, (EXPERTS, TOK_DEV), 0)
    first = (expert == ids_t[0:1, :]).astype(jnp.float32)
    second = (expert == ids_t[1:2, :]).astype(jnp.float32)
    member = first + second
    before = (
        lax.broadcasted_iota(jnp.int32, (TOK_DEV, TOK_DEV), 0)
        < lax.broadcasted_iota(jnp.int32, (TOK_DEV, TOK_DEV), 1)
    ).astype(jnp.bfloat16)
    slot = jnp.dot(member.astype(jnp.bfloat16), before, preferred_element_type=jnp.float32)
    return first, second, member, slot


def dispatch_kernel(ids_ref, update_ref, residual_ref, gain_ref, router_ref, send_a, send_b, mix_ref, normed_ref):
    squares = jnp.zeros((TOK_DEV, 1), jnp.float32)
    for half in range(2):
        for group in range(BLOCKS):
            at = half * HALF + group * BLOCK_WIDTH
            row = residual_ref[:, at : at + BLOCK_WIDTH].astype(jnp.float32) + update_ref[
                group, :, half * BLOCK_WIDTH : (half + 1) * BLOCK_WIDTH
            ].astype(jnp.float32)
            squares = squares + jnp.sum(row * row, axis=1, keepdims=True)
    factor = lax.rsqrt(squares / D + EPS)
    for half in range(2):
        for group in range(BLOCKS):
            at = half * HALF + group * BLOCK_WIDTH
            row = residual_ref[:, at : at + BLOCK_WIDTH].astype(jnp.float32) + update_ref[
                group, :, half * BLOCK_WIDTH : (half + 1) * BLOCK_WIDTH
            ].astype(jnp.float32)
            gain = gain_ref[:, at : at + BLOCK_WIDTH].astype(jnp.float32)
            normed_ref[:, at : at + BLOCK_WIDTH] = (row * factor * gain).astype(jnp.bfloat16)
    first, second, member, slot = slot_tables(ids_ref[...])
    slot_ids = lax.broadcasted_iota(jnp.int32, (SLOTS, TOK_DEV), 0).astype(jnp.float32)
    picks, tails = [], []
    last = jnp.where(slot == float(SLOTS), member, 0.0)
    for expert in range(EXPERTS):
        picks.append(
            jnp.where(slot[expert : expert + 1, :] == slot_ids, member[expert : expert + 1, :], 0.0)
        )
        tails.append(jnp.broadcast_to(last[expert : expert + 1, :], (BLOCKS, TOK_DEV)))
    pick = jnp.concatenate(picks, axis=0)
    tail = jnp.concatenate(tails, axis=0)
    tail_block = lax.broadcasted_iota(jnp.int32, (EXPERTS * BLOCKS, TOK_DEV), 0) % BLOCKS
    pick_low = pick.astype(jnp.bfloat16)
    for half in range(2):
        tail_rows = None
        for block in range(BLOCKS):
            at = half * HALF + block * BLOCK_WIDTH
            rows = normed_ref[:, at : at + BLOCK_WIDTH]
            moved = jnp.dot(pick_low, rows, preferred_element_type=jnp.float32).astype(jnp.bfloat16)
            for expert in range(EXPERTS):
                for part, send in enumerate((send_a, send_b)):
                    low = expert * SLOTS + part * PART
                    send[2 * expert + half, block * PART : (block + 1) * PART, :] = moved[
                        low : low + PART, :
                    ]
            chosen = jnp.where(tail_block == block, tail, 0.0).astype(jnp.bfloat16)
            term = jnp.dot(chosen, rows, preferred_element_type=jnp.float32)
            tail_rows = term if tail_rows is None else tail_rows + term
        tail_rows = tail_rows.astype(jnp.bfloat16)
        for expert in range(EXPERTS):
            send_b[2 * expert + half, BLOCKS * PART :, :] = tail_rows[
                expert * BLOCKS : (expert + 1) * BLOCKS, :
            ]
    logits = lax.dot_general(
        router_ref[...],
        normed_ref[...],
        (((1,), (1,)), ((), ())),
        preferred_element_type=jnp.float32,
    )
    chosen_first = jnp.sum(first * logits, axis=0, keepdims=True)
    chosen_second = jnp.sum(second * logits, axis=0, keepdims=True)
    mix_first = 1.0 / (1.0 + jnp.exp(chosen_second - chosen_first))
    mix_second = 1.0 / (1.0 + jnp.exp(chosen_first - chosen_second))
    share = first * mix_first + second * mix_second
    for expert in range(EXPERTS):
        mine = share[expert : expert + 1, :]
        mix_ref[expert * SLOTS : (expert + 1) * SLOTS, :] = picks[expert] * mine
        mix_ref[
            EXPERTS * SLOTS + expert * BLOCKS : EXPERTS * SLOTS + (expert + 1) * BLOCKS, :
        ] = tails[expert] * mine


def dispatch(ids_t, update, residual, gain, router_t):
    return pl.pallas_call(
        dispatch_kernel,
        out_shape=(
            jax.ShapeDtypeStruct((16, BLOCKS * PART, BLOCK_WIDTH), jnp.bfloat16),
            jax.ShapeDtypeStruct((16, BLOCKS * (PART + 1), BLOCK_WIDTH), jnp.bfloat16),
            jax.ShapeDtypeStruct((EXPERTS * (SLOTS + BLOCKS), TOK_DEV), jnp.float32),
        ),
        in_specs=[VMEM] * 5,
        out_specs=(VMEM, VMEM, VMEM),
        scratch_shapes=[pltpu.VMEM((TOK_DEV, D), jnp.bfloat16)],
        compiler_params=params(32),
        cost_estimate=cost(800_000_000, 8_000_000),
        name="dispatch",
    )(ids_t, update, residual, gain, router_t)


ROWS = 16 * PART


def row_pick(block):
    source = lax.broadcasted_iota(jnp.int32, (16, 16 * BLOCKS), 0)
    place = lax.broadcasted_iota(jnp.int32, (16, 16 * BLOCKS), 1)
    return (place == source * BLOCKS + block).astype(jnp.bfloat16)


def first_kernel(tailed, rows_ref, u_ref, out_ref, low_ref, x_ref, tail_ref, w_ref, sems, row_sems):
    copies = []
    for group in range(GROUPS):
        rows = pl.ds(group * GROUP_DEPTH, GROUP_DEPTH)
        copies.append(pltpu.make_async_copy(u_ref.at[0, rows], w_ref.at[rows], sems.at[group]))
    moves = []
    for block in range(BLOCKS):
        moves.append(
            pltpu.make_async_copy(
                rows_ref.at[:, pl.ds(block * PART, PART), :],
                x_ref.at[pl.ds(0, 16), :, pl.ds(block * BLOCK_WIDTH, BLOCK_WIDTH)],
                row_sems.at[block],
            )
        )
    if tailed:
        moves.append(
            pltpu.make_async_copy(
                rows_ref.at[:, pl.ds(BLOCKS * PART, BLOCKS), :], tail_ref, row_sems.at[BLOCKS]
            )
        )
    for move in moves:
        move.start()
    for copy in copies:
        copy.start()
    for move in moves:
        move.wait()
    if tailed:
        tail = tail_ref[...].reshape(16 * BLOCKS, BLOCK_WIDTH)
        for block in range(BLOCKS):
            picked = jnp.dot(row_pick(block), tail, preferred_element_type=jnp.float32)
            x_ref[16, :, block * BLOCK_WIDTH : (block + 1) * BLOCK_WIDTH] = picked.astype(
                jnp.bfloat16
            )
    count = ROWS + 16 * tailed
    for group in range(GROUPS):
        at = group * GROUP_DEPTH
        copies[group].wait()
        rows = x_ref[0 : count // 16, :, at : at + GROUP_DEPTH].reshape(count, GROUP_DEPTH)
        term = jnp.dot(rows, w_ref[at : at + GROUP_DEPTH, :], preferred_element_type=jnp.float32)
        if group == 0:
            out_ref[...] = term
        elif group < GROUPS - 1:
            out_ref[...] += term
        else:
            total = out_ref[...] + term
            out_ref[...] = total
            low_ref[...] = total.astype(jnp.bfloat16)


GROUPS = 4
GROUP_DEPTH = HALF // GROUPS


def first_factor(received, u_gate_up, tailed):
    count = ROWS + 16 * tailed
    return pl.pallas_call(
        functools.partial(first_kernel, tailed),
        out_shape=(
            jax.ShapeDtypeStruct((count, 2 * RANK), jnp.float32),
            jax.ShapeDtypeStruct((count, 2 * RANK), jnp.bfloat16),
        ),
        in_specs=[ANY, HBM],
        out_specs=(VMEM, VMEM),
        scratch_shapes=[
            pltpu.VMEM((17, 16, HALF), jnp.bfloat16),
            pltpu.VMEM((16, BLOCKS, BLOCK_WIDTH), jnp.bfloat16),
            pltpu.VMEM((HALF, 2 * RANK), jnp.bfloat16),
            pltpu.SemaphoreType.DMA((GROUPS,)),
            pltpu.SemaphoreType.DMA((BLOCKS + 1,)),
        ],
        compiler_params=params(60),
        cost_estimate=cost(1_700_000_000, 9_000_000),
        name="first_factor",
    )(received, u_gate_up)


FF_TILE = 512
FF_STEPS = FF_PIECE // FF_TILE


def middle_kernel(own_ref, got_ref, v_ref, u_ref, out_ref, low_ref, rank_ref, vs_ref, us_ref, sems):
    copies = []
    for step in range(FF_STEPS):
        columns = pl.ds(step * FF_TILE, FF_TILE)
        copies.append(
            (
                pltpu.make_async_copy(
                    v_ref.at[0, :, :, columns], vs_ref.at[:, :, columns], sems.at[2 * step]
                ),
                pltpu.make_async_copy(
                    u_ref.at[0, columns, :], us_ref.at[columns, :], sems.at[2 * step + 1]
                ),
            )
        )
    for pair in copies:
        for copy in pair:
            copy.start()
    rank_ref[...] = (own_ref[...] + got_ref[...].astype(jnp.float32)).astype(jnp.bfloat16)
    for step in range(FF_STEPS):
        columns = slice(step * FF_TILE, (step + 1) * FF_TILE)
        for copy in copies[step]:
            copy.wait()
        gate = jnp.dot(rank_ref[:, :RANK], vs_ref[0, :, columns], preferred_element_type=jnp.float32)
        up = jnp.dot(rank_ref[:, RANK:], vs_ref[1, :, columns], preferred_element_type=jnp.float32)
        hidden = (gate / (1.0 + jnp.exp(-gate)) * up).astype(jnp.bfloat16)
        term = jnp.dot(hidden, us_ref[columns, :], preferred_element_type=jnp.float32)
        if step == 0:
            out_ref[...] = term
        elif step < FF_STEPS - 1:
            out_ref[...] += term
        else:
            total = out_ref[...] + term
            out_ref[...] = total
            low_ref[...] = total.astype(jnp.bfloat16)


def middle(own, got, v_gate_up, u_down):
    count = own.shape[0]
    return pl.pallas_call(
        middle_kernel,
        out_shape=(
            jax.ShapeDtypeStruct((count, RANK), jnp.float32),
            jax.ShapeDtypeStruct((count, RANK), jnp.bfloat16),
        ),
        in_specs=[VMEM, VMEM, HBM, HBM],
        out_specs=(VMEM, VMEM),
        scratch_shapes=[
            pltpu.VMEM((count, 2 * RANK), jnp.bfloat16),
            pltpu.VMEM((2, RANK, FF_PIECE), jnp.bfloat16),
            pltpu.VMEM((FF_PIECE, RANK), jnp.bfloat16),
            pltpu.SemaphoreType.DMA((2 * FF_STEPS,)),
        ],
        compiler_params=params(60),
        cost_estimate=cost(3_400_000_000, 14_000_000, 1_100_000),
        name="middle",
    )(own, got, v_gate_up, u_down)


def last_kernel(tailed, own_ref, got_ref, v_ref, out_ref, down_ref, w_ref, sems):
    copies = []
    for block in range(BLOCKS):
        columns = pl.ds(block * BLOCK_WIDTH, BLOCK_WIDTH)
        copies.append(
            pltpu.make_async_copy(v_ref.at[0, :, columns], w_ref.at[:, columns], sems.at[block])
        )
    for copy in copies:
        copy.start()
    down_ref[...] = (own_ref[...] + got_ref[...].astype(jnp.float32)).astype(jnp.bfloat16)
    total = None
    place = lax.broadcasted_iota(jnp.int32, (16 * BLOCKS, 16), 0)
    source = lax.broadcasted_iota(jnp.int32, (16 * BLOCKS, 16), 1)
    for block in range(BLOCKS):
        copies[block].wait()
        weights = w_ref[:, block * BLOCK_WIDTH : (block + 1) * BLOCK_WIDTH]
        result = jnp.dot(down_ref[:ROWS, :], weights, preferred_element_type=jnp.float32)
        result = result.astype(jnp.bfloat16).reshape(16, PART, BLOCK_WIDTH)
        out_ref[:, block * PART : (block + 1) * PART, :] = result
        if tailed:
            spread = (place == source * BLOCKS + block).astype(jnp.bfloat16)
            lifted = jnp.dot(spread, down_ref[ROWS:, :], preferred_element_type=jnp.float32)
            term = jnp.dot(lifted.astype(jnp.bfloat16), weights, preferred_element_type=jnp.float32)
            total = term if total is None else total + term
    if tailed:
        out_ref[:, BLOCKS * PART :, :] = total.astype(jnp.bfloat16).reshape(16, BLOCKS, BLOCK_WIDTH)


def last_factor(own, got, v_down, tailed):
    count = own.shape[0]
    return pl.pallas_call(
        functools.partial(last_kernel, tailed),
        out_shape=jax.ShapeDtypeStruct((16, BLOCKS * (PART + tailed), BLOCK_WIDTH), jnp.bfloat16),
        in_specs=[VMEM, VMEM, HBM],
        out_specs=VMEM,
        scratch_shapes=[
            pltpu.VMEM((count, RANK), jnp.bfloat16),
            pltpu.VMEM((RANK, HALF), jnp.bfloat16),
            pltpu.SemaphoreType.DMA((BLOCKS,)),
        ],
        compiler_params=params(60),
        cost_estimate=cost(850_000_000, 6_000_000),
        name="last_factor",
    )(own, got, v_down)


def experts(received, weights, tailed):
    u_gate_up, v_gate_up, u_down, v_down = weights
    rank_own, rank_low = first_factor(received, u_gate_up, tailed)
    down_own, down_low = middle(rank_own, other_core(rank_low), v_gate_up, u_down)
    return last_factor(down_own, other_core(down_low), v_down, tailed)


def combine_kernel(mix_ref, update_ref, residual_ref, back_a, back_b, out_ref):
    mix = mix_ref[: EXPERTS * SLOTS, :].T
    tail = mix_ref[EXPERTS * SLOTS :, :].T
    mix_high = mix.astype(jnp.bfloat16)
    mix_low = (mix - mix_high.astype(jnp.float32)).astype(jnp.bfloat16)
    tail_block = lax.broadcasted_iota(jnp.int32, (TOK_DEV, EXPERTS * BLOCKS), 1) % BLOCKS
    for half in range(2):
        tail_rows = jnp.concatenate(
            [back_b[2 * expert + half, BLOCKS * PART :, :] for expert in range(EXPERTS)], axis=0
        )
        for block in range(BLOCKS):
            rows = jnp.concatenate(
                [
                    back[2 * expert + half, block * PART : (block + 1) * PART, :]
                    for expert in range(EXPERTS)
                    for back in (back_a, back_b)
                ],
                axis=0,
            )
            here = jnp.where(tail_block == block, tail, 0.0)
            here_high = here.astype(jnp.bfloat16)
            here_low = (here - here_high.astype(jnp.float32)).astype(jnp.bfloat16)
            mixture = jnp.dot(mix_high, rows, preferred_element_type=jnp.float32)
            mixture = mixture + jnp.dot(mix_low, rows, preferred_element_type=jnp.float32)
            mixture = mixture + jnp.dot(here_high, tail_rows, preferred_element_type=jnp.float32)
            mixture = mixture + jnp.dot(here_low, tail_rows, preferred_element_type=jnp.float32)
            at = half * HALF + block * BLOCK_WIDTH
            stream = residual_ref[:, at : at + BLOCK_WIDTH].astype(jnp.float32) + update_ref[
                block, :, half * BLOCK_WIDTH : (half + 1) * BLOCK_WIDTH
            ].astype(jnp.float32)
            out_ref[:, at : at + BLOCK_WIDTH] = (stream + mixture).astype(jnp.bfloat16)


def combine(mix, update, residual, back_a, back_b):
    return pl.pallas_call(
        combine_kernel,
        out_shape=jax.ShapeDtypeStruct((TOK_DEV, D), jnp.bfloat16),
        in_specs=[VMEM] * 5,
        out_specs=VMEM,
        compiler_params=params(32),
        cost_estimate=cost(1_000_000_000, 8_000_000),
        name="combine",
    )(mix, update, residual, back_a, back_b)


def per_device(
    queries,
    keys,
    values,
    residual,
    proj_weight,
    norm_gain,
    router,
    expert_ids,
    u_gate_up,
    v_gate_up,
    u_down,
    v_down,
):
    zh, x, zl = lax.axis_index("zh"), lax.axis_index("x"), lax.axis_index("zl")
    y, c = lax.axis_index("y"), lax.axis_index("c")
    z = zh * 2 + zl
    chunk = zh * 8 + x * 2 + zl

    kv = jnp.stack(
        [
            jnp.concatenate([keys[:, at : at + HEAD_DIM], values[:, at : at + HEAD_DIM]], axis=1)
            for at in range(0, 4 * HEAD_DIM, HEAD_DIM)
        ]
    )
    kv = lax.all_to_all(kv, "y", split_axis=0, concat_axis=0, tiled=True)
    kv = kv.reshape(4 * TOK_DEV, 2 * HEAD_DIM)
    early, late = kv[:256], kv[256:]

    q = jnp.stack([queries[:, at : at + GROUP_WIDTH] for at in range(0, 8 * GROUP_WIDTH, GROUP_WIDTH)])
    copies = jnp.broadcast_to(proj_weight[None], (16, GROUP_WIDTH, GROUP_WIDTH))
    q = lax.all_to_all(q, GROUP, split_axis=0, concat_axis=0, tiled=True)
    q = q.reshape(2, Q_ROWS, GROUP_WIDTH)

    def joined(pieces):
        return jnp.concatenate(pieces, axis=0)

    early = joined(ring_pieces(early, Z))
    late = joined(ring_pieces(late, "x"))
    own = ring_pieces(early, "x") + ring_pieces(late, Z)
    q_far = mirrored(q[1])
    query_pair = jnp.stack([q[0], q_far])
    swapped = [other_core(p) for p in own]

    far_chunk = 15 - chunk
    order = jnp.arange(15, dtype=jnp.int32)
    is_far = order >= chunk
    slot_list = jnp.concatenate([is_far.astype(jnp.int32), jnp.array([0, 1], jnp.int32)])
    chunk_list = jnp.concatenate(
        [jnp.where(is_far, order - chunk, order), jnp.stack([chunk, far_chunk])]
    )
    there_z = chunk_list // 8 * 2 + chunk_list % 2
    there_x = chunk_list // 2 % 4
    rel_z = relative(z, there_z)
    rel_x = relative(x, there_x)
    rows = jnp.stack([slot_list, rel_x * 4 + rel_z, rel_z * 4 + rel_x], axis=1)
    items = jnp.concatenate([jnp.array([15, 2], jnp.int32), rows.reshape(-1)]).astype(jnp.int32)
    key_ids = jnp.arange(KEY_PART, dtype=jnp.int32)
    base = key_ids // TOK_DEV * 256 + key_ids % TOK_DEV
    kpos = jnp.stack(
        [
            base + c * TOK_DEV,
            base + c * TOK_DEV + 512,
            base + (1 - c) * TOK_DEV,
            base + (1 - c) * TOK_DEV + 512,
        ]
    ).astype(jnp.int32)

    attended = attention(items, kpos, query_pair, own + swapped)
    weight_rows = lax.all_to_all(copies, PLANE, split_axis=0, concat_axis=0, tiled=True)
    weight_rows = weight_rows.reshape(8, 2, GROUP_WIDTH, GROUP_WIDTH)
    from_y = jnp.stack([y, (y - 1) % 4, (y + 1) % 4, (y + 2) % 4])
    groups = jnp.concatenate([from_y * 2 + c, from_y * 2 + 1 - c]).astype(jnp.int32)
    near = ring_pieces(attended[0], "y")
    far = mirrored(attended[1])
    near = near + [other_core(p) for p in near]
    far = ring_pieces(far, "y")
    far = far + [other_core(p) for p in far]
    projected = projection(0, groups, weight_rows, near, None)
    projected = projection(4, groups, weight_rows, far, projected)
    update = lax.all_to_all(projected, GROUP, split_axis=0, concat_axis=0, tiled=True)

    weights = (u_gate_up, v_gate_up, u_down, v_down)
    ids_t = expert_ids.T
    send_a, send_b, mix = dispatch(ids_t, update, residual, norm_gain.reshape(1, D), router.T)
    got_a = lax.all_to_all(send_a, EXP, split_axis=0, concat_axis=0, tiled=True)
    got_b = lax.all_to_all(send_b, EXP, split_axis=0, concat_axis=0, tiled=True)
    out_a = experts(got_a, weights, False)
    back_a = lax.all_to_all(out_a, EXP, split_axis=0, concat_axis=0, tiled=True)
    out_b = experts(got_b, weights, True)
    back_b = lax.all_to_all(out_b, EXP, split_axis=0, concat_axis=0, tiled=True)
    return combine(mix, update, residual, back_a, back_b)


def solution(mesh):
    fine = Mesh(mesh.devices.reshape(2, 4, 2, 4, 2), ("zh", "x", "zl", "y", "c"))
    seq, exp = ("zh", "x"), ("zl", "y", "c")
    in_specs = (
        P(seq + exp, None),
        P(seq + exp, None),
        P(seq + exp, None),
        P(seq + exp, None),
        P(seq, exp),
        P(),
        P(),
        P(seq + exp, None),
        P(exp, None, None),
        P(exp, None, None, None),
        P(exp, None, None),
        P(exp, None, None),
    )

    return jax.shard_map(
        per_device, mesh=fine, in_specs=in_specs, out_specs=P(seq + exp, None), check_vma=False
    )
```

```python
import functools

import jax
import jax.numpy as jnp
from jax import lax
from jax.experimental import pallas as pl
from jax.experimental.pallas import tpu as pltpu
from jax.sharding import Mesh
from jax.sharding import PartitionSpec as P


D = 6144
HEAD_DIM = 128
GROUP_HEADS = 3
GROUP_WIDTH = GROUP_HEADS * HEAD_DIM
EXPERTS = 8
RANK = 512
FF_PIECE = 4096
TOK_DEV = 128
HALF = D // 2
BLOCKS = 8
BLOCK_WIDTH = HALF // BLOCKS
SLOTS = 32
PART = 16
EPS = 1e-05
SCALE = HEAD_DIM**-0.5 * 1.4426950408889634
LOW = -1e30
Q_ROWS = 512
Q_TILE = 256
KEY_PART = 256

Z = ("zh", "zl")
PLANE = ("zh", "x", "zl")
GROUP = ("y", "c")
EXP = ("zl", "y", "c")


VMEM = pl.BlockSpec(memory_space=pltpu.VMEM)
SMEM = pl.BlockSpec(memory_space=pltpu.SMEM)
ANY = pl.BlockSpec(memory_space=pl.ANY)
HBM = pl.BlockSpec(memory_space=pltpu.HBM)


def params(mib=48, **more):
    return pltpu.CompilerParams(vmem_limit_bytes=mib << 20, **more)


def cost(flops, moved, transcendentals=0):
    return pl.CostEstimate(flops=flops, bytes_accessed=moved, transcendentals=transcendentals)


def shifted(value, axis, step):
    return lax.ppermute(value, axis, [(i, (i + step) % 4) for i in range(4)])


def other_core(value):
    return lax.ppermute(value, "c", [(0, 1), (1, 0)])


def mirrored(value):
    return lax.ppermute(value, PLANE, [(i, 15 - i) for i in range(16)])


def ring_pieces(value, axis):
    half = value.shape[0] // 2
    up = shifted(value, axis, 1)
    down = shifted(value, axis, -1)
    far_up = shifted(up[:half], axis, 1)
    far_down = shifted(down[half:], axis, -1)
    return [value, up, down, far_up, far_down]


def relative(mine, theirs):
    gap = (mine - theirs) % 4
    return jnp.where(gap == 3, 2, jnp.where(gap == 2, 3, gap))


def direct_pieces(value, axis):
    return [value] + [shifted(value, axis, step) for step in (1, -1, 2)]


def attention_kernel(items, kpos_ref, q_ref, *refs):
    pieces = refs[:20]
    out_ref = refs[20]
    kv_ref, max_ref, acc_ref, sems = refs[21:]
    copies = []
    for which in range(4):
        for number in range(5):
            source = pieces[which * 5 + number]
            if number < 3:
                target = kv_ref.at[which, pl.ds(number * 4, 4)]
            else:
                target = kv_ref.at[which, pl.ds(12 + (number - 3) * 2, 2)]
            copies.append(pltpu.make_async_copy(source, target, sems.at[which * 5 + number]))
    for copy in copies:
        copy.start()
    max_ref[...] = jnp.full(max_ref.shape, LOW, jnp.float32)
    acc_ref[...] = jnp.zeros(acc_ref.shape, jnp.float32)
    for copy in copies:
        copy.wait()

    def work(slot, at, masked):
        keys, values = [], []
        ones = jnp.ones((KEY_PART, HEAD_DIM), jnp.bfloat16)
        for which in range(4):
            block = at[which % 2]
            keys.append(kv_ref[which, block, :, 0:HEAD_DIM])
            value = kv_ref[which, block, :, HEAD_DIM : 2 * HEAD_DIM]
            values.append(jnp.concatenate([value, ones], axis=1))
        for tile in range(Q_ROWS // Q_TILE):
            rows = pl.ds(tile * Q_TILE, Q_TILE)
            for head in range(GROUP_HEADS):
                query = q_ref[slot, rows, head * HEAD_DIM : (head + 1) * HEAD_DIM]
                scores = []
                for which in range(4):
                    part = lax.dot_general(
                        query,
                        keys[which],
                        (((1,), (1,)), ((), ())),
                        preferred_element_type=jnp.float32,
                    )
                    if masked:
                        row_pos = (
                            slot * Q_ROWS
                            + tile * Q_TILE
                            + lax.broadcasted_iota(jnp.int32, (Q_TILE, KEY_PART), 0)
                        )
                        part = jnp.where(kpos_ref[which : which + 1, :] <= row_pos, part, LOW)
                    scores.append(part)
                highest = jnp.maximum(
                    jnp.maximum(scores[0], scores[1]), jnp.maximum(scores[2], scores[3])
                )
                old_max = max_ref[slot, head, rows, :]
                new_max = jnp.maximum(old_max, jnp.max(highest, axis=1, keepdims=True))
                level = jnp.tile(new_max * SCALE, (1, KEY_PART // HEAD_DIM))
                update = None
                for which in range(4):
                    weights = jnp.exp2(scores[which] * SCALE - level).astype(jnp.bfloat16)
                    term = jnp.dot(weights, values[which], preferred_element_type=jnp.float32)
                    update = term if update is None else update + term
                fading = jnp.exp2((old_max - new_max) * SCALE)
                max_ref[slot, head, rows, :] = new_max
                acc_ref[slot, head, rows, 0:HEAD_DIM] = (
                    acc_ref[slot, head, rows, 0:HEAD_DIM] * fading + update[:, :HEAD_DIM]
                )
                acc_ref[slot, head, rows, HEAD_DIM:] = (
                    acc_ref[slot, head, rows, HEAD_DIM:] * fading + update[:, HEAD_DIM:]
                )

    open_count = items[0]
    masked_count = items[1]

    def open_step(number, carry):
        at = 2 + 3 * number
        work(items[at], (items[at + 1], items[at + 2]), False)
        return carry

    def masked_step(number, carry):
        at = 2 + 3 * (open_count + number)
        work(items[at], (items[at + 1], items[at + 2]), True)
        return carry

    lax.fori_loop(0, open_count, open_step, 0)
    lax.fori_loop(0, masked_count, masked_step, 0)
    for slot in range(2):
        for head in range(GROUP_HEADS):
            out_ref[slot, :, head * HEAD_DIM : (head + 1) * HEAD_DIM] = (
                acc_ref[slot, head, :, 0:HEAD_DIM] / acc_ref[slot, head, :, HEAD_DIM:]
            ).astype(jnp.bfloat16)


def attention(items, kpos, query_pair, pieces):
    shaped = [p.reshape(-1, KEY_PART, 2 * HEAD_DIM) for p in pieces]
    return pl.pallas_call(
        attention_kernel,
        out_shape=jax.ShapeDtypeStruct((2, Q_ROWS, GROUP_WIDTH), jnp.bfloat16),
        in_specs=[SMEM, VMEM, VMEM] + [ANY] * 20,
        out_specs=VMEM,
        scratch_shapes=[
            pltpu.VMEM((4, 16, KEY_PART, 2 * HEAD_DIM), jnp.bfloat16),
            pltpu.VMEM((2, GROUP_HEADS, Q_ROWS, HEAD_DIM), jnp.float32),
            pltpu.VMEM((2, GROUP_HEADS, Q_ROWS, 2 * HEAD_DIM), jnp.float32),
            pltpu.SemaphoreType.DMA((20,)),
        ],
        compiler_params=params(28),
        cost_estimate=cost(27_000_000_000, 10_000_000, 26_000_000),
        name="attention",
    )(items, kpos, query_pair, *shaped)


def projection_kernel(first, groups, w_ref, *refs):
    pieces = refs[:10]
    if first:
        w_all = w_ref
        out_ref, rows_ref, done_ref, sems, w_sems, out_sem = refs[-6:]
    else:
        out_ref, w_all, rows_ref, done_ref, sems, w_sems, out_sem = refs[-7:]
    copies = []
    for core in range(2):
        for number in range(4):
            at = (core * 4 + number) * GROUP_WIDTH
            for side in range(0 if first else 2):
                copies.append(
                    pltpu.make_async_copy(
                        w_ref.at[groups[core * 4 + number], side],
                        w_all.at[pl.ds(at, GROUP_WIDTH), pl.ds(side * GROUP_WIDTH, GROUP_WIDTH)],
                        w_sems.at[(core * 4 + number) * 2 + side],
                    )
                )
        for number in range(5):
            at = (core * 4 + min(number, 3)) * GROUP_WIDTH
            source = pieces[core * 5 + number]
            low = 256 if number == 4 else 0
            copies.append(
                pltpu.make_async_copy(
                    source,
                    rows_ref.at[pl.ds(low, source.shape[0]), pl.ds(at, GROUP_WIDTH)],
                    sems.at[core * 5 + number],
                )
            )
    for copy in copies:
        copy.start()
    for copy in copies:
        copy.wait()
    for tile in range(Q_ROWS // Q_TILE):
        total = jnp.dot(
            rows_ref[tile * Q_TILE : (tile + 1) * Q_TILE, :],
            w_all[...],
            preferred_element_type=jnp.float32,
        )
        done_ref[tile * 2 : (tile + 1) * 2] = total.astype(jnp.bfloat16).reshape(
            2, TOK_DEV, 2 * GROUP_WIDTH
        )
    out = pltpu.make_async_copy(done_ref, out_ref.at[pl.ds(first, 4)], out_sem)
    out.start()
    out.wait()


def projection(first, groups, weights, pieces, before):
    more = [] if before is None else [before]
    out = jax.ShapeDtypeStruct((8, TOK_DEV, 2 * GROUP_WIDTH), jnp.bfloat16)
    arranged = jax.ShapeDtypeStruct((8 * GROUP_WIDTH, 2 * GROUP_WIDTH), jnp.bfloat16)
    return pl.pallas_call(
        functools.partial(projection_kernel, first),
        out_shape=out if more else (out, arranged),
        in_specs=[SMEM] + [VMEM if more else ANY] + [ANY] * (10 + len(more)),
        out_specs=ANY if more else (ANY, VMEM),
        scratch_shapes=[
            pltpu.VMEM((Q_ROWS, 8 * GROUP_WIDTH), jnp.bfloat16),
            pltpu.VMEM((4, TOK_DEV, 2 * GROUP_WIDTH), jnp.bfloat16),
            pltpu.SemaphoreType.DMA((10,)),
            pltpu.SemaphoreType.DMA((16,)),
            pltpu.SemaphoreType.DMA,
        ],
        input_output_aliases={12: 0} if more else {},
        compiler_params=params(16),
        cost_estimate=cost(2_500_000_000, 9_000_000),
        name="projection",
    )(groups, weights, *pieces, *more)


def slot_tables(ids_t):
    expert = lax.broadcasted_iota(jnp.int32, (EXPERTS, TOK_DEV), 0)
    first = (expert == ids_t[0:1, :]).astype(jnp.float32)
    second = (expert == ids_t[1:2, :]).astype(jnp.float32)
    member = first + second
    before = (
        lax.broadcasted_iota(jnp.int32, (TOK_DEV, TOK_DEV), 0)
        < lax.broadcasted_iota(jnp.int32, (TOK_DEV, TOK_DEV), 1)
    ).astype(jnp.bfloat16)
    slot = jnp.dot(member.astype(jnp.bfloat16), before, preferred_element_type=jnp.float32)
    return first, second, member, slot


def dispatch_kernel(ids_ref, update_ref, residual_ref, gain_ref, router_ref, send_ref, mix_ref, normed_ref):
    squares = jnp.zeros((TOK_DEV, 1), jnp.float32)
    for half in range(2):
        for group in range(BLOCKS):
            at = half * HALF + group * BLOCK_WIDTH
            row = residual_ref[:, at : at + BLOCK_WIDTH].astype(jnp.float32) + update_ref[
                group, :, half * BLOCK_WIDTH : (half + 1) * BLOCK_WIDTH
            ].astype(jnp.float32)
            squares = squares + jnp.sum(row * row, axis=1, keepdims=True)
    factor = lax.rsqrt(squares / D + EPS)
    for half in range(2):
        for group in range(BLOCKS):
            at = half * HALF + group * BLOCK_WIDTH
            row = residual_ref[:, at : at + BLOCK_WIDTH].astype(jnp.float32) + update_ref[
                group, :, half * BLOCK_WIDTH : (half + 1) * BLOCK_WIDTH
            ].astype(jnp.float32)
            gain = gain_ref[:, at : at + BLOCK_WIDTH].astype(jnp.float32)
            normed_ref[:, at : at + BLOCK_WIDTH] = (row * factor * gain).astype(jnp.bfloat16)
    first, second, member, slot = slot_tables(ids_ref[...])
    slot_ids = lax.broadcasted_iota(jnp.int32, (SLOTS, TOK_DEV), 0).astype(jnp.float32)
    picks, tails = [], []
    last = jnp.where(slot == float(SLOTS), member, 0.0)
    for expert in range(EXPERTS):
        picks.append(
            jnp.where(slot[expert : expert + 1, :] == slot_ids, member[expert : expert + 1, :], 0.0)
        )
        tails.append(jnp.broadcast_to(last[expert : expert + 1, :], (BLOCKS, TOK_DEV)))
    pick = jnp.concatenate(picks, axis=0)
    tail = jnp.concatenate(tails, axis=0)
    tail_block = lax.broadcasted_iota(jnp.int32, (EXPERTS * BLOCKS, TOK_DEV), 0) % BLOCKS
    pick_low = pick.astype(jnp.bfloat16)
    for half in range(2):
        tail_rows = None
        for block in range(BLOCKS):
            at = half * HALF + block * BLOCK_WIDTH
            rows = normed_ref[:, at : at + BLOCK_WIDTH]
            moved = jnp.dot(pick_low, rows, preferred_element_type=jnp.float32).astype(jnp.bfloat16)
            for expert in range(EXPERTS):
                send_ref[2 * expert + half, block * SLOTS : (block + 1) * SLOTS, :] = moved[
                    expert * SLOTS : (expert + 1) * SLOTS, :
                ]
            chosen = jnp.where(tail_block == block, tail, 0.0).astype(jnp.bfloat16)
            term = jnp.dot(chosen, rows, preferred_element_type=jnp.float32)
            tail_rows = term if tail_rows is None else tail_rows + term
        tail_rows = tail_rows.astype(jnp.bfloat16)
        for expert in range(EXPERTS):
            send_ref[2 * expert + half, BLOCKS * SLOTS :, :] = tail_rows[
                expert * BLOCKS : (expert + 1) * BLOCKS, :
            ]
    logits = lax.dot_general(
        router_ref[...],
        normed_ref[...],
        (((1,), (1,)), ((), ())),
        preferred_element_type=jnp.float32,
    )
    chosen_first = jnp.sum(first * logits, axis=0, keepdims=True)
    chosen_second = jnp.sum(second * logits, axis=0, keepdims=True)
    mix_first = 1.0 / (1.0 + jnp.exp(chosen_second - chosen_first))
    mix_second = 1.0 / (1.0 + jnp.exp(chosen_first - chosen_second))
    share = first * mix_first + second * mix_second
    for expert in range(EXPERTS):
        mine = share[expert : expert + 1, :]
        mix_ref[expert * SLOTS : (expert + 1) * SLOTS, :] = picks[expert] * mine
        mix_ref[
            EXPERTS * SLOTS + expert * BLOCKS : EXPERTS * SLOTS + (expert + 1) * BLOCKS, :
        ] = tails[expert] * mine


def dispatch(ids_t, update, residual, gain, router_t):
    return pl.pallas_call(
        dispatch_kernel,
        out_shape=(
            jax.ShapeDtypeStruct((16, BLOCKS * (SLOTS + 1), BLOCK_WIDTH), jnp.bfloat16),
            jax.ShapeDtypeStruct((EXPERTS * (SLOTS + BLOCKS), TOK_DEV), jnp.float32),
        ),
        in_specs=[VMEM] * 5,
        out_specs=(VMEM, VMEM),
        scratch_shapes=[pltpu.VMEM((TOK_DEV, D), jnp.bfloat16)],
        compiler_params=params(32),
        cost_estimate=cost(800_000_000, 8_000_000),
        name="dispatch",
    )(ids_t, update, residual, gain, router_t)


PARTS = SLOTS // PART
ROWS = 16 * SLOTS
ALL_ROWS = ROWS + 16
GROUPS = 4
GROUP_DEPTH = HALF // GROUPS


def row_pick(block):
    source = lax.broadcasted_iota(jnp.int32, (16, 16 * BLOCKS), 0)
    place = lax.broadcasted_iota(jnp.int32, (16, 16 * BLOCKS), 1)
    return (place == source * BLOCKS + block).astype(jnp.bfloat16)


def first_kernel(rows_ref, u_ref, low_ref, x_ref, tail_ref, w_ref, acc_ref, sems, row_sems):
    copies = []
    for group in range(GROUPS):
        rows = pl.ds(group * GROUP_DEPTH, GROUP_DEPTH)
        copies.append(pltpu.make_async_copy(u_ref.at[0, rows], w_ref.at[rows], sems.at[group]))
    moves = [
        pltpu.make_async_copy(
            rows_ref.at[:, pl.ds(BLOCKS * SLOTS, BLOCKS), :], tail_ref, row_sems.at[2 * BLOCKS]
        )
    ]
    for block in range(BLOCKS):
        for part in range(PARTS):
            moves.append(
                pltpu.make_async_copy(
                    rows_ref.at[:, pl.ds(block * SLOTS + part * PART, PART), :],
                    x_ref.at[pl.ds(part * 16, 16), :, pl.ds(block * BLOCK_WIDTH, BLOCK_WIDTH)],
                    row_sems.at[block * PARTS + part],
                )
            )
    for move in moves[: 1 + 2 * PARTS]:
        move.start()
    copies[0].start()
    for move in moves[1 + 2 * PARTS :]:
        move.start()
    for copy in copies[1:]:
        copy.start()
    moves[0].wait()
    tail = tail_ref[...].reshape(16 * BLOCKS, BLOCK_WIDTH)
    for block in range(BLOCKS):
        picked = jnp.dot(row_pick(block), tail, preferred_element_type=jnp.float32)
        x_ref[2 * 16, :, block * BLOCK_WIDTH : (block + 1) * BLOCK_WIDTH] = picked.astype(
            jnp.bfloat16
        )
    each = BLOCKS // GROUPS * PARTS
    for group in range(GROUPS):
        at = group * GROUP_DEPTH
        for move in moves[1 + group * each : 1 + (group + 1) * each]:
            move.wait()
        copies[group].wait()
        rows = x_ref[:, :, at : at + GROUP_DEPTH].reshape(ALL_ROWS, GROUP_DEPTH)
        term = jnp.dot(rows, w_ref[at : at + GROUP_DEPTH, :], preferred_element_type=jnp.float32)
        if group == 0:
            acc_ref[...] = term
        elif group < GROUPS - 1:
            acc_ref[...] += term
        else:
            low_ref[...] = (acc_ref[...] + term).astype(jnp.bfloat16)


def first_factor(received, u_gate_up):
    return pl.pallas_call(
        first_kernel,
        out_shape=jax.ShapeDtypeStruct((ALL_ROWS, 2 * RANK), jnp.bfloat16),
        in_specs=[ANY, ANY],
        out_specs=VMEM,
        scratch_shapes=[
            pltpu.VMEM((16 * PARTS + 1, PART, HALF), jnp.bfloat16),
            pltpu.VMEM((16, BLOCKS, BLOCK_WIDTH), jnp.bfloat16),
            pltpu.VMEM((HALF, 2 * RANK), jnp.bfloat16),
            pltpu.VMEM((ALL_ROWS, 2 * RANK), jnp.float32),
            pltpu.SemaphoreType.DMA((GROUPS,)),
            pltpu.SemaphoreType.DMA((BLOCKS * PARTS + 1,)),
        ],
        compiler_params=params(58),
        cost_estimate=cost(3_400_000_000, 9_000_000),
        name="first_factor",
    )(received, u_gate_up)


FF_TILE = 512
FF_STEPS = FF_PIECE // FF_TILE


def middle_kernel(own_ref, got_ref, v_ref, u_ref, low_ref, rank_ref, vs_ref, us_ref, acc_ref, sems):
    copies = []
    for step in range(FF_STEPS):
        columns = pl.ds(step * FF_TILE, FF_TILE)
        copies.append(
            (
                pltpu.make_async_copy(
                    v_ref.at[0, :, :, columns], vs_ref.at[:, :, columns], sems.at[2 * step]
                ),
                pltpu.make_async_copy(
                    u_ref.at[0, columns, :], us_ref.at[columns, :], sems.at[2 * step + 1]
                ),
            )
        )
    for pair in copies:
        for copy in pair:
            copy.start()
    rank_ref[...] = (
        own_ref[...].astype(jnp.float32) + got_ref[...].astype(jnp.float32)
    ).astype(jnp.bfloat16)
    for step in range(FF_STEPS):
        columns = slice(step * FF_TILE, (step + 1) * FF_TILE)
        for copy in copies[step]:
            copy.wait()
        gate = jnp.dot(rank_ref[:, :RANK], vs_ref[0, :, columns], preferred_element_type=jnp.float32)
        up = jnp.dot(rank_ref[:, RANK:], vs_ref[1, :, columns], preferred_element_type=jnp.float32)
        hidden = (gate / (1.0 + jnp.exp(-gate)) * up).astype(jnp.bfloat16)
        term = jnp.dot(hidden, us_ref[columns, :], preferred_element_type=jnp.float32)
        if step == 0:
            acc_ref[...] = term
        elif step < FF_STEPS - 1:
            acc_ref[...] += term
        else:
            low_ref[...] = (acc_ref[...] + term).astype(jnp.bfloat16)


def middle(own, got, v_gate_up, u_down):
    return pl.pallas_call(
        middle_kernel,
        out_shape=jax.ShapeDtypeStruct((ALL_ROWS, RANK), jnp.bfloat16),
        in_specs=[VMEM, VMEM, ANY, ANY],
        out_specs=VMEM,
        scratch_shapes=[
            pltpu.VMEM((ALL_ROWS, 2 * RANK), jnp.bfloat16),
            pltpu.VMEM((2, RANK, FF_PIECE), jnp.bfloat16),
            pltpu.VMEM((FF_PIECE, RANK), jnp.bfloat16),
            pltpu.VMEM((ALL_ROWS, RANK), jnp.float32),
            pltpu.SemaphoreType.DMA((2 * FF_STEPS,)),
        ],
        compiler_params=params(60),
        cost_estimate=cost(6_700_000_000, 14_000_000, 2_200_000),
        name="middle",
    )(own, got, v_gate_up, u_down)


def last_kernel(own_ref, got_ref, v_ref, out_ref, down_ref, w_ref, sems):
    copies = []
    for block in range(BLOCKS):
        columns = pl.ds(block * BLOCK_WIDTH, BLOCK_WIDTH)
        copies.append(
            pltpu.make_async_copy(v_ref.at[0, :, columns], w_ref.at[:, columns], sems.at[block])
        )
    for copy in copies:
        copy.start()
    down_ref[...] = (
        own_ref[...].astype(jnp.float32) + got_ref[...].astype(jnp.float32)
    ).astype(jnp.bfloat16)
    total = None
    place = lax.broadcasted_iota(jnp.int32, (16 * BLOCKS, 16), 0)
    source = lax.broadcasted_iota(jnp.int32, (16 * BLOCKS, 16), 1)
    for block in range(BLOCKS):
        copies[block].wait()
        weights = w_ref[:, block * BLOCK_WIDTH : (block + 1) * BLOCK_WIDTH]
        spread = (place == source * BLOCKS + block).astype(jnp.bfloat16)
        lifted = jnp.dot(spread, down_ref[ROWS:, :], preferred_element_type=jnp.float32)
        rows = jnp.concatenate([down_ref[:ROWS, :], lifted.astype(jnp.bfloat16)], axis=0)
        result = jnp.dot(rows, weights, preferred_element_type=jnp.float32)
        main = result[:ROWS].astype(jnp.bfloat16).reshape(PARTS, 16, PART, BLOCK_WIDTH)
        for part in range(PARTS):
            at = block * SLOTS + part * PART
            out_ref[:, at : at + PART, :] = main[part]
        total = result[ROWS:] if total is None else total + result[ROWS:]
    out_ref[:, BLOCKS * SLOTS :, :] = total.astype(jnp.bfloat16).reshape(16, BLOCKS, BLOCK_WIDTH)


def last_factor(own, got, v_down):
    return pl.pallas_call(
        last_kernel,
        out_shape=jax.ShapeDtypeStruct((16, BLOCKS * (SLOTS + 1), BLOCK_WIDTH), jnp.bfloat16),
        in_specs=[VMEM, VMEM, ANY],
        out_specs=VMEM,
        scratch_shapes=[
            pltpu.VMEM((ALL_ROWS, RANK), jnp.bfloat16),
            pltpu.VMEM((RANK, HALF), jnp.bfloat16),
            pltpu.SemaphoreType.DMA((BLOCKS,)),
        ],
        compiler_params=params(61),
        cost_estimate=cost(1_700_000_000, 6_000_000),
        name="last_factor",
    )(own, got, v_down)


def combine_kernel(mix_ref, update_ref, residual_ref, back_ref, out_ref):
    mix = mix_ref[: EXPERTS * SLOTS, :].T
    tail = mix_ref[EXPERTS * SLOTS :, :].T
    mix_high = mix.astype(jnp.bfloat16)
    mix_low = (mix - mix_high.astype(jnp.float32)).astype(jnp.bfloat16)
    tail_block = lax.broadcasted_iota(jnp.int32, (TOK_DEV, EXPERTS * BLOCKS), 1) % BLOCKS
    for half in range(2):
        tail_rows = jnp.concatenate(
            [back_ref[2 * expert + half, BLOCKS * SLOTS :, :] for expert in range(EXPERTS)], axis=0
        )
        for block in range(BLOCKS):
            rows = jnp.concatenate(
                [
                    back_ref[2 * expert + half, block * SLOTS : (block + 1) * SLOTS, :]
                    for expert in range(EXPERTS)
                ],
                axis=0,
            )
            here = jnp.where(tail_block == block, tail, 0.0)
            here_high = here.astype(jnp.bfloat16)
            here_low = (here - here_high.astype(jnp.float32)).astype(jnp.bfloat16)
            mixture = jnp.dot(mix_high, rows, preferred_element_type=jnp.float32)
            mixture = mixture + jnp.dot(mix_low, rows, preferred_element_type=jnp.float32)
            mixture = mixture + jnp.dot(here_high, tail_rows, preferred_element_type=jnp.float32)
            mixture = mixture + jnp.dot(here_low, tail_rows, preferred_element_type=jnp.float32)
            at = half * HALF + block * BLOCK_WIDTH
            stream = residual_ref[:, at : at + BLOCK_WIDTH].astype(jnp.float32) + update_ref[
                block, :, half * BLOCK_WIDTH : (half + 1) * BLOCK_WIDTH
            ].astype(jnp.float32)
            out_ref[:, at : at + BLOCK_WIDTH] = (stream + mixture).astype(jnp.bfloat16)


def combine(mix, update, residual, back):
    return pl.pallas_call(
        combine_kernel,
        out_shape=jax.ShapeDtypeStruct((TOK_DEV, D), jnp.bfloat16),
        in_specs=[VMEM] * 4,
        out_specs=VMEM,
        compiler_params=params(32),
        cost_estimate=cost(1_000_000_000, 8_000_000),
        name="combine",
    )(mix, update, residual, back)


def per_device(
    queries,
    keys,
    values,
    residual,
    proj_weight,
    norm_gain,
    router,
    expert_ids,
    u_gate_up,
    v_gate_up,
    u_down,
    v_down,
):
    zh, x, zl = lax.axis_index("zh"), lax.axis_index("x"), lax.axis_index("zl")
    y, c = lax.axis_index("y"), lax.axis_index("c")
    z = zh * 2 + zl
    chunk = zh * 8 + x * 2 + zl

    kv = jnp.stack(
        [
            jnp.concatenate([keys[:, at : at + HEAD_DIM], values[:, at : at + HEAD_DIM]], axis=1)
            for at in range(0, 4 * HEAD_DIM, HEAD_DIM)
        ]
    )
    kv = lax.all_to_all(kv, "y", split_axis=0, concat_axis=0, tiled=True)
    kv = kv.reshape(4 * TOK_DEV, 2 * HEAD_DIM)
    early, late = kv[:256], kv[256:]

    q = jnp.stack([queries[:, at : at + GROUP_WIDTH] for at in range(0, 8 * GROUP_WIDTH, GROUP_WIDTH)])
    copies = jnp.broadcast_to(proj_weight[None], (16, GROUP_WIDTH, GROUP_WIDTH))
    q = lax.all_to_all(q, GROUP, split_axis=0, concat_axis=0, tiled=True)
    q = q.reshape(2, Q_ROWS, GROUP_WIDTH)

    def joined(pieces):
        return jnp.concatenate(pieces, axis=0)

    early = joined(direct_pieces(early, Z))
    late = joined(direct_pieces(late, "x"))
    own = ring_pieces(early, "x") + ring_pieces(late, Z)
    q_far = mirrored(q[1])
    query_pair = jnp.stack([q[0], q_far])
    swapped = [other_core(p) for p in own]

    far_chunk = 15 - chunk
    order = jnp.arange(15, dtype=jnp.int32)
    is_far = order >= chunk
    slot_list = jnp.concatenate([is_far.astype(jnp.int32), jnp.array([0, 1], jnp.int32)])
    chunk_list = jnp.concatenate(
        [jnp.where(is_far, order - chunk, order), jnp.stack([chunk, far_chunk])]
    )
    there_z = chunk_list // 8 * 2 + chunk_list % 2
    there_x = chunk_list // 2 % 4
    rel_z = relative(z, there_z)
    rel_x = relative(x, there_x)
    rows = jnp.stack([slot_list, rel_x * 4 + rel_z, rel_z * 4 + rel_x], axis=1)
    items = jnp.concatenate([jnp.array([15, 2], jnp.int32), rows.reshape(-1)]).astype(jnp.int32)
    key_ids = jnp.arange(KEY_PART, dtype=jnp.int32)
    base = key_ids // TOK_DEV * 256 + key_ids % TOK_DEV
    kpos = jnp.stack(
        [
            base + c * TOK_DEV,
            base + c * TOK_DEV + 512,
            base + (1 - c) * TOK_DEV,
            base + (1 - c) * TOK_DEV + 512,
        ]
    ).astype(jnp.int32)

    attended = attention(items, kpos, query_pair, own + swapped)
    weight_rows = lax.all_to_all(copies, PLANE, split_axis=0, concat_axis=0, tiled=True)
    weight_rows = weight_rows.reshape(8, 2, GROUP_WIDTH, GROUP_WIDTH)
    from_y = jnp.stack([y, (y - 1) % 4, (y + 1) % 4, (y + 2) % 4])
    groups = jnp.concatenate([from_y * 2 + c, from_y * 2 + 1 - c]).astype(jnp.int32)
    near = ring_pieces(attended[0], "y")
    far = mirrored(attended[1])
    near = near + [other_core(p) for p in near]
    far = ring_pieces(far, "y")
    far = far + [other_core(p) for p in far]
    projected, arranged = projection(0, groups, weight_rows, near, None)
    projected = projection(4, groups, arranged, far, projected)
    update = lax.all_to_all(projected, GROUP, split_axis=0, concat_axis=0, tiled=True)

    ids_t = expert_ids.T
    send, mix = dispatch(ids_t, update, residual, norm_gain.reshape(1, D), router.T)
    received = lax.all_to_all(send, EXP, split_axis=0, concat_axis=0, tiled=True)
    rank_low = first_factor(received, u_gate_up)
    down_low = middle(rank_low, other_core(rank_low), v_gate_up, u_down)
    out_rows = last_factor(down_low, other_core(down_low), v_down)
    back = lax.all_to_all(out_rows, EXP, split_axis=0, concat_axis=0, tiled=True)
    return combine(mix, update, residual, back)


def solution(mesh):
    fine = Mesh(mesh.devices.reshape(2, 4, 2, 4, 2), ("zh", "x", "zl", "y", "c"))
    seq, exp = ("zh", "x"), ("zl", "y", "c")
    in_specs = (
        P(seq + exp, None),
        P(seq + exp, None),
        P(seq + exp, None),
        P(seq + exp, None),
        P(seq, exp),
        P(),
        P(),
        P(seq + exp, None),
        P(exp, None, None),
        P(exp, None, None, None),
        P(exp, None, None),
        P(exp, None, None),
    )

    return jax.shard_map(
        per_device, mesh=fine, in_specs=in_specs, out_specs=P(seq + exp, None), check_vma=False
    )
```

```python
import functools

import jax
import jax.numpy as jnp
from jax import lax
from jax.experimental import pallas as pl
from jax.experimental.pallas import tpu as pltpu
from jax.sharding import Mesh
from jax.sharding import PartitionSpec as P


D = 6144
HEAD_DIM = 128
GROUP_HEADS = 3
GROUP_WIDTH = GROUP_HEADS * HEAD_DIM
EXPERTS = 8
RANK = 512
FF_PIECE = 4096
TOK_DEV = 128
HALF = D // 2
BLOCKS = 8
BLOCK_WIDTH = HALF // BLOCKS
SLOTS = 32
PART = 16
EPS = 1e-05
SCALE = HEAD_DIM**-0.5 * 1.4426950408889634
LOW = -1e30
Q_ROWS = 512
Q_TILE = 256
KEY_PART = 256

Z = ("zh", "zl")
PLANE = ("zh", "x", "zl")
GROUP = ("y", "c")
EXP = ("zl", "y", "c")


VMEM = pl.BlockSpec(memory_space=pltpu.VMEM)
SMEM = pl.BlockSpec(memory_space=pltpu.SMEM)
ANY = pl.BlockSpec(memory_space=pl.ANY)
HBM = pl.BlockSpec(memory_space=pltpu.HBM)


def params(mib=48, **more):
    return pltpu.CompilerParams(vmem_limit_bytes=mib << 20, **more)


def cost(flops, moved, transcendentals=0):
    return pl.CostEstimate(flops=flops, bytes_accessed=moved, transcendentals=transcendentals)


def shifted(value, axis, step):
    return lax.ppermute(value, axis, [(i, (i + step) % 4) for i in range(4)])


def other_core(value):
    return lax.ppermute(value, "c", [(0, 1), (1, 0)])


def mirrored(value):
    return lax.ppermute(value, PLANE, [(i, 15 - i) for i in range(16)])


def ring_pieces(value, axis):
    half = value.shape[0] // 2
    up = shifted(value, axis, 1)
    down = shifted(value, axis, -1)
    far_up = shifted(up[:half], axis, 1)
    far_down = shifted(down[half:], axis, -1)
    return [value, up, down, far_up, far_down]


def relative(mine, theirs):
    gap = (mine - theirs) % 4
    return jnp.where(gap == 3, 2, jnp.where(gap == 2, 3, gap))


def direct_pieces(value, axis):
    return [value] + [shifted(value, axis, step) for step in (1, -1, 2)]


def pack_kernel(*refs):
    sources, out_ref, sems = refs[:-2], refs[-2], refs[-1]
    count, width = out_ref.shape[0], out_ref.shape[2] // len(sources)
    copies = []
    for place in range(count):
        for number, source in enumerate(sources):
            copies.append(
                pltpu.make_async_copy(
                    source.at[:, pl.ds(place * width, width)],
                    out_ref.at[place, :, pl.ds(number * width, width)],
                    sems.at[place * len(sources) + number],
                )
            )
    for copy in copies:
        copy.start()
    for copy in copies:
        copy.wait()


def packed(sources, shape):
    return pl.pallas_call(
        pack_kernel,
        out_shape=jax.ShapeDtypeStruct(shape, jnp.bfloat16),
        in_specs=[ANY] * len(sources),
        out_specs=VMEM,
        scratch_shapes=[pltpu.SemaphoreType.DMA((shape[0] * len(sources),))],
        compiler_params=params(8),
        cost_estimate=cost(1_000_000_000, 2_000_000),
        name="pack",
    )(*sources)


def pack_kv(keys, values):
    return packed((keys, values), (4, TOK_DEV, 2 * HEAD_DIM))


def pack_q(queries):
    return packed((queries,), (8, TOK_DEV, GROUP_WIDTH))


def attention_kernel(items, kpos_ref, q_ref, *refs):
    pieces = refs[:20]
    out_ref = refs[20]
    kv_ref, max_ref, acc_ref, sems = refs[21:]
    copies = []
    for which in range(4):
        for number in range(5):
            source = pieces[which * 5 + number]
            if number < 3:
                target = kv_ref.at[which, pl.ds(number * 4, 4)]
            else:
                target = kv_ref.at[which, pl.ds(12 + (number - 3) * 2, 2)]
            copies.append(pltpu.make_async_copy(source, target, sems.at[which * 5 + number]))
    for copy in copies:
        copy.start()
    max_ref[...] = jnp.full(max_ref.shape, LOW, jnp.float32)
    acc_ref[...] = jnp.zeros(acc_ref.shape, jnp.float32)
    for copy in copies:
        copy.wait()

    def work(slot, at, masked):
        keys, values = [], []
        ones = jnp.ones((KEY_PART, HEAD_DIM), jnp.bfloat16)
        for which in range(4):
            block = at[which % 2]
            keys.append(kv_ref[which, block, :, 0:HEAD_DIM])
            value = kv_ref[which, block, :, HEAD_DIM : 2 * HEAD_DIM]
            values.append(jnp.concatenate([value, ones], axis=1))
        for tile in range(Q_ROWS // Q_TILE):
            rows = pl.ds(tile * Q_TILE, Q_TILE)
            for head in range(GROUP_HEADS):
                query = q_ref[slot, rows, head * HEAD_DIM : (head + 1) * HEAD_DIM]
                scores = []
                for which in range(4):
                    part = lax.dot_general(
                        query,
                        keys[which],
                        (((1,), (1,)), ((), ())),
                        preferred_element_type=jnp.float32,
                    )
                    if masked:
                        row_pos = (
                            slot * Q_ROWS
                            + tile * Q_TILE
                            + lax.broadcasted_iota(jnp.int32, (Q_TILE, KEY_PART), 0)
                        )
                        part = jnp.where(kpos_ref[which : which + 1, :] <= row_pos, part, LOW)
                    scores.append(part)
                highest = jnp.maximum(
                    jnp.maximum(scores[0], scores[1]), jnp.maximum(scores[2], scores[3])
                )
                old_max = max_ref[slot, head, rows, :]
                new_max = jnp.maximum(old_max, jnp.max(highest, axis=1, keepdims=True))
                level = jnp.tile(new_max * SCALE, (1, KEY_PART // HEAD_DIM))
                update = None
                for which in range(4):
                    weights = jnp.exp2(scores[which] * SCALE - level).astype(jnp.bfloat16)
                    term = jnp.dot(weights, values[which], preferred_element_type=jnp.float32)
                    update = term if update is None else update + term
                fading = jnp.exp2((old_max - new_max) * SCALE)
                max_ref[slot, head, rows, :] = new_max
                acc_ref[slot, head, rows, 0:HEAD_DIM] = (
                    acc_ref[slot, head, rows, 0:HEAD_DIM] * fading + update[:, :HEAD_DIM]
                )
                acc_ref[slot, head, rows, HEAD_DIM:] = (
                    acc_ref[slot, head, rows, HEAD_DIM:] * fading + update[:, HEAD_DIM:]
                )

    open_count = items[0]
    masked_count = items[1]

    def open_step(number, carry):
        at = 2 + 3 * number
        work(items[at], (items[at + 1], items[at + 2]), False)
        return carry

    def masked_step(number, carry):
        at = 2 + 3 * (open_count + number)
        work(items[at], (items[at + 1], items[at + 2]), True)
        return carry

    lax.fori_loop(0, open_count, open_step, 0)
    lax.fori_loop(0, masked_count, masked_step, 0)
    for slot in range(2):
        for head in range(GROUP_HEADS):
            out_ref[slot, :, head * HEAD_DIM : (head + 1) * HEAD_DIM] = (
                acc_ref[slot, head, :, 0:HEAD_DIM] / acc_ref[slot, head, :, HEAD_DIM:]
            ).astype(jnp.bfloat16)


def attention(items, kpos, query_pair, pieces):
    shaped = [p.reshape(-1, KEY_PART, 2 * HEAD_DIM) for p in pieces]
    return pl.pallas_call(
        attention_kernel,
        out_shape=jax.ShapeDtypeStruct((2, Q_ROWS, GROUP_WIDTH), jnp.bfloat16),
        in_specs=[SMEM, VMEM, VMEM] + [ANY] * 20,
        out_specs=VMEM,
        scratch_shapes=[
            pltpu.VMEM((4, 16, KEY_PART, 2 * HEAD_DIM), jnp.bfloat16),
            pltpu.VMEM((2, GROUP_HEADS, Q_ROWS, HEAD_DIM), jnp.float32),
            pltpu.VMEM((2, GROUP_HEADS, Q_ROWS, 2 * HEAD_DIM), jnp.float32),
            pltpu.SemaphoreType.DMA((20,)),
        ],
        compiler_params=params(28),
        cost_estimate=cost(27_000_000_000, 10_000_000, 26_000_000),
        name="attention",
    )(items, kpos, query_pair, *shaped)


def projection_kernel(first, groups, w_ref, *refs):
    pieces = refs[:10]
    if first:
        w_all = w_ref
        out_ref, rows_ref, done_ref, sems, w_sems, out_sem = refs[-6:]
    else:
        out_ref, w_all, rows_ref, done_ref, sems, w_sems, out_sem = refs[-7:]
    copies = []
    for core in range(2):
        for number in range(4):
            at = (core * 4 + number) * GROUP_WIDTH
            for side in range(0 if first else 2):
                copies.append(
                    pltpu.make_async_copy(
                        w_ref.at[groups[core * 4 + number], side],
                        w_all.at[pl.ds(at, GROUP_WIDTH), pl.ds(side * GROUP_WIDTH, GROUP_WIDTH)],
                        w_sems.at[(core * 4 + number) * 2 + side],
                    )
                )
        for number in range(5):
            at = (core * 4 + min(number, 3)) * GROUP_WIDTH
            source = pieces[core * 5 + number]
            low = 256 if number == 4 else 0
            copies.append(
                pltpu.make_async_copy(
                    source,
                    rows_ref.at[pl.ds(low, source.shape[0]), pl.ds(at, GROUP_WIDTH)],
                    sems.at[core * 5 + number],
                )
            )
    for copy in copies:
        copy.start()
    for copy in copies:
        copy.wait()
    for tile in range(Q_ROWS // Q_TILE):
        total = jnp.dot(
            rows_ref[tile * Q_TILE : (tile + 1) * Q_TILE, :],
            w_all[...],
            preferred_element_type=jnp.float32,
        )
        done_ref[tile * 2 : (tile + 1) * 2] = total.astype(jnp.bfloat16).reshape(
            2, TOK_DEV, 2 * GROUP_WIDTH
        )
    out = pltpu.make_async_copy(done_ref, out_ref.at[pl.ds(first, 4)], out_sem)
    out.start()
    out.wait()


def projection(first, groups, weights, pieces, before):
    more = [] if before is None else [before]
    out = jax.ShapeDtypeStruct((8, TOK_DEV, 2 * GROUP_WIDTH), jnp.bfloat16)
    arranged = jax.ShapeDtypeStruct((8 * GROUP_WIDTH, 2 * GROUP_WIDTH), jnp.bfloat16)
    return pl.pallas_call(
        functools.partial(projection_kernel, first),
        out_shape=out if more else (out, arranged),
        in_specs=[SMEM] + [VMEM if more else ANY] + [ANY] * (10 + len(more)),
        out_specs=ANY if more else (ANY, VMEM),
        scratch_shapes=[
            pltpu.VMEM((Q_ROWS, 8 * GROUP_WIDTH), jnp.bfloat16),
            pltpu.VMEM((4, TOK_DEV, 2 * GROUP_WIDTH), jnp.bfloat16),
            pltpu.SemaphoreType.DMA((10,)),
            pltpu.SemaphoreType.DMA((16,)),
            pltpu.SemaphoreType.DMA,
        ],
        input_output_aliases={12: 0} if more else {},
        compiler_params=params(16),
        cost_estimate=cost(2_500_000_000, 9_000_000),
        name="projection",
    )(groups, weights, *pieces, *more)


def slot_tables(ids_t):
    expert = lax.broadcasted_iota(jnp.int32, (EXPERTS, TOK_DEV), 0)
    first = (expert == ids_t[0:1, :]).astype(jnp.float32)
    second = (expert == ids_t[1:2, :]).astype(jnp.float32)
    member = first + second
    before = (
        lax.broadcasted_iota(jnp.int32, (TOK_DEV, TOK_DEV), 0)
        < lax.broadcasted_iota(jnp.int32, (TOK_DEV, TOK_DEV), 1)
    ).astype(jnp.bfloat16)
    slot = jnp.dot(member.astype(jnp.bfloat16), before, preferred_element_type=jnp.float32)
    return first, second, member, slot


def dispatch_kernel(ids_ref, update_ref, residual_ref, gain_ref, router_ref, send_ref, mix_ref, normed_ref):
    squares = jnp.zeros((TOK_DEV, 1), jnp.float32)
    for half in range(2):
        for group in range(BLOCKS):
            at = half * HALF + group * BLOCK_WIDTH
            row = residual_ref[:, at : at + BLOCK_WIDTH].astype(jnp.float32) + update_ref[
                group, :, half * BLOCK_WIDTH : (half + 1) * BLOCK_WIDTH
            ].astype(jnp.float32)
            squares = squares + jnp.sum(row * row, axis=1, keepdims=True)
    factor = lax.rsqrt(squares / D + EPS)
    for half in range(2):
        for group in range(BLOCKS):
            at = half * HALF + group * BLOCK_WIDTH
            row = residual_ref[:, at : at + BLOCK_WIDTH].astype(jnp.float32) + update_ref[
                group, :, half * BLOCK_WIDTH : (half + 1) * BLOCK_WIDTH
            ].astype(jnp.float32)
            gain = gain_ref[:, at : at + BLOCK_WIDTH].astype(jnp.float32)
            normed_ref[:, at : at + BLOCK_WIDTH] = (row * factor * gain).astype(jnp.bfloat16)
    first, second, member, slot = slot_tables(ids_ref[...])
    slot_ids = lax.broadcasted_iota(jnp.int32, (SLOTS, TOK_DEV), 0).astype(jnp.float32)
    picks, tails = [], []
    last = jnp.where(slot == float(SLOTS), member, 0.0)
    for expert in range(EXPERTS):
        picks.append(
            jnp.where(slot[expert : expert + 1, :] == slot_ids, member[expert : expert + 1, :], 0.0)
        )
        tails.append(jnp.broadcast_to(last[expert : expert + 1, :], (BLOCKS, TOK_DEV)))
    pick = jnp.concatenate(picks, axis=0)
    tail = jnp.concatenate(tails, axis=0)
    tail_block = lax.broadcasted_iota(jnp.int32, (EXPERTS * BLOCKS, TOK_DEV), 0) % BLOCKS
    pick_low = pick.astype(jnp.bfloat16)
    for half in range(2):
        tail_rows = None
        for block in range(BLOCKS):
            at = half * HALF + block * BLOCK_WIDTH
            rows = normed_ref[:, at : at + BLOCK_WIDTH]
            moved = jnp.dot(pick_low, rows, preferred_element_type=jnp.float32).astype(jnp.bfloat16)
            for expert in range(EXPERTS):
                send_ref[2 * expert + half, block * SLOTS : (block + 1) * SLOTS, :] = moved[
                    expert * SLOTS : (expert + 1) * SLOTS, :
                ]
            chosen = jnp.where(tail_block == block, tail, 0.0).astype(jnp.bfloat16)
            term = jnp.dot(chosen, rows, preferred_element_type=jnp.float32)
            tail_rows = term if tail_rows is None else tail_rows + term
        tail_rows = tail_rows.astype(jnp.bfloat16)
        for expert in range(EXPERTS):
            send_ref[2 * expert + half, BLOCKS * SLOTS :, :] = tail_rows[
                expert * BLOCKS : (expert + 1) * BLOCKS, :
            ]
    logits = lax.dot_general(
        router_ref[...],
        normed_ref[...],
        (((1,), (1,)), ((), ())),
        preferred_element_type=jnp.float32,
    )
    chosen_first = jnp.sum(first * logits, axis=0, keepdims=True)
    chosen_second = jnp.sum(second * logits, axis=0, keepdims=True)
    mix_first = 1.0 / (1.0 + jnp.exp(chosen_second - chosen_first))
    mix_second = 1.0 / (1.0 + jnp.exp(chosen_first - chosen_second))
    share = first * mix_first + second * mix_second
    for expert in range(EXPERTS):
        mine = share[expert : expert + 1, :]
        mix_ref[expert * SLOTS : (expert + 1) * SLOTS, :] = picks[expert] * mine
        mix_ref[
            EXPERTS * SLOTS + expert * BLOCKS : EXPERTS * SLOTS + (expert + 1) * BLOCKS, :
        ] = tails[expert] * mine


def dispatch(ids_t, update, residual, gain, router_t):
    return pl.pallas_call(
        dispatch_kernel,
        out_shape=(
            jax.ShapeDtypeStruct((16, BLOCKS * (SLOTS + 1), BLOCK_WIDTH), jnp.bfloat16),
            jax.ShapeDtypeStruct((EXPERTS * (SLOTS + BLOCKS), TOK_DEV), jnp.float32),
        ),
        in_specs=[VMEM] * 5,
        out_specs=(VMEM, VMEM),
        scratch_shapes=[pltpu.VMEM((TOK_DEV, D), jnp.bfloat16)],
        compiler_params=params(32),
        cost_estimate=cost(800_000_000, 8_000_000),
        name="dispatch",
    )(ids_t, update, residual, gain, router_t)


PARTS = SLOTS // PART
ROWS = 16 * SLOTS
ALL_ROWS = ROWS + 16
GROUPS = 4
GROUP_DEPTH = HALF // GROUPS


def row_pick(block):
    source = lax.broadcasted_iota(jnp.int32, (16, 16 * BLOCKS), 0)
    place = lax.broadcasted_iota(jnp.int32, (16, 16 * BLOCKS), 1)
    return (place == source * BLOCKS + block).astype(jnp.bfloat16)


def first_kernel(rows_ref, u_ref, low_ref, x_ref, tail_ref, w_ref, acc_ref, sems, row_sems):
    copies = []
    for group in range(GROUPS):
        rows = pl.ds(group * GROUP_DEPTH, GROUP_DEPTH)
        copies.append(pltpu.make_async_copy(u_ref.at[0, rows], w_ref.at[rows], sems.at[group]))
    moves = [
        pltpu.make_async_copy(
            rows_ref.at[:, pl.ds(BLOCKS * SLOTS, BLOCKS), :], tail_ref, row_sems.at[2 * BLOCKS]
        )
    ]
    for block in range(BLOCKS):
        for part in range(PARTS):
            moves.append(
                pltpu.make_async_copy(
                    rows_ref.at[:, pl.ds(block * SLOTS + part * PART, PART), :],
                    x_ref.at[pl.ds(part * 16, 16), :, pl.ds(block * BLOCK_WIDTH, BLOCK_WIDTH)],
                    row_sems.at[block * PARTS + part],
                )
            )
    for move in moves[: 1 + 2 * PARTS]:
        move.start()
    copies[0].start()
    for move in moves[1 + 2 * PARTS :]:
        move.start()
    for copy in copies[1:]:
        copy.start()
    moves[0].wait()
    tail = tail_ref[...].reshape(16 * BLOCKS, BLOCK_WIDTH)
    for block in range(BLOCKS):
        picked = jnp.dot(row_pick(block), tail, preferred_element_type=jnp.float32)
        x_ref[2 * 16, :, block * BLOCK_WIDTH : (block + 1) * BLOCK_WIDTH] = picked.astype(
            jnp.bfloat16
        )
    each = BLOCKS // GROUPS * PARTS
    for group in range(GROUPS):
        at = group * GROUP_DEPTH
        for move in moves[1 + group * each : 1 + (group + 1) * each]:
            move.wait()
        copies[group].wait()
        rows = x_ref[:, :, at : at + GROUP_DEPTH].reshape(ALL_ROWS, GROUP_DEPTH)
        term = jnp.dot(rows, w_ref[at : at + GROUP_DEPTH, :], preferred_element_type=jnp.float32)
        if group == 0:
            acc_ref[...] = term
        elif group < GROUPS - 1:
            acc_ref[...] += term
        else:
            low_ref[...] = (acc_ref[...] + term).astype(jnp.bfloat16)


def first_factor(received, u_gate_up):
    return pl.pallas_call(
        first_kernel,
        out_shape=jax.ShapeDtypeStruct((ALL_ROWS, 2 * RANK), jnp.bfloat16),
        in_specs=[ANY, ANY],
        out_specs=VMEM,
        scratch_shapes=[
            pltpu.VMEM((16 * PARTS + 1, PART, HALF), jnp.bfloat16),
            pltpu.VMEM((16, BLOCKS, BLOCK_WIDTH), jnp.bfloat16),
            pltpu.VMEM((HALF, 2 * RANK), jnp.bfloat16),
            pltpu.VMEM((ALL_ROWS, 2 * RANK), jnp.float32),
            pltpu.SemaphoreType.DMA((GROUPS,)),
            pltpu.SemaphoreType.DMA((BLOCKS * PARTS + 1,)),
        ],
        compiler_params=params(58),
        cost_estimate=cost(3_400_000_000, 9_000_000),
        name="first_factor",
    )(received, u_gate_up)


FF_TILE = 512
FF_STEPS = FF_PIECE // FF_TILE


def middle_kernel(own_ref, got_ref, v_ref, u_ref, low_ref, rank_ref, vs_ref, us_ref, acc_ref, sems):
    copies = []
    for step in range(FF_STEPS):
        columns = pl.ds(step * FF_TILE, FF_TILE)
        copies.append(
            (
                pltpu.make_async_copy(
                    v_ref.at[0, :, :, columns], vs_ref.at[:, :, columns], sems.at[2 * step]
                ),
                pltpu.make_async_copy(
                    u_ref.at[0, columns, :], us_ref.at[columns, :], sems.at[2 * step + 1]
                ),
            )
        )
    for pair in copies:
        for copy in pair:
            copy.start()
    rank_ref[...] = (
        own_ref[...].astype(jnp.float32) + got_ref[...].astype(jnp.float32)
    ).astype(jnp.bfloat16)
    for step in range(FF_STEPS):
        columns = slice(step * FF_TILE, (step + 1) * FF_TILE)
        for copy in copies[step]:
            copy.wait()
        gate = jnp.dot(rank_ref[:, :RANK], vs_ref[0, :, columns], preferred_element_type=jnp.float32)
        up = jnp.dot(rank_ref[:, RANK:], vs_ref[1, :, columns], preferred_element_type=jnp.float32)
        low = 0.5 * gate
        hidden = ((low + low * jnp.tanh(low)) * up).astype(jnp.bfloat16)
        term = jnp.dot(hidden, us_ref[columns, :], preferred_element_type=jnp.float32)
        if step == 0:
            acc_ref[...] = term
        elif step < FF_STEPS - 1:
            acc_ref[...] += term
        else:
            low_ref[...] = (acc_ref[...] + term).astype(jnp.bfloat16)


def middle(own, got, v_gate_up, u_down):
    return pl.pallas_call(
        middle_kernel,
        out_shape=jax.ShapeDtypeStruct((ALL_ROWS, RANK), jnp.bfloat16),
        in_specs=[VMEM, VMEM, ANY, ANY],
        out_specs=VMEM,
        scratch_shapes=[
            pltpu.VMEM((ALL_ROWS, 2 * RANK), jnp.bfloat16),
            pltpu.VMEM((2, RANK, FF_PIECE), jnp.bfloat16),
            pltpu.VMEM((FF_PIECE, RANK), jnp.bfloat16),
            pltpu.VMEM((ALL_ROWS, RANK), jnp.float32),
            pltpu.SemaphoreType.DMA((2 * FF_STEPS,)),
        ],
        compiler_params=params(60),
        cost_estimate=cost(6_700_000_000, 14_000_000, 2_200_000),
        name="middle",
    )(own, got, v_gate_up, u_down)


def last_kernel(own_ref, got_ref, v_ref, out_ref, down_ref, w_ref, sems):
    copies = []
    for block in range(BLOCKS):
        columns = pl.ds(block * BLOCK_WIDTH, BLOCK_WIDTH)
        copies.append(
            pltpu.make_async_copy(v_ref.at[0, :, columns], w_ref.at[:, columns], sems.at[block])
        )
    for copy in copies:
        copy.start()
    down_ref[...] = (
        own_ref[...].astype(jnp.float32) + got_ref[...].astype(jnp.float32)
    ).astype(jnp.bfloat16)
    total = None
    place = lax.broadcasted_iota(jnp.int32, (16 * BLOCKS, 16), 0)
    source = lax.broadcasted_iota(jnp.int32, (16 * BLOCKS, 16), 1)
    for block in range(BLOCKS):
        copies[block].wait()
        weights = w_ref[:, block * BLOCK_WIDTH : (block + 1) * BLOCK_WIDTH]
        spread = (place == source * BLOCKS + block).astype(jnp.bfloat16)
        lifted = jnp.dot(spread, down_ref[ROWS:, :], preferred_element_type=jnp.float32)
        rows = jnp.concatenate([down_ref[:ROWS, :], lifted.astype(jnp.bfloat16)], axis=0)
        result = jnp.dot(rows, weights, preferred_element_type=jnp.float32)
        main = result[:ROWS].astype(jnp.bfloat16).reshape(PARTS, 16, PART, BLOCK_WIDTH)
        for part in range(PARTS):
            at = block * SLOTS + part * PART
            out_ref[:, at : at + PART, :] = main[part]
        total = result[ROWS:] if total is None else total + result[ROWS:]
    out_ref[:, BLOCKS * SLOTS :, :] = total.astype(jnp.bfloat16).reshape(16, BLOCKS, BLOCK_WIDTH)


def last_factor(own, got, v_down):
    return pl.pallas_call(
        last_kernel,
        out_shape=jax.ShapeDtypeStruct((16, BLOCKS * (SLOTS + 1), BLOCK_WIDTH), jnp.bfloat16),
        in_specs=[VMEM, VMEM, ANY],
        out_specs=VMEM,
        scratch_shapes=[
            pltpu.VMEM((ALL_ROWS, RANK), jnp.bfloat16),
            pltpu.VMEM((RANK, HALF), jnp.bfloat16),
            pltpu.SemaphoreType.DMA((BLOCKS,)),
        ],
        compiler_params=params(24),
        cost_estimate=cost(1_700_000_000, 6_000_000),
        name="last_factor",
    )(own, got, v_down)


def combine_kernel(mix_ref, update_ref, residual_ref, back_ref, out_ref):
    mix = mix_ref[: EXPERTS * SLOTS, :].T
    tail = mix_ref[EXPERTS * SLOTS :, :].T
    mix_high = mix.astype(jnp.bfloat16)
    mix_low = (mix - mix_high.astype(jnp.float32)).astype(jnp.bfloat16)
    tail_block = lax.broadcasted_iota(jnp.int32, (TOK_DEV, EXPERTS * BLOCKS), 1) % BLOCKS
    for half in range(2):
        tail_rows = jnp.concatenate(
            [back_ref[2 * expert + half, BLOCKS * SLOTS :, :] for expert in range(EXPERTS)], axis=0
        )
        for block in range(BLOCKS):
            rows = jnp.concatenate(
                [
                    back_ref[2 * expert + half, block * SLOTS : (block + 1) * SLOTS, :]
                    for expert in range(EXPERTS)
                ],
                axis=0,
            )
            here = jnp.where(tail_block == block, tail, 0.0)
            here_high = here.astype(jnp.bfloat16)
            here_low = (here - here_high.astype(jnp.float32)).astype(jnp.bfloat16)
            mixture = jnp.dot(mix_high, rows, preferred_element_type=jnp.float32)
            mixture = mixture + jnp.dot(mix_low, rows, preferred_element_type=jnp.float32)
            mixture = mixture + jnp.dot(here_high, tail_rows, preferred_element_type=jnp.float32)
            mixture = mixture + jnp.dot(here_low, tail_rows, preferred_element_type=jnp.float32)
            at = half * HALF + block * BLOCK_WIDTH
            stream = residual_ref[:, at : at + BLOCK_WIDTH].astype(jnp.float32) + update_ref[
                block, :, half * BLOCK_WIDTH : (half + 1) * BLOCK_WIDTH
            ].astype(jnp.float32)
            out_ref[:, at : at + BLOCK_WIDTH] = (stream + mixture).astype(jnp.bfloat16)


def combine(mix, update, residual, back):
    return pl.pallas_call(
        combine_kernel,
        out_shape=jax.ShapeDtypeStruct((TOK_DEV, D), jnp.bfloat16),
        in_specs=[VMEM] * 4,
        out_specs=VMEM,
        compiler_params=params(32),
        cost_estimate=cost(1_000_000_000, 8_000_000),
        name="combine",
    )(mix, update, residual, back)


def per_device(
    queries,
    keys,
    values,
    residual,
    proj_weight,
    norm_gain,
    router,
    expert_ids,
    u_gate_up,
    v_gate_up,
    u_down,
    v_down,
):
    zh, x, zl = lax.axis_index("zh"), lax.axis_index("x"), lax.axis_index("zl")
    y, c = lax.axis_index("y"), lax.axis_index("c")
    z = zh * 2 + zl
    chunk = zh * 8 + x * 2 + zl

    pairs = [
        (p * 4 + row, (15 - p if row >= 2 else p) * 4 + row)
        for p in range(16)
        for row in range(4)
    ]
    q = lax.ppermute(queries, PLANE + ("y",), pairs)
    kv = pack_kv(keys, values)
    kv = lax.all_to_all(kv, "y", split_axis=0, concat_axis=0, tiled=True)
    kv = kv.reshape(4 * TOK_DEV, 2 * HEAD_DIM)
    early, late = kv[:256], kv[256:]

    copies = jnp.broadcast_to(proj_weight[None], (16, GROUP_WIDTH, GROUP_WIDTH))
    q = pack_q(q)
    q = lax.all_to_all(q, GROUP, split_axis=0, concat_axis=0, tiled=True)
    query_pair = q.reshape(2, Q_ROWS, GROUP_WIDTH)

    def joined(pieces):
        return jnp.concatenate(pieces, axis=0)

    early = joined(direct_pieces(early, Z))
    late = joined(direct_pieces(late, "x"))
    own = ring_pieces(early, "x") + ring_pieces(late, Z)
    swapped = [other_core(p) for p in own]

    far_chunk = 15 - chunk
    order = jnp.arange(15, dtype=jnp.int32)
    is_far = order >= chunk
    slot_list = jnp.concatenate([is_far.astype(jnp.int32), jnp.array([0, 1], jnp.int32)])
    chunk_list = jnp.concatenate(
        [jnp.where(is_far, order - chunk, order), jnp.stack([chunk, far_chunk])]
    )
    there_z = chunk_list // 8 * 2 + chunk_list % 2
    there_x = chunk_list // 2 % 4
    rel_z = relative(z, there_z)
    rel_x = relative(x, there_x)
    rows = jnp.stack([slot_list, rel_x * 4 + rel_z, rel_z * 4 + rel_x], axis=1)
    items = jnp.concatenate([jnp.array([15, 2], jnp.int32), rows.reshape(-1)]).astype(jnp.int32)
    key_ids = jnp.arange(KEY_PART, dtype=jnp.int32)
    base = key_ids // TOK_DEV * 256 + key_ids % TOK_DEV
    kpos = jnp.stack(
        [
            base + c * TOK_DEV,
            base + c * TOK_DEV + 512,
            base + (1 - c) * TOK_DEV,
            base + (1 - c) * TOK_DEV + 512,
        ]
    ).astype(jnp.int32)

    attended = attention(items, kpos, query_pair, own + swapped)
    weight_rows = lax.all_to_all(copies, PLANE, split_axis=0, concat_axis=0, tiled=True)
    weight_rows = weight_rows.reshape(8, 2, GROUP_WIDTH, GROUP_WIDTH)
    from_y = jnp.stack([y, (y - 1) % 4, (y + 1) % 4, (y + 2) % 4])
    groups = jnp.concatenate([from_y * 2 + c, from_y * 2 + 1 - c]).astype(jnp.int32)
    near = ring_pieces(attended[0], "y")
    far = mirrored(attended[1])
    near = near + [other_core(p) for p in near]
    far = ring_pieces(far, "y")
    far = far + [other_core(p) for p in far]
    projected, arranged = projection(0, groups, weight_rows, near, None)
    projected = projection(4, groups, arranged, far, projected)
    update = lax.all_to_all(projected, GROUP, split_axis=0, concat_axis=0, tiled=True)

    ids_t = expert_ids.T
    send, mix = dispatch(ids_t, update, residual, norm_gain.reshape(1, D), router.T)
    received = lax.all_to_all(send, EXP, split_axis=0, concat_axis=0, tiled=True)
    rank_low = first_factor(received, u_gate_up)
    down_low = middle(rank_low, other_core(rank_low), v_gate_up, u_down)
    out_rows = last_factor(down_low, other_core(down_low), v_down)
    back = lax.all_to_all(out_rows, EXP, split_axis=0, concat_axis=0, tiled=True)
    return combine(mix, update, residual, back)


def solution(mesh):
    fine = Mesh(mesh.devices.reshape(2, 4, 2, 4, 2), ("zh", "x", "zl", "y", "c"))
    seq, exp = ("zh", "x"), ("zl", "y", "c")
    in_specs = (
        P(seq + exp, None),
        P(seq + exp, None),
        P(seq + exp, None),
        P(seq + exp, None),
        P(seq, exp),
        P(),
        P(),
        P(seq + exp, None),
        P(exp, None, None),
        P(exp, None, None, None),
        P(exp, None, None),
        P(exp, None, None),
    )

    return jax.shard_map(
        per_device, mesh=fine, in_specs=in_specs, out_specs=P(seq + exp, None), check_vma=False
    )
```

```python
import functools

import jax
import jax.numpy as jnp
from jax import lax
from jax.experimental import pallas as pl
from jax.experimental.pallas import tpu as pltpu
from jax.sharding import Mesh
from jax.sharding import PartitionSpec as P


D = 6144
HEAD_DIM = 128
GROUP_HEADS = 3
GROUP_WIDTH = GROUP_HEADS * HEAD_DIM
EXPERTS = 8
RANK = 512
FF_PIECE = 4096
TOK_DEV = 128
HALF_TOK = TOK_DEV // 2
HALF = D // 2
BLOCKS = 8
BLOCK_WIDTH = HALF // BLOCKS
SLOTS = 32
PART = 16
EPS = 1e-05
SCALE = HEAD_DIM**-0.5 * 1.4426950408889634
LOW = -1e30
Q_ROWS = 512
Q_TILE = 256
KEY_PART = 256
SOURCES = Q_TILE // HALF_TOK

Z = ("zh", "zl")
PLANE = ("zh", "x", "zl")
GROUP = ("y", "c")
EXP = ("zl", "y", "c")


VMEM = pl.BlockSpec(memory_space=pltpu.VMEM)
SMEM = pl.BlockSpec(memory_space=pltpu.SMEM)
ANY = pl.BlockSpec(memory_space=pl.ANY)
HBM = pl.BlockSpec(memory_space=pltpu.HBM)


def params(mib=48, **more):
    return pltpu.CompilerParams(vmem_limit_bytes=mib << 20, **more)


def cost(flops, moved, transcendentals=0):
    return pl.CostEstimate(flops=flops, bytes_accessed=moved, transcendentals=transcendentals)


def shifted(value, axis, step):
    return lax.ppermute(value, axis, [(i, (i + step) % 4) for i in range(4)])


def other_core(value):
    return lax.ppermute(value, "c", [(0, 1), (1, 0)])


def mirrored(value):
    return lax.ppermute(value, PLANE, [(i, 15 - i) for i in range(16)])


def ring_pieces(value, axis):
    half = value.shape[0] // 2
    up = shifted(value, axis, 1)
    down = shifted(value, axis, -1)
    far_up = shifted(up[:half], axis, 1)
    far_down = shifted(down[half:], axis, -1)
    return [value, up, down, far_up, far_down]


def relative(mine, theirs):
    gap = (mine - theirs) % 4
    return jnp.where(gap == 3, 2, jnp.where(gap == 2, 3, gap))


def direct_pieces(value, axis):
    return [value] + [shifted(value, axis, step) for step in (1, -1, 2)]


def pack_kernel(*refs):
    sources, out_ref, sems = refs[:-2], refs[-2], refs[-1]
    count, width = out_ref.shape[0], out_ref.shape[2] // len(sources)
    copies = []
    for place in range(count):
        for number, source in enumerate(sources):
            copies.append(
                pltpu.make_async_copy(
                    source.at[:, pl.ds(place * width, width)],
                    out_ref.at[place, :, pl.ds(number * width, width)],
                    sems.at[place * len(sources) + number],
                )
            )
    for copy in copies:
        copy.start()
    for copy in copies:
        copy.wait()


def packed(sources, shape):
    return pl.pallas_call(
        pack_kernel,
        out_shape=jax.ShapeDtypeStruct(shape, jnp.bfloat16),
        in_specs=[ANY] * len(sources),
        out_specs=VMEM,
        scratch_shapes=[pltpu.SemaphoreType.DMA((shape[0] * len(sources),))],
        compiler_params=params(8),
        cost_estimate=cost(1_000_000_000, 2_000_000),
        name="pack",
    )(*sources)


def pack_kv(keys, values):
    return packed((keys, values), (4, TOK_DEV, 2 * HEAD_DIM))


def pack_q_kernel(near_ref, far_ref, out_ref, sems):
    copies = []
    for place in range(8):
        columns = pl.ds(place * GROUP_WIDTH, GROUP_WIDTH)
        for slot, source in enumerate((near_ref, far_ref)):
            copies.append(
                pltpu.make_async_copy(
                    source.at[pl.ds(0, HALF_TOK), columns],
                    out_ref.at[place, pl.ds(slot * HALF_TOK, HALF_TOK), :],
                    sems.at[place * 2 + slot],
                )
            )
    for copy in copies:
        copy.start()
    for copy in copies:
        copy.wait()


def pack_q(queries, far):
    return pl.pallas_call(
        pack_q_kernel,
        out_shape=jax.ShapeDtypeStruct((8, TOK_DEV, GROUP_WIDTH), jnp.bfloat16),
        in_specs=[ANY, ANY],
        out_specs=VMEM,
        scratch_shapes=[pltpu.SemaphoreType.DMA((16,))],
        compiler_params=params(8),
        cost_estimate=cost(1_000_000_000, 2_000_000),
        name="pack_q",
    )(queries, far)


def attention_kernel(items, kpos_ref, q_ref, *refs):
    pieces = refs[:20]
    out_ref = refs[20]
    kv_ref, max_ref, acc_ref, sems = refs[21:]
    copies = []
    for which in range(4):
        for number in range(5):
            source = pieces[which * 5 + number]
            if number < 3:
                target = kv_ref.at[which, pl.ds(number * 4, 4)]
            else:
                target = kv_ref.at[which, pl.ds(12 + (number - 3) * 2, 2)]
            copies.append(pltpu.make_async_copy(source, target, sems.at[which * 5 + number]))
    for copy in copies:
        copy.start()
    max_ref[...] = jnp.full(max_ref.shape, LOW, jnp.float32)
    acc_ref[...] = jnp.zeros(acc_ref.shape, jnp.float32)
    for copy in copies:
        copy.wait()

    def work(slot, at, masked):
        keys, values = [], []
        ones = jnp.ones((KEY_PART, HEAD_DIM), jnp.bfloat16)
        for which in range(4):
            block = at[which % 2]
            keys.append(kv_ref[which, block, :, 0:HEAD_DIM])
            value = kv_ref[which, block, :, HEAD_DIM : 2 * HEAD_DIM]
            values.append(jnp.concatenate([value, ones], axis=1))
        for tile in range(Q_ROWS // Q_TILE):
            rows = pl.ds(tile * Q_TILE, Q_TILE)
            for head in range(GROUP_HEADS):
                query = q_ref[
                    pl.ds(tile * SOURCES, SOURCES),
                    pl.ds(pl.multiple_of(slot * HALF_TOK, HALF_TOK), HALF_TOK),
                    head * HEAD_DIM : (head + 1) * HEAD_DIM,
                ].reshape(Q_TILE, HEAD_DIM)
                scores = []
                for which in range(4):
                    part = lax.dot_general(
                        query,
                        keys[which],
                        (((1,), (1,)), ((), ())),
                        preferred_element_type=jnp.float32,
                    )
                    if masked:
                        row = lax.broadcasted_iota(jnp.int32, (Q_TILE, KEY_PART), 0)
                        row_pos = (
                            (tile * SOURCES + row // HALF_TOK) * TOK_DEV
                            + slot * HALF_TOK
                            + row % HALF_TOK
                        )
                        part = jnp.where(kpos_ref[which : which + 1, :] <= row_pos, part, LOW)
                    scores.append(part)
                highest = jnp.maximum(
                    jnp.maximum(scores[0], scores[1]), jnp.maximum(scores[2], scores[3])
                )
                old_max = max_ref[slot, head, rows, :]
                new_max = jnp.maximum(old_max, jnp.max(highest, axis=1, keepdims=True))
                level = jnp.tile(new_max * SCALE, (1, KEY_PART // HEAD_DIM))
                update = None
                for which in range(4):
                    weights = jnp.exp2(scores[which] * SCALE - level).astype(jnp.bfloat16)
                    term = jnp.dot(weights, values[which], preferred_element_type=jnp.float32)
                    update = term if update is None else update + term
                fading = jnp.exp2((old_max - new_max) * SCALE)
                max_ref[slot, head, rows, :] = new_max
                acc_ref[slot, head, rows, 0:HEAD_DIM] = (
                    acc_ref[slot, head, rows, 0:HEAD_DIM] * fading + update[:, :HEAD_DIM]
                )
                acc_ref[slot, head, rows, HEAD_DIM:] = (
                    acc_ref[slot, head, rows, HEAD_DIM:] * fading + update[:, HEAD_DIM:]
                )

    open_count = items[0]
    masked_count = items[1]

    def open_step(number, carry):
        at = 2 + 3 * number
        work(items[at], (items[at + 1], items[at + 2]), False)
        return carry

    def masked_step(number, carry):
        at = 2 + 3 * (open_count + number)
        work(items[at], (items[at + 1], items[at + 2]), True)
        return carry

    lax.fori_loop(0, open_count, open_step, 0)
    lax.fori_loop(0, masked_count, masked_step, 0)
    for slot in range(2):
        for head in range(GROUP_HEADS):
            out_ref[slot, :, head * HEAD_DIM : (head + 1) * HEAD_DIM] = (
                acc_ref[slot, head, :, 0:HEAD_DIM] / acc_ref[slot, head, :, HEAD_DIM:]
            ).astype(jnp.bfloat16)


def attention(items, kpos, query_pair, pieces):
    shaped = [p.reshape(-1, KEY_PART, 2 * HEAD_DIM) for p in pieces]
    return pl.pallas_call(
        attention_kernel,
        out_shape=jax.ShapeDtypeStruct((2, Q_ROWS, GROUP_WIDTH), jnp.bfloat16),
        in_specs=[SMEM, VMEM, VMEM] + [ANY] * 20,
        out_specs=VMEM,
        scratch_shapes=[
            pltpu.VMEM((4, 16, KEY_PART, 2 * HEAD_DIM), jnp.bfloat16),
            pltpu.VMEM((2, GROUP_HEADS, Q_ROWS, HEAD_DIM), jnp.float32),
            pltpu.VMEM((2, GROUP_HEADS, Q_ROWS, 2 * HEAD_DIM), jnp.float32),
            pltpu.SemaphoreType.DMA((20,)),
        ],
        compiler_params=params(28),
        cost_estimate=cost(27_000_000_000, 10_000_000, 26_000_000),
        name="attention",
    )(items, kpos, query_pair, *shaped)


def projection_kernel(first, groups, w_ref, *refs):
    pieces = refs[:10]
    if first:
        w_all = w_ref
        out_ref, rows_ref, done_ref, sems, w_sems, out_sem = refs[-6:]
    else:
        out_ref, w_all, rows_ref, done_ref, sems, w_sems, out_sem = refs[-7:]
    copies = []
    for core in range(2):
        for number in range(4):
            at = (core * 4 + number) * GROUP_WIDTH
            for side in range(0 if first else 2):
                copies.append(
                    pltpu.make_async_copy(
                        w_ref.at[groups[core * 4 + number], side],
                        w_all.at[pl.ds(at, GROUP_WIDTH), pl.ds(side * GROUP_WIDTH, GROUP_WIDTH)],
                        w_sems.at[(core * 4 + number) * 2 + side],
                    )
                )
        for number in range(5):
            at = (core * 4 + min(number, 3)) * GROUP_WIDTH
            source = pieces[core * 5 + number]
            low = 256 if number == 4 else 0
            copies.append(
                pltpu.make_async_copy(
                    source,
                    rows_ref.at[pl.ds(low, source.shape[0]), pl.ds(at, GROUP_WIDTH)],
                    sems.at[core * 5 + number],
                )
            )
    for copy in copies:
        copy.start()
    for copy in copies:
        copy.wait()
    for tile in range(Q_ROWS // Q_TILE):
        total = jnp.dot(
            rows_ref[tile * Q_TILE : (tile + 1) * Q_TILE, :],
            w_all[...],
            preferred_element_type=jnp.float32,
        )
        done_ref[tile * SOURCES : (tile + 1) * SOURCES] = total.astype(jnp.bfloat16).reshape(
            SOURCES, HALF_TOK, 2 * GROUP_WIDTH
        )
    out = pltpu.make_async_copy(done_ref, out_ref.at[:, pl.ds(first, HALF_TOK), :], out_sem)
    out.start()
    out.wait()


def projection(first, groups, weights, pieces, before):
    more = [] if before is None else [before]
    out = jax.ShapeDtypeStruct((8, TOK_DEV, 2 * GROUP_WIDTH), jnp.bfloat16)
    arranged = jax.ShapeDtypeStruct((8 * GROUP_WIDTH, 2 * GROUP_WIDTH), jnp.bfloat16)
    return pl.pallas_call(
        functools.partial(projection_kernel, first),
        out_shape=out if more else (out, arranged),
        in_specs=[SMEM] + [VMEM if more else ANY] + [ANY] * (10 + len(more)),
        out_specs=ANY if more else (ANY, VMEM),
        scratch_shapes=[
            pltpu.VMEM((Q_ROWS, 8 * GROUP_WIDTH), jnp.bfloat16),
            pltpu.VMEM((8, HALF_TOK, 2 * GROUP_WIDTH), jnp.bfloat16),
            pltpu.SemaphoreType.DMA((10,)),
            pltpu.SemaphoreType.DMA((16,)),
            pltpu.SemaphoreType.DMA,
        ],
        input_output_aliases={12: 0} if more else {},
        compiler_params=params(16),
        cost_estimate=cost(2_500_000_000, 9_000_000),
        name="projection",
    )(groups, weights, *pieces, *more)


def slot_tables(ids_t):
    expert = lax.broadcasted_iota(jnp.int32, (EXPERTS, TOK_DEV), 0)
    first = (expert == ids_t[0:1, :]).astype(jnp.float32)
    second = (expert == ids_t[1:2, :]).astype(jnp.float32)
    member = first + second
    before = (
        lax.broadcasted_iota(jnp.int32, (TOK_DEV, TOK_DEV), 0)
        < lax.broadcasted_iota(jnp.int32, (TOK_DEV, TOK_DEV), 1)
    ).astype(jnp.bfloat16)
    slot = jnp.dot(member.astype(jnp.bfloat16), before, preferred_element_type=jnp.float32)
    return first, second, member, slot


def dispatch_kernel(ids_ref, update_ref, residual_ref, gain_ref, router_ref, send_ref, mix_ref, normed_ref):
    squares = jnp.zeros((TOK_DEV, 1), jnp.float32)
    for half in range(2):
        for group in range(BLOCKS):
            at = half * HALF + group * BLOCK_WIDTH
            row = residual_ref[:, at : at + BLOCK_WIDTH].astype(jnp.float32) + update_ref[
                group, :, half * BLOCK_WIDTH : (half + 1) * BLOCK_WIDTH
            ].astype(jnp.float32)
            squares = squares + jnp.sum(row * row, axis=1, keepdims=True)
    factor = lax.rsqrt(squares / D + EPS)
    for half in range(2):
        for group in range(BLOCKS):
            at = half * HALF + group * BLOCK_WIDTH
            row = residual_ref[:, at : at + BLOCK_WIDTH].astype(jnp.float32) + update_ref[
                group, :, half * BLOCK_WIDTH : (half + 1) * BLOCK_WIDTH
            ].astype(jnp.float32)
            gain = gain_ref[:, at : at + BLOCK_WIDTH].astype(jnp.float32)
            normed_ref[:, at : at + BLOCK_WIDTH] = (row * factor * gain).astype(jnp.bfloat16)
    first, second, member, slot = slot_tables(ids_ref[...])
    slot_ids = lax.broadcasted_iota(jnp.int32, (SLOTS, TOK_DEV), 0).astype(jnp.float32)
    picks, tails = [], []
    last = jnp.where(slot == float(SLOTS), member, 0.0)
    for expert in range(EXPERTS):
        picks.append(
            jnp.where(slot[expert : expert + 1, :] == slot_ids, member[expert : expert + 1, :], 0.0)
        )
        tails.append(jnp.broadcast_to(last[expert : expert + 1, :], (BLOCKS, TOK_DEV)))
    pick = jnp.concatenate(picks, axis=0)
    tail = jnp.concatenate(tails, axis=0)
    tail_block = lax.broadcasted_iota(jnp.int32, (EXPERTS * BLOCKS, TOK_DEV), 0) % BLOCKS
    pick_low = pick.astype(jnp.bfloat16)
    for half in range(2):
        tail_rows = None
        for block in range(BLOCKS):
            at = half * HALF + block * BLOCK_WIDTH
            rows = normed_ref[:, at : at + BLOCK_WIDTH]
            moved = jnp.dot(pick_low, rows, preferred_element_type=jnp.float32).astype(jnp.bfloat16)
            for expert in range(EXPERTS):
                send_ref[2 * expert + half, block * SLOTS : (block + 1) * SLOTS, :] = moved[
                    expert * SLOTS : (expert + 1) * SLOTS, :
                ]
            chosen = jnp.where(tail_block == block, tail, 0.0).astype(jnp.bfloat16)
            term = jnp.dot(chosen, rows, preferred_element_type=jnp.float32)
            tail_rows = term if tail_rows is None else tail_rows + term
        tail_rows = tail_rows.astype(jnp.bfloat16)
        for expert in range(EXPERTS):
            send_ref[2 * expert + half, BLOCKS * SLOTS :, :] = tail_rows[
                expert * BLOCKS : (expert + 1) * BLOCKS, :
            ]
    logits = lax.dot_general(
        router_ref[...],
        normed_ref[...],
        (((1,), (1,)), ((), ())),
        preferred_element_type=jnp.float32,
    )
    chosen_first = jnp.sum(first * logits, axis=0, keepdims=True)
    chosen_second = jnp.sum(second * logits, axis=0, keepdims=True)
    mix_first = 1.0 / (1.0 + jnp.exp(chosen_second - chosen_first))
    mix_second = 1.0 / (1.0 + jnp.exp(chosen_first - chosen_second))
    share = first * mix_first + second * mix_second
    for expert in range(EXPERTS):
        mine = share[expert : expert + 1, :]
        mix_ref[expert * SLOTS : (expert + 1) * SLOTS, :] = picks[expert] * mine
        mix_ref[
            EXPERTS * SLOTS + expert * BLOCKS : EXPERTS * SLOTS + (expert + 1) * BLOCKS, :
        ] = tails[expert] * mine


def dispatch(ids_t, update, residual, gain, router_t):
    return pl.pallas_call(
        dispatch_kernel,
        out_shape=(
            jax.ShapeDtypeStruct((16, BLOCKS * (SLOTS + 1), BLOCK_WIDTH), jnp.bfloat16),
            jax.ShapeDtypeStruct((EXPERTS * (SLOTS + BLOCKS), TOK_DEV), jnp.float32),
        ),
        in_specs=[VMEM] * 5,
        out_specs=(VMEM, VMEM),
        scratch_shapes=[pltpu.VMEM((TOK_DEV, D), jnp.bfloat16)],
        compiler_params=params(32),
        cost_estimate=cost(800_000_000, 8_000_000),
        name="dispatch",
    )(ids_t, update, residual, gain, router_t)


PARTS = SLOTS // PART
ROWS = 16 * SLOTS
ALL_ROWS = ROWS + 16
GROUPS = 4
GROUP_DEPTH = HALF // GROUPS


def row_pick(block):
    source = lax.broadcasted_iota(jnp.int32, (16, 16 * BLOCKS), 0)
    place = lax.broadcasted_iota(jnp.int32, (16, 16 * BLOCKS), 1)
    return (place == source * BLOCKS + block).astype(jnp.bfloat16)


def first_kernel(rows_ref, u_ref, low_ref, x_ref, tail_ref, w_ref, acc_ref, sems, row_sems):
    copies = []
    for group in range(GROUPS):
        rows = pl.ds(group * GROUP_DEPTH, GROUP_DEPTH)
        copies.append(pltpu.make_async_copy(u_ref.at[0, rows], w_ref.at[rows], sems.at[group]))
    moves = [
        pltpu.make_async_copy(
            rows_ref.at[:, pl.ds(BLOCKS * SLOTS, BLOCKS), :], tail_ref, row_sems.at[2 * BLOCKS]
        )
    ]
    for block in range(BLOCKS):
        for part in range(PARTS):
            moves.append(
                pltpu.make_async_copy(
                    rows_ref.at[:, pl.ds(block * SLOTS + part * PART, PART), :],
                    x_ref.at[pl.ds(part * 16, 16), :, pl.ds(block * BLOCK_WIDTH, BLOCK_WIDTH)],
                    row_sems.at[block * PARTS + part],
                )
            )
    for move in moves[: 1 + 2 * PARTS]:
        move.start()
    copies[0].start()
    for move in moves[1 + 2 * PARTS :]:
        move.start()
    for copy in copies[1:]:
        copy.start()
    moves[0].wait()
    tail = tail_ref[...].reshape(16 * BLOCKS, BLOCK_WIDTH)
    for block in range(BLOCKS):
        picked = jnp.dot(row_pick(block), tail, preferred_element_type=jnp.float32)
        x_ref[2 * 16, :, block * BLOCK_WIDTH : (block + 1) * BLOCK_WIDTH] = picked.astype(
            jnp.bfloat16
        )
    each = BLOCKS // GROUPS * PARTS
    for group in range(GROUPS):
        at = group * GROUP_DEPTH
        for move in moves[1 + group * each : 1 + (group + 1) * each]:
            move.wait()
        copies[group].wait()
        rows = x_ref[:, :, at : at + GROUP_DEPTH].reshape(ALL_ROWS, GROUP_DEPTH)
        term = jnp.dot(rows, w_ref[at : at + GROUP_DEPTH, :], preferred_element_type=jnp.float32)
        if group == 0:
            acc_ref[...] = term
        elif group < GROUPS - 1:
            acc_ref[...] += term
        else:
            low_ref[...] = (acc_ref[...] + term).astype(jnp.bfloat16)


def first_factor(received, u_gate_up):
    return pl.pallas_call(
        first_kernel,
        out_shape=jax.ShapeDtypeStruct((ALL_ROWS, 2 * RANK), jnp.bfloat16),
        in_specs=[ANY, ANY],
        out_specs=VMEM,
        scratch_shapes=[
            pltpu.VMEM((16 * PARTS + 1, PART, HALF), jnp.bfloat16),
            pltpu.VMEM((16, BLOCKS, BLOCK_WIDTH), jnp.bfloat16),
            pltpu.VMEM((HALF, 2 * RANK), jnp.bfloat16),
            pltpu.VMEM((ALL_ROWS, 2 * RANK), jnp.float32),
            pltpu.SemaphoreType.DMA((GROUPS,)),
            pltpu.SemaphoreType.DMA((BLOCKS * PARTS + 1,)),
        ],
        compiler_params=params(58),
        cost_estimate=cost(3_400_000_000, 9_000_000),
        name="first_factor",
    )(received, u_gate_up)


FF_TILE = 512
FF_STEPS = FF_PIECE // FF_TILE


def middle_kernel(own_ref, got_ref, v_ref, u_ref, low_ref, rank_ref, vs_ref, us_ref, acc_ref, sems):
    copies = []
    for step in range(FF_STEPS):
        columns = pl.ds(step * FF_TILE, FF_TILE)
        copies.append(
            (
                pltpu.make_async_copy(
                    v_ref.at[0, :, :, columns], vs_ref.at[:, :, columns], sems.at[2 * step]
                ),
                pltpu.make_async_copy(
                    u_ref.at[0, columns, :], us_ref.at[columns, :], sems.at[2 * step + 1]
                ),
            )
        )
    for pair in copies:
        for copy in pair:
            copy.start()
    rank_ref[...] = (
        own_ref[...].astype(jnp.float32) + got_ref[...].astype(jnp.float32)
    ).astype(jnp.bfloat16)
    for step in range(FF_STEPS):
        columns = slice(step * FF_TILE, (step + 1) * FF_TILE)
        for copy in copies[step]:
            copy.wait()
        gate = jnp.dot(rank_ref[:, :RANK], vs_ref[0, :, columns], preferred_element_type=jnp.float32)
        up = jnp.dot(rank_ref[:, RANK:], vs_ref[1, :, columns], preferred_element_type=jnp.float32)
        low = 0.5 * gate
        hidden = ((low + low * jnp.tanh(low)) * up).astype(jnp.bfloat16)
        term = jnp.dot(hidden, us_ref[columns, :], preferred_element_type=jnp.float32)
        if step == 0:
            acc_ref[...] = term
        elif step < FF_STEPS - 1:
            acc_ref[...] += term
        else:
            low_ref[...] = (acc_ref[...] + term).astype(jnp.bfloat16)


def middle(own, got, v_gate_up, u_down):
    return pl.pallas_call(
        middle_kernel,
        out_shape=jax.ShapeDtypeStruct((ALL_ROWS, RANK), jnp.bfloat16),
        in_specs=[VMEM, VMEM, ANY, ANY],
        out_specs=VMEM,
        scratch_shapes=[
            pltpu.VMEM((ALL_ROWS, 2 * RANK), jnp.bfloat16),
            pltpu.VMEM((2, RANK, FF_PIECE), jnp.bfloat16),
            pltpu.VMEM((FF_PIECE, RANK), jnp.bfloat16),
            pltpu.VMEM((ALL_ROWS, RANK), jnp.float32),
            pltpu.SemaphoreType.DMA((2 * FF_STEPS,)),
        ],
        compiler_params=params(60),
        cost_estimate=cost(6_700_000_000, 14_000_000, 2_200_000),
        name="middle",
    )(own, got, v_gate_up, u_down)


def last_kernel(own_ref, got_ref, v_ref, out_ref, down_ref, w_ref, sems):
    copies = []
    for block in range(BLOCKS):
        columns = pl.ds(block * BLOCK_WIDTH, BLOCK_WIDTH)
        copies.append(
            pltpu.make_async_copy(v_ref.at[0, :, columns], w_ref.at[:, columns], sems.at[block])
        )
    for copy in copies:
        copy.start()
    down_ref[...] = (
        own_ref[...].astype(jnp.float32) + got_ref[...].astype(jnp.float32)
    ).astype(jnp.bfloat16)
    total = None
    place = lax.broadcasted_iota(jnp.int32, (16 * BLOCKS, 16), 0)
    source = lax.broadcasted_iota(jnp.int32, (16 * BLOCKS, 16), 1)
    for block in range(BLOCKS):
        copies[block].wait()
        weights = w_ref[:, block * BLOCK_WIDTH : (block + 1) * BLOCK_WIDTH]
        spread = (place == source * BLOCKS + block).astype(jnp.bfloat16)
        lifted = jnp.dot(spread, down_ref[ROWS:, :], preferred_element_type=jnp.float32)
        rows = jnp.concatenate([down_ref[:ROWS, :], lifted.astype(jnp.bfloat16)], axis=0)
        result = jnp.dot(rows, weights, preferred_element_type=jnp.float32)
        main = result[:ROWS].astype(jnp.bfloat16).reshape(PARTS, 16, PART, BLOCK_WIDTH)
        for part in range(PARTS):
            at = block * SLOTS + part * PART
            out_ref[:, at : at + PART, :] = main[part]
        total = result[ROWS:] if total is None else total + result[ROWS:]
    out_ref[:, BLOCKS * SLOTS :, :] = total.astype(jnp.bfloat16).reshape(16, BLOCKS, BLOCK_WIDTH)


def last_factor(own, got, v_down):
    return pl.pallas_call(
        last_kernel,
        out_shape=jax.ShapeDtypeStruct((16, BLOCKS * (SLOTS + 1), BLOCK_WIDTH), jnp.bfloat16),
        in_specs=[VMEM, VMEM, ANY],
        out_specs=VMEM,
        scratch_shapes=[
            pltpu.VMEM((ALL_ROWS, RANK), jnp.bfloat16),
            pltpu.VMEM((RANK, HALF), jnp.bfloat16),
            pltpu.SemaphoreType.DMA((BLOCKS,)),
        ],
        compiler_params=params(24),
        cost_estimate=cost(1_700_000_000, 6_000_000),
        name="last_factor",
    )(own, got, v_down)


def combine_kernel(mix_ref, update_ref, residual_ref, back_ref, out_ref):
    mix = mix_ref[: EXPERTS * SLOTS, :].T
    tail = mix_ref[EXPERTS * SLOTS :, :].T
    mix_high = mix.astype(jnp.bfloat16)
    mix_low = (mix - mix_high.astype(jnp.float32)).astype(jnp.bfloat16)
    tail_block = lax.broadcasted_iota(jnp.int32, (TOK_DEV, EXPERTS * BLOCKS), 1) % BLOCKS
    for half in range(2):
        tail_rows = jnp.concatenate(
            [back_ref[2 * expert + half, BLOCKS * SLOTS :, :] for expert in range(EXPERTS)], axis=0
        )
        for block in range(BLOCKS):
            rows = jnp.concatenate(
                [
                    back_ref[2 * expert + half, block * SLOTS : (block + 1) * SLOTS, :]
                    for expert in range(EXPERTS)
                ],
                axis=0,
            )
            here = jnp.where(tail_block == block, tail, 0.0)
            here_high = here.astype(jnp.bfloat16)
            here_low = (here - here_high.astype(jnp.float32)).astype(jnp.bfloat16)
            mixture = jnp.dot(mix_high, rows, preferred_element_type=jnp.float32)
            mixture = mixture + jnp.dot(mix_low, rows, preferred_element_type=jnp.float32)
            mixture = mixture + jnp.dot(here_high, tail_rows, preferred_element_type=jnp.float32)
            mixture = mixture + jnp.dot(here_low, tail_rows, preferred_element_type=jnp.float32)
            at = half * HALF + block * BLOCK_WIDTH
            stream = residual_ref[:, at : at + BLOCK_WIDTH].astype(jnp.float32) + update_ref[
                block, :, half * BLOCK_WIDTH : (half + 1) * BLOCK_WIDTH
            ].astype(jnp.float32)
            out_ref[:, at : at + BLOCK_WIDTH] = (stream + mixture).astype(jnp.bfloat16)


def combine(mix, update, residual, back):
    return pl.pallas_call(
        combine_kernel,
        out_shape=jax.ShapeDtypeStruct((TOK_DEV, D), jnp.bfloat16),
        in_specs=[VMEM] * 4,
        out_specs=VMEM,
        compiler_params=params(32),
        cost_estimate=cost(1_000_000_000, 8_000_000),
        name="combine",
    )(mix, update, residual, back)


def per_device(
    queries,
    keys,
    values,
    residual,
    proj_weight,
    norm_gain,
    router,
    expert_ids,
    u_gate_up,
    v_gate_up,
    u_down,
    v_down,
):
    zh, x, zl = lax.axis_index("zh"), lax.axis_index("x"), lax.axis_index("zl")
    y, c = lax.axis_index("y"), lax.axis_index("c")
    z = zh * 2 + zl
    chunk = zh * 8 + x * 2 + zl

    q_far = mirrored(queries[HALF_TOK:])
    kv = pack_kv(keys, values)
    kv = lax.all_to_all(kv, "y", split_axis=0, concat_axis=0, tiled=True)
    kv = kv.reshape(4 * TOK_DEV, 2 * HEAD_DIM)
    early, late = kv[:256], kv[256:]

    copies = jnp.broadcast_to(proj_weight[None], (16, GROUP_WIDTH, GROUP_WIDTH))
    q = pack_q(queries, q_far)
    q = lax.all_to_all(q, GROUP, split_axis=0, concat_axis=0, tiled=True)

    def joined(pieces):
        return jnp.concatenate(pieces, axis=0)

    early = joined(direct_pieces(early, Z))
    late = joined(direct_pieces(late, "x"))
    own = ring_pieces(early, "x") + ring_pieces(late, Z)
    swapped = [other_core(p) for p in own]

    far_chunk = 15 - chunk
    order = jnp.arange(15, dtype=jnp.int32)
    is_far = order >= chunk
    slot_list = jnp.concatenate([is_far.astype(jnp.int32), jnp.array([0, 1], jnp.int32)])
    chunk_list = jnp.concatenate(
        [jnp.where(is_far, order - chunk, order), jnp.stack([chunk, far_chunk])]
    )
    there_z = chunk_list // 8 * 2 + chunk_list % 2
    there_x = chunk_list // 2 % 4
    rel_z = relative(z, there_z)
    rel_x = relative(x, there_x)
    rows = jnp.stack([slot_list, rel_x * 4 + rel_z, rel_z * 4 + rel_x], axis=1)
    items = jnp.concatenate([jnp.array([15, 2], jnp.int32), rows.reshape(-1)]).astype(jnp.int32)
    key_ids = jnp.arange(KEY_PART, dtype=jnp.int32)
    base = key_ids // TOK_DEV * 256 + key_ids % TOK_DEV
    kpos = jnp.stack(
        [
            base + c * TOK_DEV,
            base + c * TOK_DEV + 512,
            base + (1 - c) * TOK_DEV,
            base + (1 - c) * TOK_DEV + 512,
        ]
    ).astype(jnp.int32)

    attended = attention(items, kpos, q, own + swapped)
    weight_rows = lax.all_to_all(copies, PLANE, split_axis=0, concat_axis=0, tiled=True)
    weight_rows = weight_rows.reshape(8, 2, GROUP_WIDTH, GROUP_WIDTH)
    from_y = jnp.stack([y, (y - 1) % 4, (y + 1) % 4, (y + 2) % 4])
    groups = jnp.concatenate([from_y * 2 + c, from_y * 2 + 1 - c]).astype(jnp.int32)
    near = ring_pieces(attended[0], "y")
    far = mirrored(attended[1])
    near = near + [other_core(p) for p in near]
    far = ring_pieces(far, "y")
    far = far + [other_core(p) for p in far]
    projected, arranged = projection(0, groups, weight_rows, near, None)
    projected = projection(HALF_TOK, groups, arranged, far, projected)
    update = lax.all_to_all(projected, GROUP, split_axis=0, concat_axis=0, tiled=True)

    ids_t = expert_ids.T
    send, mix = dispatch(ids_t, update, residual, norm_gain.reshape(1, D), router.T)
    received = lax.all_to_all(send, EXP, split_axis=0, concat_axis=0, tiled=True)
    rank_low = first_factor(received, u_gate_up)
    down_low = middle(rank_low, other_core(rank_low), v_gate_up, u_down)
    out_rows = last_factor(down_low, other_core(down_low), v_down)
    back = lax.all_to_all(out_rows, EXP, split_axis=0, concat_axis=0, tiled=True)
    return combine(mix, update, residual, back)


def solution(mesh):
    fine = Mesh(mesh.devices.reshape(2, 4, 2, 4, 2), ("zh", "x", "zl", "y", "c"))
    seq, exp = ("zh", "x"), ("zl", "y", "c")
    in_specs = (
        P(seq + exp, None),
        P(seq + exp, None),
        P(seq + exp, None),
        P(seq + exp, None),
        P(seq, exp),
        P(),
        P(),
        P(seq + exp, None),
        P(exp, None, None),
        P(exp, None, None, None),
        P(exp, None, None),
        P(exp, None, None),
    )

    return jax.shard_map(
        per_device, mesh=fine, in_specs=in_specs, out_specs=P(seq + exp, None), check_vma=False
    )
```

```python
import functools

import jax
import jax.numpy as jnp
from jax import lax
from jax.experimental import pallas as pl
from jax.experimental.pallas import tpu as pltpu
from jax.sharding import Mesh
from jax.sharding import PartitionSpec as P


D = 6144
HEAD_DIM = 128
GROUP_HEADS = 3
GROUP_WIDTH = GROUP_HEADS * HEAD_DIM
EXPERTS = 8
RANK = 512
FF_PIECE = 4096
TOK_DEV = 128
HALF_TOK = TOK_DEV // 2
HALF = D // 2
BLOCKS = 8
BLOCK_WIDTH = HALF // BLOCKS
SLOTS = 32
PART = 16
EPS = 1e-05
SCALE = HEAD_DIM**-0.5 * 1.4426950408889634
LOW = -1e30
Q_ROWS = 512
Q_TILE = 512
KEY_PART = 256
SOURCES = Q_TILE // HALF_TOK

Z = ("zh", "zl")
PLANE = ("zh", "x", "zl")
GROUP = ("y", "c")
EXP = ("zl", "y", "c")


VMEM = pl.BlockSpec(memory_space=pltpu.VMEM)
SMEM = pl.BlockSpec(memory_space=pltpu.SMEM)
ANY = pl.BlockSpec(memory_space=pl.ANY)
HBM = pl.BlockSpec(memory_space=pltpu.HBM)


def params(mib=48, **more):
    return pltpu.CompilerParams(vmem_limit_bytes=mib << 20, **more)


def cost(flops, moved, transcendentals=0):
    return pl.CostEstimate(flops=flops, bytes_accessed=moved, transcendentals=transcendentals)


def shifted(value, axis, step):
    return lax.ppermute(value, axis, [(i, (i + step) % 4) for i in range(4)])


def other_core(value):
    return lax.ppermute(value, "c", [(0, 1), (1, 0)])


def mirrored(value):
    return lax.ppermute(value, PLANE, [(i, 15 - i) for i in range(16)])


def ring_pieces(value, axis):
    half = value.shape[0] // 2
    up = shifted(value, axis, 1)
    down = shifted(value, axis, -1)
    far_up = shifted(up[:half], axis, 1)
    far_down = shifted(down[half:], axis, -1)
    return [value, up, down, far_up, far_down]


def relative(mine, theirs):
    gap = (mine - theirs) % 4
    return jnp.where(gap == 3, 2, jnp.where(gap == 2, 3, gap))


def direct_pieces(value, axis):
    return [value] + [shifted(value, axis, step) for step in (1, -1, 2)]


def pack_kernel(*refs):
    sources, out_ref, sems = refs[:-2], refs[-2], refs[-1]
    count, width = out_ref.shape[0], out_ref.shape[2] // len(sources)
    copies = []
    for place in range(count):
        for number, source in enumerate(sources):
            copies.append(
                pltpu.make_async_copy(
                    source.at[:, pl.ds(place * width, width)],
                    out_ref.at[place, :, pl.ds(number * width, width)],
                    sems.at[place * len(sources) + number],
                )
            )
    for copy in copies:
        copy.start()
    for copy in copies:
        copy.wait()


def packed(sources, shape):
    return pl.pallas_call(
        pack_kernel,
        out_shape=jax.ShapeDtypeStruct(shape, jnp.bfloat16),
        in_specs=[ANY] * len(sources),
        out_specs=VMEM,
        scratch_shapes=[pltpu.SemaphoreType.DMA((shape[0] * len(sources),))],
        compiler_params=params(8),
        cost_estimate=cost(1_000_000_000, 2_000_000),
        name="pack",
    )(*sources)


def pack_kv(keys, values):
    return packed((keys, values), (4, TOK_DEV, 2 * HEAD_DIM))


def pack_q_kernel(near_ref, far_ref, out_ref, sems):
    copies = []
    for place in range(8):
        columns = pl.ds(place * GROUP_WIDTH, GROUP_WIDTH)
        for slot, source in enumerate((near_ref, far_ref)):
            copies.append(
                pltpu.make_async_copy(
                    source.at[pl.ds(0, HALF_TOK), columns],
                    out_ref.at[place, pl.ds(slot * HALF_TOK, HALF_TOK), :],
                    sems.at[place * 2 + slot],
                )
            )
    for copy in copies:
        copy.start()
    for copy in copies:
        copy.wait()


def pack_q(queries, far):
    return pl.pallas_call(
        pack_q_kernel,
        out_shape=jax.ShapeDtypeStruct((8, TOK_DEV, GROUP_WIDTH), jnp.bfloat16),
        in_specs=[ANY, ANY],
        out_specs=VMEM,
        scratch_shapes=[pltpu.SemaphoreType.DMA((16,))],
        compiler_params=params(8),
        cost_estimate=cost(1_000_000_000, 2_000_000),
        name="pack_q",
    )(queries, far)


def attention_kernel(items, kpos_ref, q_ref, *refs):
    pieces = refs[:20]
    out_ref = refs[20]
    kv_ref, max_ref, acc_ref, sems = refs[21:]
    copies = []
    for which in range(4):
        for number in range(5):
            source = pieces[which * 5 + number]
            if number < 3:
                target = kv_ref.at[which, pl.ds(number * 4, 4)]
            else:
                target = kv_ref.at[which, pl.ds(12 + (number - 3) * 2, 2)]
            copies.append(pltpu.make_async_copy(source, target, sems.at[which * 5 + number]))
    for copy in copies:
        copy.start()
    max_ref[...] = jnp.full(max_ref.shape, LOW, jnp.float32)
    acc_ref[...] = jnp.zeros(acc_ref.shape, jnp.float32)
    for copy in copies:
        copy.wait()

    def load(at):
        keys, values = [], []
        ones = jnp.ones((KEY_PART, HEAD_DIM), jnp.bfloat16)
        for which in range(4):
            block = at[which % 2]
            keys.append(kv_ref[which, block, :, 0:HEAD_DIM])
            value = kv_ref[which, block, :, HEAD_DIM : 2 * HEAD_DIM]
            values.append(jnp.concatenate([value, ones], axis=1))
        return keys, values

    def score(slot, keys, tile, head):
        low = head * HEAD_DIM
        lanes = pl.ds(low if isinstance(low, int) else pl.multiple_of(low, HEAD_DIM), HEAD_DIM)
        query = q_ref[
            pl.ds(tile * SOURCES, SOURCES),
            pl.ds(pl.multiple_of(slot * HALF_TOK, HALF_TOK), HALF_TOK),
            lanes,
        ].reshape(Q_TILE, HEAD_DIM)
        return [
            lax.dot_general(
                query, key, (((1,), (1,)), ((), ())), preferred_element_type=jnp.float32
            )
            for key in keys
        ]

    def absorb(slot, values, tile, head, scores):
        rows = pl.ds(tile * Q_TILE, Q_TILE)
        highest = jnp.maximum(
            jnp.maximum(scores[0], scores[1]), jnp.maximum(scores[2], scores[3])
        )
        old_max = max_ref[slot, head, rows, :]
        new_max = jnp.maximum(old_max, jnp.max(highest, axis=1, keepdims=True))
        level = jnp.tile(new_max * SCALE, (1, KEY_PART // HEAD_DIM))
        update = None
        for which in range(4):
            weights = jnp.exp2(scores[which] * SCALE - level).astype(jnp.bfloat16)
            term = jnp.dot(weights, values[which], preferred_element_type=jnp.float32)
            update = term if update is None else update + term
        fading = jnp.exp2((old_max - new_max) * SCALE)
        max_ref[slot, head, rows, :] = new_max
        acc_ref[slot, head, rows, 0:HEAD_DIM] = (
            acc_ref[slot, head, rows, 0:HEAD_DIM] * fading + update[:, :HEAD_DIM]
        )
        acc_ref[slot, head, rows, HEAD_DIM:] = (
            acc_ref[slot, head, rows, HEAD_DIM:] * fading + update[:, HEAD_DIM:]
        )

    def work(slot, at, masked):
        keys, values = load(at)
        if masked:

            def masked_head(head, carry):
                for tile in range(Q_ROWS // Q_TILE):
                    scores = score(slot, keys, tile, head)
                    row = lax.broadcasted_iota(jnp.int32, (Q_TILE, KEY_PART), 0)
                    row_pos = (
                        (tile * SOURCES + row // HALF_TOK) * TOK_DEV
                        + slot * HALF_TOK
                        + row % HALF_TOK
                    )
                    scores = [
                        jnp.where(kpos_ref[which : which + 1, :] <= row_pos, part, LOW)
                        for which, part in enumerate(scores)
                    ]
                    absorb(slot, values, tile, head, scores)
                return carry

            lax.fori_loop(0, GROUP_HEADS, masked_head, 0)
            return
        steps = [(t, h) for t in range(Q_ROWS // Q_TILE) for h in range(GROUP_HEADS)]
        waiting = score(slot, keys, *steps[0])
        for number, (tile, head) in enumerate(steps):
            ready = waiting
            if number + 1 < len(steps):
                waiting = score(slot, keys, *steps[number + 1])
            absorb(slot, values, tile, head, ready)

    open_count = items[0]
    masked_count = items[1]

    def open_step(number, carry):
        at = 2 + 3 * number
        work(items[at], (items[at + 1], items[at + 2]), False)
        return carry

    def masked_step(number, carry):
        at = 2 + 3 * (open_count + number)
        work(items[at], (items[at + 1], items[at + 2]), True)
        return carry

    lax.fori_loop(0, open_count, open_step, 0)
    lax.fori_loop(0, masked_count, masked_step, 0)
    for slot in range(2):
        for head in range(GROUP_HEADS):
            out_ref[slot, :, head * HEAD_DIM : (head + 1) * HEAD_DIM] = (
                acc_ref[slot, head, :, 0:HEAD_DIM] / acc_ref[slot, head, :, HEAD_DIM:]
            ).astype(jnp.bfloat16)


def attention(items, kpos, query_pair, pieces):
    shaped = [p.reshape(-1, KEY_PART, 2 * HEAD_DIM) for p in pieces]
    return pl.pallas_call(
        attention_kernel,
        out_shape=jax.ShapeDtypeStruct((2, Q_ROWS, GROUP_WIDTH), jnp.bfloat16),
        in_specs=[SMEM, VMEM, VMEM] + [ANY] * 20,
        out_specs=VMEM,
        scratch_shapes=[
            pltpu.VMEM((4, 16, KEY_PART, 2 * HEAD_DIM), jnp.bfloat16),
            pltpu.VMEM((2, GROUP_HEADS, Q_ROWS, HEAD_DIM), jnp.float32),
            pltpu.VMEM((2, GROUP_HEADS, Q_ROWS, 2 * HEAD_DIM), jnp.float32),
            pltpu.SemaphoreType.DMA((20,)),
        ],
        compiler_params=params(28),
        cost_estimate=cost(27_000_000_000, 10_000_000, 26_000_000),
        name="attention",
    )(items, kpos, query_pair, *shaped)


def projection_kernel(first, groups, w_ref, *refs):
    pieces = refs[:10]
    if first:
        w_all = w_ref
        out_ref, rows_ref, done_ref, sems, w_sems, out_sem = refs[-6:]
    else:
        out_ref, w_all, rows_ref, done_ref, sems, w_sems, out_sem = refs[-7:]
    copies = []
    for core in range(2):
        for number in range(4):
            at = (core * 4 + number) * GROUP_WIDTH
            for side in range(0 if first else 2):
                copies.append(
                    pltpu.make_async_copy(
                        w_ref.at[groups[core * 4 + number], side],
                        w_all.at[pl.ds(at, GROUP_WIDTH), pl.ds(side * GROUP_WIDTH, GROUP_WIDTH)],
                        w_sems.at[(core * 4 + number) * 2 + side],
                    )
                )
        for number in range(5):
            at = (core * 4 + min(number, 3)) * GROUP_WIDTH
            source = pieces[core * 5 + number]
            low = 256 if number == 4 else 0
            copies.append(
                pltpu.make_async_copy(
                    source,
                    rows_ref.at[pl.ds(low, source.shape[0]), pl.ds(at, GROUP_WIDTH)],
                    sems.at[core * 5 + number],
                )
            )
    for copy in copies:
        copy.start()
    for copy in copies:
        copy.wait()
    for tile in range(Q_ROWS // Q_TILE):
        total = jnp.dot(
            rows_ref[tile * Q_TILE : (tile + 1) * Q_TILE, :],
            w_all[...],
            preferred_element_type=jnp.float32,
        )
        done_ref[tile * SOURCES : (tile + 1) * SOURCES] = total.astype(jnp.bfloat16).reshape(
            SOURCES, HALF_TOK, 2 * GROUP_WIDTH
        )
    out = pltpu.make_async_copy(done_ref, out_ref.at[:, pl.ds(first, HALF_TOK), :], out_sem)
    out.start()
    out.wait()


def projection(first, groups, weights, pieces, before):
    more = [] if before is None else [before]
    out = jax.ShapeDtypeStruct((8, TOK_DEV, 2 * GROUP_WIDTH), jnp.bfloat16)
    arranged = jax.ShapeDtypeStruct((8 * GROUP_WIDTH, 2 * GROUP_WIDTH), jnp.bfloat16)
    return pl.pallas_call(
        functools.partial(projection_kernel, first),
        out_shape=out if more else (out, arranged),
        in_specs=[SMEM] + [VMEM if more else ANY] + [ANY] * (10 + len(more)),
        out_specs=HBM if more else (HBM, VMEM),
        scratch_shapes=[
            pltpu.VMEM((Q_ROWS, 8 * GROUP_WIDTH), jnp.bfloat16),
            pltpu.VMEM((8, HALF_TOK, 2 * GROUP_WIDTH), jnp.bfloat16),
            pltpu.SemaphoreType.DMA((10,)),
            pltpu.SemaphoreType.DMA((16,)),
            pltpu.SemaphoreType.DMA,
        ],
        input_output_aliases={12: 0} if more else {},
        compiler_params=params(16),
        cost_estimate=cost(2_500_000_000, 9_000_000),
        name="projection",
    )(groups, weights, *pieces, *more)


def slot_tables(ids_t):
    expert = lax.broadcasted_iota(jnp.int32, (EXPERTS, TOK_DEV), 0)
    first = (expert == ids_t[0:1, :]).astype(jnp.float32)
    second = (expert == ids_t[1:2, :]).astype(jnp.float32)
    member = first + second
    before = (
        lax.broadcasted_iota(jnp.int32, (TOK_DEV, TOK_DEV), 0)
        < lax.broadcasted_iota(jnp.int32, (TOK_DEV, TOK_DEV), 1)
    ).astype(jnp.bfloat16)
    slot = jnp.dot(member.astype(jnp.bfloat16), before, preferred_element_type=jnp.float32)
    return first, second, member, slot


def dispatch_kernel(ids_ref, update_ref, residual_ref, gain_ref, router_ref, send_ref, mix_ref, normed_ref):
    squares = jnp.zeros((TOK_DEV, 1), jnp.float32)
    for half in range(2):
        for group in range(BLOCKS):
            at = half * HALF + group * BLOCK_WIDTH
            row = residual_ref[:, at : at + BLOCK_WIDTH].astype(jnp.float32) + update_ref[
                group, :, half * BLOCK_WIDTH : (half + 1) * BLOCK_WIDTH
            ].astype(jnp.float32)
            squares = squares + jnp.sum(row * row, axis=1, keepdims=True)
    factor = lax.rsqrt(squares / D + EPS)
    for half in range(2):
        for group in range(BLOCKS):
            at = half * HALF + group * BLOCK_WIDTH
            row = residual_ref[:, at : at + BLOCK_WIDTH].astype(jnp.float32) + update_ref[
                group, :, half * BLOCK_WIDTH : (half + 1) * BLOCK_WIDTH
            ].astype(jnp.float32)
            gain = gain_ref[:, at : at + BLOCK_WIDTH].astype(jnp.float32)
            normed_ref[:, at : at + BLOCK_WIDTH] = (row * factor * gain).astype(jnp.bfloat16)
    first, second, member, slot = slot_tables(ids_ref[...])
    slot_ids = lax.broadcasted_iota(jnp.int32, (SLOTS, TOK_DEV), 0).astype(jnp.float32)
    picks, tails = [], []
    last = jnp.where(slot == float(SLOTS), member, 0.0)
    for expert in range(EXPERTS):
        picks.append(
            jnp.where(slot[expert : expert + 1, :] == slot_ids, member[expert : expert + 1, :], 0.0)
        )
        tails.append(jnp.broadcast_to(last[expert : expert + 1, :], (BLOCKS, TOK_DEV)))
    pick = jnp.concatenate(picks, axis=0)
    tail = jnp.concatenate(tails, axis=0)
    tail_block = lax.broadcasted_iota(jnp.int32, (EXPERTS * BLOCKS, TOK_DEV), 0) % BLOCKS
    pick_low = pick.astype(jnp.bfloat16)
    for half in range(2):

        def one_block(block, tail_rows):
            at = pl.multiple_of(half * HALF + block * BLOCK_WIDTH, BLOCK_WIDTH)
            rows = normed_ref[:, pl.ds(at, BLOCK_WIDTH)]
            moved = jnp.dot(pick_low, rows, preferred_element_type=jnp.float32).astype(jnp.bfloat16)
            place = pl.ds(pl.multiple_of(block * SLOTS, SLOTS), SLOTS)
            for expert in range(EXPERTS):
                send_ref[2 * expert + half, place, :] = moved[
                    expert * SLOTS : (expert + 1) * SLOTS, :
                ]
            chosen = jnp.where(tail_block == block, tail, 0.0).astype(jnp.bfloat16)
            return tail_rows + jnp.dot(chosen, rows, preferred_element_type=jnp.float32)

        empty = jnp.zeros((EXPERTS * BLOCKS, BLOCK_WIDTH), jnp.float32)
        tail_rows = lax.fori_loop(0, BLOCKS, one_block, empty)
        tail_rows = tail_rows.astype(jnp.bfloat16)
        for expert in range(EXPERTS):
            send_ref[2 * expert + half, BLOCKS * SLOTS :, :] = tail_rows[
                expert * BLOCKS : (expert + 1) * BLOCKS, :
            ]
    logits = lax.dot_general(
        router_ref[...],
        normed_ref[...],
        (((1,), (1,)), ((), ())),
        preferred_element_type=jnp.float32,
    )
    chosen_first = jnp.sum(first * logits, axis=0, keepdims=True)
    chosen_second = jnp.sum(second * logits, axis=0, keepdims=True)
    mix_first = 1.0 / (1.0 + jnp.exp(chosen_second - chosen_first))
    mix_second = 1.0 / (1.0 + jnp.exp(chosen_first - chosen_second))
    share = first * mix_first + second * mix_second
    for expert in range(EXPERTS):
        mine = share[expert : expert + 1, :]
        mix_ref[expert * SLOTS : (expert + 1) * SLOTS, :] = picks[expert] * mine
        mix_ref[
            EXPERTS * SLOTS + expert * BLOCKS : EXPERTS * SLOTS + (expert + 1) * BLOCKS, :
        ] = tails[expert] * mine


def dispatch(ids_t, update, residual, gain, router_t):
    return pl.pallas_call(
        dispatch_kernel,
        out_shape=(
            jax.ShapeDtypeStruct((16, BLOCKS * (SLOTS + 1), BLOCK_WIDTH), jnp.bfloat16),
            jax.ShapeDtypeStruct((EXPERTS * (SLOTS + BLOCKS), TOK_DEV), jnp.float32),
        ),
        in_specs=[VMEM] * 5,
        out_specs=(VMEM, VMEM),
        scratch_shapes=[pltpu.VMEM((TOK_DEV, D), jnp.bfloat16)],
        compiler_params=params(32),
        cost_estimate=cost(800_000_000, 8_000_000),
        name="dispatch",
    )(ids_t, update, residual, gain, router_t)


PARTS = SLOTS // PART
ROWS = 16 * SLOTS
ALL_ROWS = ROWS + 16
GROUPS = 4
GROUP_DEPTH = HALF // GROUPS


def row_pick(block):
    source = lax.broadcasted_iota(jnp.int32, (16, 16 * BLOCKS), 0)
    place = lax.broadcasted_iota(jnp.int32, (16, 16 * BLOCKS), 1)
    return (place == source * BLOCKS + block).astype(jnp.bfloat16)


def first_kernel(rows_ref, u_ref, low_ref, x_ref, tail_ref, w_ref, acc_ref, sems, row_sems):
    copies = []
    for group in range(GROUPS):
        rows = pl.ds(group * GROUP_DEPTH, GROUP_DEPTH)
        copies.append(pltpu.make_async_copy(u_ref.at[0, rows], w_ref.at[rows], sems.at[group]))
    moves = [
        pltpu.make_async_copy(
            rows_ref.at[:, pl.ds(BLOCKS * SLOTS, BLOCKS), :], tail_ref, row_sems.at[2 * BLOCKS]
        )
    ]
    for block in range(BLOCKS):
        for part in range(PARTS):
            moves.append(
                pltpu.make_async_copy(
                    rows_ref.at[:, pl.ds(block * SLOTS + part * PART, PART), :],
                    x_ref.at[pl.ds(part * 16, 16), :, pl.ds(block * BLOCK_WIDTH, BLOCK_WIDTH)],
                    row_sems.at[block * PARTS + part],
                )
            )
    for move in moves[: 1 + 2 * PARTS]:
        move.start()
    copies[0].start()
    for move in moves[1 + 2 * PARTS :]:
        move.start()
    for copy in copies[1:]:
        copy.start()
    moves[0].wait()
    tail = tail_ref[...].reshape(16 * BLOCKS, BLOCK_WIDTH)
    for block in range(BLOCKS):
        picked = jnp.dot(row_pick(block), tail, preferred_element_type=jnp.float32)
        x_ref[2 * 16, :, block * BLOCK_WIDTH : (block + 1) * BLOCK_WIDTH] = picked.astype(
            jnp.bfloat16
        )
    each = BLOCKS // GROUPS * PARTS
    for group in range(GROUPS):
        at = group * GROUP_DEPTH
        for move in moves[1 + group * each : 1 + (group + 1) * each]:
            move.wait()
        copies[group].wait()
        rows = x_ref[:, :, at : at + GROUP_DEPTH].reshape(ALL_ROWS, GROUP_DEPTH)
        term = jnp.dot(rows, w_ref[at : at + GROUP_DEPTH, :], preferred_element_type=jnp.float32)
        if group == 0:
            acc_ref[...] = term
        elif group < GROUPS - 1:
            acc_ref[...] += term
        else:
            low_ref[...] = (acc_ref[...] + term).astype(jnp.bfloat16)


def first_factor(received, u_gate_up):
    return pl.pallas_call(
        first_kernel,
        out_shape=jax.ShapeDtypeStruct((ALL_ROWS, 2 * RANK), jnp.bfloat16),
        in_specs=[ANY, ANY],
        out_specs=VMEM,
        scratch_shapes=[
            pltpu.VMEM((16 * PARTS + 1, PART, HALF), jnp.bfloat16),
            pltpu.VMEM((16, BLOCKS, BLOCK_WIDTH), jnp.bfloat16),
            pltpu.VMEM((HALF, 2 * RANK), jnp.bfloat16),
            pltpu.VMEM((ALL_ROWS, 2 * RANK), jnp.float32),
            pltpu.SemaphoreType.DMA((GROUPS,)),
            pltpu.SemaphoreType.DMA((BLOCKS * PARTS + 1,)),
        ],
        compiler_params=params(58),
        cost_estimate=cost(3_400_000_000, 9_000_000),
        name="first_factor",
    )(received, u_gate_up)


FF_TILE = 512
FF_STEPS = FF_PIECE // FF_TILE


def middle_kernel(own_ref, got_ref, v_ref, u_ref, low_ref, rank_ref, vs_ref, us_ref, acc_ref, sems):
    copies = []
    for step in range(FF_STEPS):
        columns = pl.ds(step * FF_TILE, FF_TILE)
        copies.append(
            (
                pltpu.make_async_copy(
                    v_ref.at[0, :, :, columns], vs_ref.at[:, :, columns], sems.at[2 * step]
                ),
                pltpu.make_async_copy(
                    u_ref.at[0, columns, :], us_ref.at[columns, :], sems.at[2 * step + 1]
                ),
            )
        )
    for pair in copies:
        for copy in pair:
            copy.start()
    rank_ref[...] = (
        own_ref[...].astype(jnp.float32) + got_ref[...].astype(jnp.float32)
    ).astype(jnp.bfloat16)
    acc_ref[...] = jnp.zeros(acc_ref.shape, jnp.float32)

    def one_tile(step, carry):
        columns = pl.ds(pl.multiple_of(step * FF_TILE, FF_TILE), FF_TILE)
        pltpu.make_async_copy(
            v_ref.at[0, :, :, columns], vs_ref.at[:, :, columns], sems.at[2 * step]
        ).wait()
        pltpu.make_async_copy(
            u_ref.at[0, columns, :], us_ref.at[columns, :], sems.at[2 * step + 1]
        ).wait()
        gate = jnp.dot(rank_ref[:, :RANK], vs_ref[0, :, columns], preferred_element_type=jnp.float32)
        up = jnp.dot(rank_ref[:, RANK:], vs_ref[1, :, columns], preferred_element_type=jnp.float32)
        low = 0.5 * gate
        hidden = ((low + low * jnp.tanh(low)) * up).astype(jnp.bfloat16)
        acc_ref[...] += jnp.dot(hidden, us_ref[columns, :], preferred_element_type=jnp.float32)
        return carry

    lax.fori_loop(0, FF_STEPS, one_tile, 0)
    low_ref[...] = acc_ref[...].astype(jnp.bfloat16)


def middle(own, got, v_gate_up, u_down):
    return pl.pallas_call(
        middle_kernel,
        out_shape=jax.ShapeDtypeStruct((ALL_ROWS, RANK), jnp.bfloat16),
        in_specs=[VMEM, VMEM, ANY, ANY],
        out_specs=VMEM,
        scratch_shapes=[
            pltpu.VMEM((ALL_ROWS, 2 * RANK), jnp.bfloat16),
            pltpu.VMEM((2, RANK, FF_PIECE), jnp.bfloat16),
            pltpu.VMEM((FF_PIECE, RANK), jnp.bfloat16),
            pltpu.VMEM((ALL_ROWS, RANK), jnp.float32),
            pltpu.SemaphoreType.DMA((2 * FF_STEPS,)),
        ],
        compiler_params=params(60),
        cost_estimate=cost(6_700_000_000, 14_000_000, 2_200_000),
        name="middle",
    )(own, got, v_gate_up, u_down)


def last_kernel(own_ref, got_ref, v_ref, out_ref, down_ref, w_ref, tail_ref, sems):
    copies = []
    for block in range(BLOCKS):
        columns = pl.ds(block * BLOCK_WIDTH, BLOCK_WIDTH)
        copies.append(
            pltpu.make_async_copy(v_ref.at[0, :, columns], w_ref.at[:, columns], sems.at[block])
        )
    for copy in copies:
        copy.start()
    down_ref[...] = (
        own_ref[...].astype(jnp.float32) + got_ref[...].astype(jnp.float32)
    ).astype(jnp.bfloat16)
    place = lax.broadcasted_iota(jnp.int32, (16 * BLOCKS, 16), 0)
    source = lax.broadcasted_iota(jnp.int32, (16 * BLOCKS, 16), 1)
    tail_ref[...] = jnp.zeros(tail_ref.shape, jnp.float32)

    def one_block(block, carry):
        columns = pl.ds(pl.multiple_of(block * BLOCK_WIDTH, BLOCK_WIDTH), BLOCK_WIDTH)
        pltpu.make_async_copy(v_ref.at[0, :, columns], w_ref.at[:, columns], sems.at[block]).wait()
        spread = (place == source * BLOCKS + block).astype(jnp.bfloat16)
        lifted = jnp.dot(spread, down_ref[ROWS:, :], preferred_element_type=jnp.float32)
        rows = jnp.concatenate([down_ref[:ROWS, :], lifted.astype(jnp.bfloat16)], axis=0)
        result = jnp.dot(rows, w_ref[:, columns], preferred_element_type=jnp.float32)
        main = result[:ROWS].astype(jnp.bfloat16).reshape(PARTS, 16, PART, BLOCK_WIDTH)
        for part in range(PARTS):
            at = pl.ds(pl.multiple_of(block * SLOTS + part * PART, PART), PART)
            out_ref[:, at, :] = main[part]
        tail_ref[...] += result[ROWS:]
        return carry

    lax.fori_loop(0, BLOCKS, one_block, 0)
    out_ref[:, BLOCKS * SLOTS :, :] = (
        tail_ref[...].astype(jnp.bfloat16).reshape(16, BLOCKS, BLOCK_WIDTH)
    )


def last_factor(own, got, v_down):
    return pl.pallas_call(
        last_kernel,
        out_shape=jax.ShapeDtypeStruct((16, BLOCKS * (SLOTS + 1), BLOCK_WIDTH), jnp.bfloat16),
        in_specs=[VMEM, VMEM, ANY],
        out_specs=VMEM,
        scratch_shapes=[
            pltpu.VMEM((ALL_ROWS, RANK), jnp.bfloat16),
            pltpu.VMEM((RANK, HALF), jnp.bfloat16),
            pltpu.VMEM((16 * BLOCKS, BLOCK_WIDTH), jnp.float32),
            pltpu.SemaphoreType.DMA((BLOCKS,)),
        ],
        compiler_params=params(24),
        cost_estimate=cost(1_700_000_000, 6_000_000),
        name="last_factor",
    )(own, got, v_down)


def combine_kernel(mix_ref, update_ref, residual_ref, back_ref, out_ref):
    mix = mix_ref[: EXPERTS * SLOTS, :].T
    tail = mix_ref[EXPERTS * SLOTS :, :].T
    mix_high = mix.astype(jnp.bfloat16)
    mix_low = (mix - mix_high.astype(jnp.float32)).astype(jnp.bfloat16)
    tail_block = lax.broadcasted_iota(jnp.int32, (TOK_DEV, EXPERTS * BLOCKS), 1) % BLOCKS
    for half in range(2):
        tail_rows = jnp.concatenate(
            [back_ref[2 * expert + half, BLOCKS * SLOTS :, :] for expert in range(EXPERTS)], axis=0
        )

        def one_block(block, carry):
            at_rows = pl.ds(pl.multiple_of(block * SLOTS, SLOTS), SLOTS)
            rows = jnp.concatenate(
                [back_ref[2 * expert + half, at_rows, :] for expert in range(EXPERTS)], axis=0
            )
            here = jnp.where(tail_block == block, tail, 0.0)
            here_high = here.astype(jnp.bfloat16)
            here_low = (here - here_high.astype(jnp.float32)).astype(jnp.bfloat16)
            mixture = jnp.dot(mix_high, rows, preferred_element_type=jnp.float32)
            mixture = mixture + jnp.dot(mix_low, rows, preferred_element_type=jnp.float32)
            mixture = mixture + jnp.dot(here_high, tail_rows, preferred_element_type=jnp.float32)
            mixture = mixture + jnp.dot(here_low, tail_rows, preferred_element_type=jnp.float32)
            at = pl.ds(pl.multiple_of(half * HALF + block * BLOCK_WIDTH, BLOCK_WIDTH), BLOCK_WIDTH)
            stream = residual_ref[:, at].astype(jnp.float32) + update_ref[
                block, :, half * BLOCK_WIDTH : (half + 1) * BLOCK_WIDTH
            ].astype(jnp.float32)
            out_ref[:, at] = (stream + mixture).astype(jnp.bfloat16)
            return carry

        lax.fori_loop(0, BLOCKS, one_block, 0)


def combine(mix, update, residual, back):
    return pl.pallas_call(
        combine_kernel,
        out_shape=jax.ShapeDtypeStruct((TOK_DEV, D), jnp.bfloat16),
        in_specs=[VMEM] * 4,
        out_specs=VMEM,
        compiler_params=params(32),
        cost_estimate=cost(1_000_000_000, 8_000_000),
        name="combine",
    )(mix, update, residual, back)


def per_device(
    queries,
    keys,
    values,
    residual,
    proj_weight,
    norm_gain,
    router,
    expert_ids,
    u_gate_up,
    v_gate_up,
    u_down,
    v_down,
):
    zh, x, zl = lax.axis_index("zh"), lax.axis_index("x"), lax.axis_index("zl")
    y, c = lax.axis_index("y"), lax.axis_index("c")
    z = zh * 2 + zl
    chunk = zh * 8 + x * 2 + zl

    q_far = mirrored(queries[HALF_TOK:])
    kv = pack_kv(keys, values)
    kv = lax.all_to_all(kv, "y", split_axis=0, concat_axis=0, tiled=True)
    kv = kv.reshape(4 * TOK_DEV, 2 * HEAD_DIM)
    early, late = kv[:256], kv[256:]

    copies = jnp.broadcast_to(proj_weight[None], (16, GROUP_WIDTH, GROUP_WIDTH))
    q = pack_q(queries, q_far)
    q = lax.all_to_all(q, GROUP, split_axis=0, concat_axis=0, tiled=True)

    def joined(pieces):
        return jnp.concatenate(pieces, axis=0)

    early = joined(direct_pieces(early, Z))
    late = joined(direct_pieces(late, "x"))
    own = ring_pieces(early, "x") + ring_pieces(late, Z)
    swapped = [other_core(p) for p in own]

    far_chunk = 15 - chunk
    order = jnp.arange(15, dtype=jnp.int32)
    is_far = order >= chunk
    slot_list = jnp.concatenate([is_far.astype(jnp.int32), jnp.array([0, 1], jnp.int32)])
    chunk_list = jnp.concatenate(
        [jnp.where(is_far, order - chunk, order), jnp.stack([chunk, far_chunk])]
    )
    there_z = chunk_list // 8 * 2 + chunk_list % 2
    there_x = chunk_list // 2 % 4
    rel_z = relative(z, there_z)
    rel_x = relative(x, there_x)
    rows = jnp.stack([slot_list, rel_x * 4 + rel_z, rel_z * 4 + rel_x], axis=1)
    items = jnp.concatenate([jnp.array([15, 2], jnp.int32), rows.reshape(-1)]).astype(jnp.int32)
    key_ids = jnp.arange(KEY_PART, dtype=jnp.int32)
    base = key_ids // TOK_DEV * 256 + key_ids % TOK_DEV
    kpos = jnp.stack(
        [
            base + c * TOK_DEV,
            base + c * TOK_DEV + 512,
            base + (1 - c) * TOK_DEV,
            base + (1 - c) * TOK_DEV + 512,
        ]
    ).astype(jnp.int32)

    attended = attention(items, kpos, q, own + swapped)
    weight_rows = lax.all_to_all(copies, PLANE, split_axis=0, concat_axis=0, tiled=True)
    weight_rows = weight_rows.reshape(8, 2, GROUP_WIDTH, GROUP_WIDTH)
    from_y = jnp.stack([y, (y - 1) % 4, (y + 1) % 4, (y + 2) % 4])
    groups = jnp.concatenate([from_y * 2 + c, from_y * 2 + 1 - c]).astype(jnp.int32)
    near = ring_pieces(attended[0], "y")
    far = mirrored(attended[1])
    near = near + [other_core(p) for p in near]
    far = ring_pieces(far, "y")
    far = far + [other_core(p) for p in far]
    projected, arranged = projection(0, groups, weight_rows, near, None)
    projected = projection(HALF_TOK, groups, arranged, far, projected)
    update = lax.all_to_all(projected, GROUP, split_axis=0, concat_axis=0, tiled=True)

    ids_t = expert_ids.T
    send, mix = dispatch(ids_t, update, residual, norm_gain.reshape(1, D), router.T)
    received = lax.all_to_all(send, EXP, split_axis=0, concat_axis=0, tiled=True)
    rank_low = first_factor(received, u_gate_up)
    down_low = middle(rank_low, other_core(rank_low), v_gate_up, u_down)
    out_rows = last_factor(down_low, other_core(down_low), v_down)
    back = lax.all_to_all(out_rows, EXP, split_axis=0, concat_axis=0, tiled=True)
    return combine(mix, update, residual, back)


def solution(mesh):
    fine = Mesh(mesh.devices.reshape(2, 4, 2, 4, 2), ("zh", "x", "zl", "y", "c"))
    seq, exp = ("zh", "x"), ("zl", "y", "c")
    in_specs = (
        P(seq + exp, None),
        P(seq + exp, None),
        P(seq + exp, None),
        P(seq + exp, None),
        P(seq, exp),
        P(),
        P(),
        P(seq + exp, None),
        P(exp, None, None),
        P(exp, None, None, None),
        P(exp, None, None),
        P(exp, None, None),
    )

    return jax.shard_map(
        per_device, mesh=fine, in_specs=in_specs, out_specs=P(seq + exp, None), check_vma=False
    )
```

```python
import functools

import jax
import jax.numpy as jnp
from jax import lax
from jax.experimental import pallas as pl
from jax.experimental.pallas import tpu as pltpu
from jax.sharding import Mesh
from jax.sharding import PartitionSpec as P


D = 6144
HEAD_DIM = 128
GROUP_HEADS = 3
GROUP_WIDTH = GROUP_HEADS * HEAD_DIM
EXPERTS = 8
RANK = 512
FF_PIECE = 4096
TOK_DEV = 128
HALF_TOK = TOK_DEV // 2
HALF = D // 2
BLOCKS = 8
BLOCK_WIDTH = HALF // BLOCKS
SLOTS = 32
UNROLL = 8
PART = 16
EPS = 1e-05
SCALE = HEAD_DIM**-0.5 * 1.4426950408889634
LOW = -1e30
Q_ROWS = 512
Q_TILE = 512
KEY_PART = 256
SOURCES = Q_TILE // HALF_TOK

Z = ("zh", "zl")
PLANE = ("zh", "x", "zl")
GROUP = ("y", "c")
EXP = ("zl", "y", "c")


VMEM = pl.BlockSpec(memory_space=pltpu.VMEM)
SMEM = pl.BlockSpec(memory_space=pltpu.SMEM)
ANY = pl.BlockSpec(memory_space=pl.ANY)
HBM = pl.BlockSpec(memory_space=pltpu.HBM)


def params(mib=48, **more):
    return pltpu.CompilerParams(vmem_limit_bytes=mib << 20, **more)


def cost(flops, moved, transcendentals=0):
    return pl.CostEstimate(flops=flops, bytes_accessed=moved, transcendentals=transcendentals)


def shifted(value, axis, step):
    return lax.ppermute(value, axis, [(i, (i + step) % 4) for i in range(4)])


def other_core(value):
    return lax.ppermute(value, "c", [(0, 1), (1, 0)])


def mirrored(value):
    return lax.ppermute(value, PLANE, [(i, 15 - i) for i in range(16)])


def ring_pieces(value, axis):
    half = value.shape[0] // 2
    up = shifted(value, axis, 1)
    down = shifted(value, axis, -1)
    far_up = shifted(up[:half], axis, 1)
    far_down = shifted(down[half:], axis, -1)
    return [value, up, down, far_up, far_down]


def relative(mine, theirs):
    gap = (mine - theirs) % 4
    return jnp.where(gap == 3, 2, jnp.where(gap == 2, 3, gap))


def direct_pieces(value, axis):
    return [value] + [shifted(value, axis, step) for step in (1, -1, 2)]


def pack_kernel(*refs):
    sources, out_ref, sems = refs[:-2], refs[-2], refs[-1]
    count, width = out_ref.shape[0], out_ref.shape[2] // len(sources)
    copies = []
    for place in range(count):
        for number, source in enumerate(sources):
            copies.append(
                pltpu.make_async_copy(
                    source.at[:, pl.ds(place * width, width)],
                    out_ref.at[place, :, pl.ds(number * width, width)],
                    sems.at[place * len(sources) + number],
                )
            )
    for copy in copies:
        copy.start()
    for copy in copies:
        copy.wait()


def packed(sources, shape):
    return pl.pallas_call(
        pack_kernel,
        out_shape=jax.ShapeDtypeStruct(shape, jnp.bfloat16),
        in_specs=[ANY] * len(sources),
        out_specs=VMEM,
        scratch_shapes=[pltpu.SemaphoreType.DMA((shape[0] * len(sources),))],
        compiler_params=params(63),
        cost_estimate=cost(1_000_000_000, 2_000_000),
        name="pack",
    )(*sources)


def pack_kv(keys, values):
    return packed((keys, values), (4, TOK_DEV, 2 * HEAD_DIM))


def pack_q_kernel(near_ref, far_ref, out_ref, sems):
    copies = []
    for place in range(8):
        columns = pl.ds(place * GROUP_WIDTH, GROUP_WIDTH)
        for slot, source in enumerate((near_ref, far_ref)):
            copies.append(
                pltpu.make_async_copy(
                    source.at[pl.ds(0, HALF_TOK), columns],
                    out_ref.at[place, pl.ds(slot * HALF_TOK, HALF_TOK), :],
                    sems.at[place * 2 + slot],
                )
            )
    for copy in copies:
        copy.start()
    for copy in copies:
        copy.wait()


def pack_q(queries, far):
    return pl.pallas_call(
        pack_q_kernel,
        out_shape=jax.ShapeDtypeStruct((8, TOK_DEV, GROUP_WIDTH), jnp.bfloat16),
        in_specs=[ANY, ANY],
        out_specs=VMEM,
        scratch_shapes=[pltpu.SemaphoreType.DMA((16,))],
        compiler_params=params(8),
        cost_estimate=cost(1_000_000_000, 2_000_000),
        name="pack_q",
    )(queries, far)


def attention_kernel(items, kpos_ref, q_ref, *refs):
    pieces = refs[:20]
    out_ref = refs[20]
    kv_ref, max_ref, acc_ref, sems = refs[21:]
    copies = []
    for which in range(4):
        for number in range(5):
            source = pieces[which * 5 + number]
            if number < 3:
                target = kv_ref.at[which, pl.ds(number * 4, 4)]
            else:
                target = kv_ref.at[which, pl.ds(12 + (number - 3) * 2, 2)]
            copies.append(pltpu.make_async_copy(source, target, sems.at[which * 5 + number]))
    for copy in copies:
        copy.start()
    max_ref[...] = jnp.full(max_ref.shape, LOW, jnp.float32)
    acc_ref[...] = jnp.zeros(acc_ref.shape, jnp.float32)
    for copy in copies:
        copy.wait()

    def load(at):
        keys, values = [], []
        ones = jnp.ones((KEY_PART, HEAD_DIM), jnp.bfloat16)
        for which in range(4):
            block = at[which % 2]
            keys.append(kv_ref[which, block, :, 0:HEAD_DIM])
            value = kv_ref[which, block, :, HEAD_DIM : 2 * HEAD_DIM]
            values.append(jnp.concatenate([value, ones], axis=1))
        return keys, values

    def score(slot, keys, tile, head):
        low = head * HEAD_DIM
        lanes = pl.ds(low if isinstance(low, int) else pl.multiple_of(low, HEAD_DIM), HEAD_DIM)
        query = q_ref[
            pl.ds(tile * SOURCES, SOURCES),
            pl.ds(pl.multiple_of(slot * HALF_TOK, HALF_TOK), HALF_TOK),
            lanes,
        ].reshape(Q_TILE, HEAD_DIM)
        return [
            lax.dot_general(
                query, key, (((1,), (1,)), ((), ())), preferred_element_type=jnp.float32
            )
            for key in keys
        ]

    def absorb(slot, values, tile, head, scores):
        rows = pl.ds(tile * Q_TILE, Q_TILE)
        highest = jnp.maximum(
            jnp.maximum(scores[0], scores[1]), jnp.maximum(scores[2], scores[3])
        )
        old_max = max_ref[slot, head, rows, :]
        new_max = jnp.maximum(old_max, jnp.max(highest, axis=1, keepdims=True))
        level = jnp.tile(new_max * SCALE, (1, KEY_PART // HEAD_DIM))
        update = None
        for which in range(4):
            weights = jnp.exp2(scores[which] * SCALE - level).astype(jnp.bfloat16)
            term = jnp.dot(weights, values[which], preferred_element_type=jnp.float32)
            update = term if update is None else update + term
        fading = jnp.exp2((old_max - new_max) * SCALE)
        max_ref[slot, head, rows, :] = new_max
        acc_ref[slot, head, rows, 0:HEAD_DIM] = (
            acc_ref[slot, head, rows, 0:HEAD_DIM] * fading + update[:, :HEAD_DIM]
        )
        acc_ref[slot, head, rows, HEAD_DIM:] = (
            acc_ref[slot, head, rows, HEAD_DIM:] * fading + update[:, HEAD_DIM:]
        )

    def work(slot, at, masked):
        keys, values = load(at)
        if masked:

            def masked_head(head, carry):
                for tile in range(Q_ROWS // Q_TILE):
                    scores = score(slot, keys, tile, head)
                    row = lax.broadcasted_iota(jnp.int32, (Q_TILE, KEY_PART), 0)
                    row_pos = (
                        (tile * SOURCES + row // HALF_TOK) * TOK_DEV
                        + slot * HALF_TOK
                        + row % HALF_TOK
                    )
                    scores = [
                        jnp.where(kpos_ref[which : which + 1, :] <= row_pos, part, LOW)
                        for which, part in enumerate(scores)
                    ]
                    absorb(slot, values, tile, head, scores)
                return carry

            lax.fori_loop(0, GROUP_HEADS, masked_head, 0)
            return
        steps = [(t, h) for t in range(Q_ROWS // Q_TILE) for h in range(GROUP_HEADS)]
        waiting = score(slot, keys, *steps[0])
        for number, (tile, head) in enumerate(steps):
            ready = waiting
            if number + 1 < len(steps):
                waiting = score(slot, keys, *steps[number + 1])
            absorb(slot, values, tile, head, ready)

    open_count = items[0]
    masked_count = items[1]

    def open_step(number, carry):
        at = 2 + 3 * number
        work(items[at], (items[at + 1], items[at + 2]), False)
        return carry

    def masked_step(number, carry):
        at = 2 + 3 * (open_count + number)
        work(items[at], (items[at + 1], items[at + 2]), True)
        return carry

    lax.fori_loop(0, open_count, open_step, 0)
    lax.fori_loop(0, masked_count, masked_step, 0)
    for slot in range(2):
        for head in range(GROUP_HEADS):
            out_ref[slot, :, head * HEAD_DIM : (head + 1) * HEAD_DIM] = (
                acc_ref[slot, head, :, 0:HEAD_DIM] / acc_ref[slot, head, :, HEAD_DIM:]
            ).astype(jnp.bfloat16)


def attention(items, kpos, query_pair, pieces):
    shaped = [p.reshape(-1, KEY_PART, 2 * HEAD_DIM) for p in pieces]
    return pl.pallas_call(
        attention_kernel,
        out_shape=jax.ShapeDtypeStruct((2, Q_ROWS, GROUP_WIDTH), jnp.bfloat16),
        in_specs=[SMEM, VMEM, VMEM] + [ANY] * 20,
        out_specs=VMEM,
        scratch_shapes=[
            pltpu.VMEM((4, 16, KEY_PART, 2 * HEAD_DIM), jnp.bfloat16),
            pltpu.VMEM((2, GROUP_HEADS, Q_ROWS, HEAD_DIM), jnp.float32),
            pltpu.VMEM((2, GROUP_HEADS, Q_ROWS, 2 * HEAD_DIM), jnp.float32),
            pltpu.SemaphoreType.DMA((20,)),
        ],
        compiler_params=params(28),
        cost_estimate=cost(27_000_000_000, 10_000_000, 26_000_000),
        name="attention",
    )(items, kpos, query_pair, *shaped)


def projection_kernel(first, groups, w_ref, *refs):
    pieces = refs[:10]
    if first:
        w_all = w_ref
        out_ref, rows_ref, done_ref, sems, w_sems, out_sem = refs[-6:]
    else:
        out_ref, w_all, rows_ref, done_ref, sems, w_sems, out_sem = refs[-7:]
    copies = []
    for core in range(2):
        for number in range(4):
            at = (core * 4 + number) * GROUP_WIDTH
            for side in range(0 if first else 2):
                copies.append(
                    pltpu.make_async_copy(
                        w_ref.at[groups[core * 4 + number], side],
                        w_all.at[pl.ds(at, GROUP_WIDTH), pl.ds(side * GROUP_WIDTH, GROUP_WIDTH)],
                        w_sems.at[(core * 4 + number) * 2 + side],
                    )
                )
        for number in range(5):
            at = (core * 4 + min(number, 3)) * GROUP_WIDTH
            source = pieces[core * 5 + number]
            low = 256 if number == 4 else 0
            copies.append(
                pltpu.make_async_copy(
                    source,
                    rows_ref.at[pl.ds(low, source.shape[0]), pl.ds(at, GROUP_WIDTH)],
                    sems.at[core * 5 + number],
                )
            )
    for copy in copies:
        copy.start()
    for copy in copies:
        copy.wait()

    def one_side(side, carry):
        columns = pl.ds(pl.multiple_of(side * 256, 256), 256)
        total = jnp.dot(rows_ref[...], w_all[:, columns], preferred_element_type=jnp.float32)
        done_ref[:, :, columns] = total.astype(jnp.bfloat16).reshape(8, HALF_TOK, 256)
        return carry

    lax.fori_loop(0, 2 * GROUP_WIDTH // 256, one_side, 0)
    out = pltpu.make_async_copy(done_ref, out_ref.at[:, pl.ds(first, HALF_TOK), :], out_sem)
    out.start()
    out.wait()


def projection(first, groups, weights, pieces, before):
    more = [] if before is None else [before]
    out = jax.ShapeDtypeStruct((8, TOK_DEV, 2 * GROUP_WIDTH), jnp.bfloat16)
    arranged = jax.ShapeDtypeStruct((8 * GROUP_WIDTH, 2 * GROUP_WIDTH), jnp.bfloat16)
    return pl.pallas_call(
        functools.partial(projection_kernel, first),
        out_shape=out if more else (out, arranged),
        in_specs=[SMEM] + [VMEM if more else ANY] + [ANY] * (10 + len(more)),
        out_specs=HBM if more else (HBM, VMEM),
        scratch_shapes=[
            pltpu.VMEM((Q_ROWS, 8 * GROUP_WIDTH), jnp.bfloat16),
            pltpu.VMEM((8, HALF_TOK, 2 * GROUP_WIDTH), jnp.bfloat16),
            pltpu.SemaphoreType.DMA((10,)),
            pltpu.SemaphoreType.DMA((16,)),
            pltpu.SemaphoreType.DMA,
        ],
        input_output_aliases={12: 0} if more else {},
        compiler_params=params(16),
        cost_estimate=cost(2_500_000_000, 9_000_000),
        name="projection",
    )(groups, weights, *pieces, *more)


def slot_tables(ids_t):
    expert = lax.broadcasted_iota(jnp.int32, (EXPERTS, TOK_DEV), 0)
    first = (expert == ids_t[0:1, :]).astype(jnp.float32)
    second = (expert == ids_t[1:2, :]).astype(jnp.float32)
    member = first + second
    before = (
        lax.broadcasted_iota(jnp.int32, (TOK_DEV, TOK_DEV), 0)
        < lax.broadcasted_iota(jnp.int32, (TOK_DEV, TOK_DEV), 1)
    ).astype(jnp.bfloat16)
    slot = jnp.dot(member.astype(jnp.bfloat16), before, preferred_element_type=jnp.float32)
    return first, second, member, slot


def dispatch_kernel(ids_ref, update_ref, residual_ref, gain_ref, router_ref, send_ref, mix_ref, normed_ref):
    squares = jnp.zeros((TOK_DEV, 1), jnp.float32)
    for half in range(2):
        for group in range(BLOCKS):
            at = half * HALF + group * BLOCK_WIDTH
            row = residual_ref[:, at : at + BLOCK_WIDTH].astype(jnp.float32) + update_ref[
                group, :, half * BLOCK_WIDTH : (half + 1) * BLOCK_WIDTH
            ].astype(jnp.float32)
            squares = squares + jnp.sum(row * row, axis=1, keepdims=True)
    factor = lax.rsqrt(squares / D + EPS)
    for half in range(2):
        for group in range(BLOCKS):
            at = half * HALF + group * BLOCK_WIDTH
            row = residual_ref[:, at : at + BLOCK_WIDTH].astype(jnp.float32) + update_ref[
                group, :, half * BLOCK_WIDTH : (half + 1) * BLOCK_WIDTH
            ].astype(jnp.float32)
            gain = gain_ref[:, at : at + BLOCK_WIDTH].astype(jnp.float32)
            normed_ref[:, at : at + BLOCK_WIDTH] = (row * factor * gain).astype(jnp.bfloat16)
    first, second, member, slot = slot_tables(ids_ref[...])
    slot_ids = lax.broadcasted_iota(jnp.int32, (SLOTS, TOK_DEV), 0).astype(jnp.float32)
    picks, tails = [], []
    last = jnp.where(slot == float(SLOTS), member, 0.0)
    for expert in range(EXPERTS):
        picks.append(
            jnp.where(slot[expert : expert + 1, :] == slot_ids, member[expert : expert + 1, :], 0.0)
        )
        tails.append(jnp.broadcast_to(last[expert : expert + 1, :], (BLOCKS, TOK_DEV)))
    pick = jnp.concatenate(picks, axis=0)
    tail = jnp.concatenate(tails, axis=0)
    tail_block = lax.broadcasted_iota(jnp.int32, (EXPERTS * BLOCKS, TOK_DEV), 0) % BLOCKS
    pick_low = pick.astype(jnp.bfloat16)
    for half in range(2):

        def one_block(block, tail_rows):
            at = pl.multiple_of(half * HALF + block * BLOCK_WIDTH, BLOCK_WIDTH)
            rows = normed_ref[:, pl.ds(at, BLOCK_WIDTH)]
            moved = jnp.dot(pick_low, rows, preferred_element_type=jnp.float32).astype(jnp.bfloat16)
            place = pl.ds(pl.multiple_of(block * SLOTS, SLOTS), SLOTS)
            for expert in range(EXPERTS):
                send_ref[2 * expert + half, place, :] = moved[
                    expert * SLOTS : (expert + 1) * SLOTS, :
                ]
            chosen = jnp.where(tail_block == block, tail, 0.0).astype(jnp.bfloat16)
            return tail_rows + jnp.dot(chosen, rows, preferred_element_type=jnp.float32)

        empty = jnp.zeros((EXPERTS * BLOCKS, BLOCK_WIDTH), jnp.float32)
        tail_rows = lax.fori_loop(0, BLOCKS, one_block, empty, unroll=True)
        tail_rows = tail_rows.astype(jnp.bfloat16)
        for expert in range(EXPERTS):
            send_ref[2 * expert + half, BLOCKS * SLOTS :, :] = tail_rows[
                expert * BLOCKS : (expert + 1) * BLOCKS, :
            ]
    logits = lax.dot_general(
        router_ref[...],
        normed_ref[...],
        (((1,), (1,)), ((), ())),
        preferred_element_type=jnp.float32,
    )
    chosen_first = jnp.sum(first * logits, axis=0, keepdims=True)
    chosen_second = jnp.sum(second * logits, axis=0, keepdims=True)
    mix_first = 1.0 / (1.0 + jnp.exp(chosen_second - chosen_first))
    mix_second = 1.0 / (1.0 + jnp.exp(chosen_first - chosen_second))
    share = first * mix_first + second * mix_second
    for expert in range(EXPERTS):
        mine = share[expert : expert + 1, :]
        mix_ref[expert * SLOTS : (expert + 1) * SLOTS, :] = picks[expert] * mine
        mix_ref[
            EXPERTS * SLOTS + expert * BLOCKS : EXPERTS * SLOTS + (expert + 1) * BLOCKS, :
        ] = tails[expert] * mine


def dispatch(ids_t, update, residual, gain, router_t):
    return pl.pallas_call(
        dispatch_kernel,
        out_shape=(
            jax.ShapeDtypeStruct((16, BLOCKS * (SLOTS + 1), BLOCK_WIDTH), jnp.bfloat16),
            jax.ShapeDtypeStruct((EXPERTS * (SLOTS + BLOCKS), TOK_DEV), jnp.float32),
        ),
        in_specs=[VMEM] * 5,
        out_specs=(VMEM, VMEM),
        scratch_shapes=[pltpu.VMEM((TOK_DEV, D), jnp.bfloat16)],
        compiler_params=params(32),
        cost_estimate=cost(800_000_000, 8_000_000),
        name="dispatch",
    )(ids_t, update, residual, gain, router_t)


PARTS = SLOTS // PART
ROWS = 16 * SLOTS
ALL_ROWS = ROWS + 16
GROUPS = 4
GROUP_DEPTH = HALF // GROUPS


def row_pick(block):
    source = lax.broadcasted_iota(jnp.int32, (16, 16 * BLOCKS), 0)
    place = lax.broadcasted_iota(jnp.int32, (16, 16 * BLOCKS), 1)
    return (place == source * BLOCKS + block).astype(jnp.bfloat16)


def first_kernel(rows_ref, u_ref, low_ref, x_ref, tail_ref, w_ref, acc_ref, sems, row_sems):
    copies = []
    for group in range(GROUPS):
        rows = pl.ds(group * GROUP_DEPTH, GROUP_DEPTH)
        copies.append(pltpu.make_async_copy(u_ref.at[0, rows], w_ref.at[rows], sems.at[group]))
    moves = [
        pltpu.make_async_copy(
            rows_ref.at[:, pl.ds(BLOCKS * SLOTS, BLOCKS), :], tail_ref, row_sems.at[2 * BLOCKS]
        )
    ]
    for block in range(BLOCKS):
        for part in range(PARTS):
            moves.append(
                pltpu.make_async_copy(
                    rows_ref.at[:, pl.ds(block * SLOTS + part * PART, PART), :],
                    x_ref.at[pl.ds(part * 16, 16), :, pl.ds(block * BLOCK_WIDTH, BLOCK_WIDTH)],
                    row_sems.at[block * PARTS + part],
                )
            )
    for move in moves[: 1 + 2 * PARTS]:
        move.start()
    copies[0].start()
    for move in moves[1 + 2 * PARTS :]:
        move.start()
    for copy in copies[1:]:
        copy.start()
    moves[0].wait()
    tail = tail_ref[...].reshape(16 * BLOCKS, BLOCK_WIDTH)
    for block in range(BLOCKS):
        picked = jnp.dot(row_pick(block), tail, preferred_element_type=jnp.float32)
        x_ref[2 * 16, :, block * BLOCK_WIDTH : (block + 1) * BLOCK_WIDTH] = picked.astype(
            jnp.bfloat16
        )
    each = BLOCKS // GROUPS * PARTS
    for group in range(GROUPS):
        at = group * GROUP_DEPTH
        for move in moves[1 + group * each : 1 + (group + 1) * each]:
            move.wait()
        copies[group].wait()
        rows = x_ref[:, :, at : at + GROUP_DEPTH].reshape(ALL_ROWS, GROUP_DEPTH)
        acc = None if group == 0 else acc_ref

        def one_tile(tile, carry, at=at, rows=rows, acc=acc, last=group == GROUPS - 1):
            columns = pl.ds(pl.multiple_of(tile * RANK_TILE, RANK_TILE), RANK_TILE)
            weights = w_ref[at : at + GROUP_DEPTH, columns]
            term = jnp.dot(rows, weights, preferred_element_type=jnp.float32)
            if acc is not None:
                term = acc[:, columns] + term
            if last:
                low_ref[:, columns] = term.astype(jnp.bfloat16)
            else:
                acc_ref[:, columns] = term
            return carry

        lax.fori_loop(0, 2 * RANK // RANK_TILE, one_tile, 0)


RANK_TILE = 512


def first_factor(received, u_gate_up):
    return pl.pallas_call(
        first_kernel,
        out_shape=jax.ShapeDtypeStruct((ALL_ROWS, 2 * RANK), jnp.bfloat16),
        in_specs=[ANY, ANY],
        out_specs=VMEM,
        scratch_shapes=[
            pltpu.VMEM((16 * PARTS + 1, PART, HALF), jnp.bfloat16),
            pltpu.VMEM((16, BLOCKS, BLOCK_WIDTH), jnp.bfloat16),
            pltpu.VMEM((HALF, 2 * RANK), jnp.bfloat16),
            pltpu.VMEM((ALL_ROWS, 2 * RANK), jnp.float32),
            pltpu.SemaphoreType.DMA((GROUPS,)),
            pltpu.SemaphoreType.DMA((BLOCKS * PARTS + 1,)),
        ],
        compiler_params=params(58),
        cost_estimate=cost(3_400_000_000, 9_000_000),
        name="first_factor",
    )(received, u_gate_up)


FF_TILE = 1024
FF_STEPS = FF_PIECE // FF_TILE


def middle_kernel(own_ref, got_ref, v_ref, u_ref, low_ref, rank_ref, vs_ref, us_ref, acc_ref, sems):
    copies = []
    for step in range(FF_STEPS):
        columns = pl.ds(step * FF_TILE, FF_TILE)
        copies.append(
            (
                pltpu.make_async_copy(
                    v_ref.at[0, :, :, columns], vs_ref.at[:, :, columns], sems.at[2 * step]
                ),
                pltpu.make_async_copy(
                    u_ref.at[0, columns, :], us_ref.at[columns, :], sems.at[2 * step + 1]
                ),
            )
        )
    for pair in copies:
        for copy in pair:
            copy.start()
    rank_ref[...] = (
        own_ref[...].astype(jnp.float32) + got_ref[...].astype(jnp.float32)
    ).astype(jnp.bfloat16)
    acc_ref[...] = jnp.zeros(acc_ref.shape, jnp.float32)

    def one_tile(step, carry):
        columns = pl.ds(pl.multiple_of(step * FF_TILE, FF_TILE), FF_TILE)
        pltpu.make_async_copy(
            v_ref.at[0, :, :, columns], vs_ref.at[:, :, columns], sems.at[2 * step]
        ).wait()
        pltpu.make_async_copy(
            u_ref.at[0, columns, :], us_ref.at[columns, :], sems.at[2 * step + 1]
        ).wait()
        gate = jnp.dot(rank_ref[:, :RANK], vs_ref[0, :, columns], preferred_element_type=jnp.float32)
        up = jnp.dot(rank_ref[:, RANK:], vs_ref[1, :, columns], preferred_element_type=jnp.float32)
        low = 0.5 * gate
        hidden = ((low + low * jnp.tanh(low)) * up).astype(jnp.bfloat16)
        acc_ref[...] += jnp.dot(hidden, us_ref[columns, :], preferred_element_type=jnp.float32)
        return carry

    lax.fori_loop(0, FF_STEPS, one_tile, 0)
    low_ref[...] = acc_ref[...].astype(jnp.bfloat16)


def middle(own, got, v_gate_up, u_down):
    return pl.pallas_call(
        middle_kernel,
        out_shape=jax.ShapeDtypeStruct((ALL_ROWS, RANK), jnp.bfloat16),
        in_specs=[VMEM, VMEM, ANY, ANY],
        out_specs=VMEM,
        scratch_shapes=[
            pltpu.VMEM((ALL_ROWS, 2 * RANK), jnp.bfloat16),
            pltpu.VMEM((2, RANK, FF_PIECE), jnp.bfloat16),
            pltpu.VMEM((FF_PIECE, RANK), jnp.bfloat16),
            pltpu.VMEM((ALL_ROWS, RANK), jnp.float32),
            pltpu.SemaphoreType.DMA((2 * FF_STEPS,)),
        ],
        compiler_params=params(60),
        cost_estimate=cost(6_700_000_000, 14_000_000, 2_200_000),
        name="middle",
    )(own, got, v_gate_up, u_down)


def last_kernel(own_ref, got_ref, v_ref, out_ref, down_ref, w_ref, tail_ref, sems):
    copies = []
    for block in range(BLOCKS):
        columns = pl.ds(block * BLOCK_WIDTH, BLOCK_WIDTH)
        copies.append(
            pltpu.make_async_copy(v_ref.at[0, :, columns], w_ref.at[:, columns], sems.at[block])
        )
    for copy in copies:
        copy.start()
    down_ref[...] = (
        own_ref[...].astype(jnp.float32) + got_ref[...].astype(jnp.float32)
    ).astype(jnp.bfloat16)
    place = lax.broadcasted_iota(jnp.int32, (16 * BLOCKS, 16), 0)
    source = lax.broadcasted_iota(jnp.int32, (16 * BLOCKS, 16), 1)
    tail_ref[...] = jnp.zeros(tail_ref.shape, jnp.float32)

    def one_block(block, carry):
        columns = pl.ds(pl.multiple_of(block * BLOCK_WIDTH, BLOCK_WIDTH), BLOCK_WIDTH)
        pltpu.make_async_copy(v_ref.at[0, :, columns], w_ref.at[:, columns], sems.at[block]).wait()
        spread = (place == source * BLOCKS + block).astype(jnp.bfloat16)
        lifted = jnp.dot(spread, down_ref[ROWS:, :], preferred_element_type=jnp.float32)
        rows = jnp.concatenate([down_ref[:ROWS, :], lifted.astype(jnp.bfloat16)], axis=0)
        result = jnp.dot(rows, w_ref[:, columns], preferred_element_type=jnp.float32)
        main = result[:ROWS].astype(jnp.bfloat16).reshape(PARTS, 16, PART, BLOCK_WIDTH)
        for part in range(PARTS):
            at = pl.ds(pl.multiple_of(block * SLOTS + part * PART, PART), PART)
            out_ref[:, at, :] = main[part]
        tail_ref[...] += result[ROWS:]
        return carry

    lax.fori_loop(0, BLOCKS, one_block, 0)
    out_ref[:, BLOCKS * SLOTS :, :] = (
        tail_ref[...].astype(jnp.bfloat16).reshape(16, BLOCKS, BLOCK_WIDTH)
    )


def last_factor(own, got, v_down):
    return pl.pallas_call(
        last_kernel,
        out_shape=jax.ShapeDtypeStruct((16, BLOCKS * (SLOTS + 1), BLOCK_WIDTH), jnp.bfloat16),
        in_specs=[VMEM, VMEM, ANY],
        out_specs=VMEM,
        scratch_shapes=[
            pltpu.VMEM((ALL_ROWS, RANK), jnp.bfloat16),
            pltpu.VMEM((RANK, HALF), jnp.bfloat16),
            pltpu.VMEM((16 * BLOCKS, BLOCK_WIDTH), jnp.float32),
            pltpu.SemaphoreType.DMA((BLOCKS,)),
        ],
        compiler_params=params(24),
        cost_estimate=cost(1_700_000_000, 6_000_000),
        name="last_factor",
    )(own, got, v_down)


def combine_kernel(mix_ref, update_ref, residual_ref, back_ref, out_ref):
    mix = mix_ref[: EXPERTS * SLOTS, :].T
    tail = mix_ref[EXPERTS * SLOTS :, :].T
    mix_high = mix.astype(jnp.bfloat16)
    mix_low = (mix - mix_high.astype(jnp.float32)).astype(jnp.bfloat16)
    tail_block = lax.broadcasted_iota(jnp.int32, (TOK_DEV, EXPERTS * BLOCKS), 1) % BLOCKS
    for half in range(2):
        tail_rows = jnp.concatenate(
            [back_ref[2 * expert + half, BLOCKS * SLOTS :, :] for expert in range(EXPERTS)], axis=0
        )

        def one_block(block, carry):
            at_rows = pl.ds(pl.multiple_of(block * SLOTS, SLOTS), SLOTS)
            rows = jnp.concatenate(
                [back_ref[2 * expert + half, at_rows, :] for expert in range(EXPERTS)], axis=0
            )
            here = jnp.where(tail_block == block, tail, 0.0)
            here_high = here.astype(jnp.bfloat16)
            here_low = (here - here_high.astype(jnp.float32)).astype(jnp.bfloat16)
            mixture = jnp.dot(mix_high, rows, preferred_element_type=jnp.float32)
            mixture = mixture + jnp.dot(mix_low, rows, preferred_element_type=jnp.float32)
            mixture = mixture + jnp.dot(here_high, tail_rows, preferred_element_type=jnp.float32)
            mixture = mixture + jnp.dot(here_low, tail_rows, preferred_element_type=jnp.float32)
            at = pl.ds(pl.multiple_of(half * HALF + block * BLOCK_WIDTH, BLOCK_WIDTH), BLOCK_WIDTH)
            stream = residual_ref[:, at].astype(jnp.float32) + update_ref[
                block, :, half * BLOCK_WIDTH : (half + 1) * BLOCK_WIDTH
            ].astype(jnp.float32)
            out_ref[:, at] = (stream + mixture).astype(jnp.bfloat16)
            return carry

        lax.fori_loop(0, BLOCKS, one_block, 0, unroll=UNROLL)


def combine(mix, update, residual, back):
    return pl.pallas_call(
        combine_kernel,
        out_shape=jax.ShapeDtypeStruct((TOK_DEV, D), jnp.bfloat16),
        in_specs=[VMEM] * 4,
        out_specs=VMEM,
        compiler_params=params(32),
        cost_estimate=cost(1_000_000_000, 8_000_000),
        name="combine",
    )(mix, update, residual, back)


def per_device(
    queries,
    keys,
    values,
    residual,
    proj_weight,
    norm_gain,
    router,
    expert_ids,
    u_gate_up,
    v_gate_up,
    u_down,
    v_down,
):
    zh, x, zl = lax.axis_index("zh"), lax.axis_index("x"), lax.axis_index("zl")
    y, c = lax.axis_index("y"), lax.axis_index("c")
    z = zh * 2 + zl
    chunk = zh * 8 + x * 2 + zl

    q_far = mirrored(queries[HALF_TOK:])
    kv = pack_kv(keys, values)
    kv = lax.all_to_all(kv, "y", split_axis=0, concat_axis=0, tiled=True)
    kv = kv.reshape(4 * TOK_DEV, 2 * HEAD_DIM)
    early, late = kv[:256], kv[256:]

    copies = jnp.broadcast_to(proj_weight[None], (16, GROUP_WIDTH, GROUP_WIDTH))
    q = pack_q(queries, q_far)
    q = lax.all_to_all(q, GROUP, split_axis=0, concat_axis=0, tiled=True)

    def joined(pieces):
        return jnp.concatenate(pieces, axis=0)

    early = joined(direct_pieces(early, Z))
    late = joined(direct_pieces(late, "x"))
    own = ring_pieces(early, "x") + ring_pieces(late, Z)
    swapped = [other_core(p) for p in own]

    far_chunk = 15 - chunk
    order = jnp.arange(15, dtype=jnp.int32)
    is_far = order >= chunk
    slot_list = jnp.concatenate([is_far.astype(jnp.int32), jnp.array([0, 1], jnp.int32)])
    chunk_list = jnp.concatenate(
        [jnp.where(is_far, order - chunk, order), jnp.stack([chunk, far_chunk])]
    )
    there_z = chunk_list // 8 * 2 + chunk_list % 2
    there_x = chunk_list // 2 % 4
    rel_z = relative(z, there_z)
    rel_x = relative(x, there_x)
    rows = jnp.stack([slot_list, rel_x * 4 + rel_z, rel_z * 4 + rel_x], axis=1)
    items = jnp.concatenate([jnp.array([15, 2], jnp.int32), rows.reshape(-1)]).astype(jnp.int32)
    key_ids = jnp.arange(KEY_PART, dtype=jnp.int32)
    base = key_ids // TOK_DEV * 256 + key_ids % TOK_DEV
    kpos = jnp.stack(
        [
            base + c * TOK_DEV,
            base + c * TOK_DEV + 512,
            base + (1 - c) * TOK_DEV,
            base + (1 - c) * TOK_DEV + 512,
        ]
    ).astype(jnp.int32)

    attended = attention(items, kpos, q, own + swapped)
    weight_rows = lax.all_to_all(copies, PLANE, split_axis=0, concat_axis=0, tiled=True)
    weight_rows = weight_rows.reshape(8, 2, GROUP_WIDTH, GROUP_WIDTH)
    from_y = jnp.stack([y, (y - 1) % 4, (y + 1) % 4, (y + 2) % 4])
    groups = jnp.concatenate([from_y * 2 + c, from_y * 2 + 1 - c]).astype(jnp.int32)
    near = ring_pieces(attended[0], "y")
    far = mirrored(attended[1])
    near = near + [other_core(p) for p in near]
    far = ring_pieces(far, "y")
    far = far + [other_core(p) for p in far]
    projected, arranged = projection(0, groups, weight_rows, near, None)
    projected = projection(HALF_TOK, groups, arranged, far, projected)
    update = lax.all_to_all(projected, GROUP, split_axis=0, concat_axis=0, tiled=True)

    ids_t = expert_ids.T
    send, mix = dispatch(ids_t, update, residual, norm_gain.reshape(1, D), router.T)
    received = lax.all_to_all(send, EXP, split_axis=0, concat_axis=0, tiled=True)
    rank_low = first_factor(received, u_gate_up)
    down_low = middle(rank_low, other_core(rank_low), v_gate_up, u_down)
    out_rows = last_factor(down_low, other_core(down_low), v_down)
    back = lax.all_to_all(out_rows, EXP, split_axis=0, concat_axis=0, tiled=True)
    return combine(mix, update, residual, back)


def solution(mesh):
    fine = Mesh(mesh.devices.reshape(2, 4, 2, 4, 2), ("zh", "x", "zl", "y", "c"))
    seq, exp = ("zh", "x"), ("zl", "y", "c")
    in_specs = (
        P(seq + exp, None),
        P(seq + exp, None),
        P(seq + exp, None),
        P(seq + exp, None),
        P(seq, exp),
        P(),
        P(),
        P(seq + exp, None),
        P(exp, None, None),
        P(exp, None, None, None),
        P(exp, None, None),
        P(exp, None, None),
    )

    return jax.shard_map(
        per_device, mesh=fine, in_specs=in_specs, out_specs=P(seq + exp, None), check_vma=False
    )
```
